32 devices in a mesh: dp: 2 (over x), tp: 4 (over z), cp: 4 (over y, core).
Axes of the slice: x: 2, y: 2, z: 4, core: 2. Of those that a mesh axis runs over, the one named last changes fastest.
Arguments:
- x: bfloat16 [8192, 4096], P(('dp', 'cp')), parts along dimension 0
- k_cache: bfloat16 [2048, 8, 128], P(('dp', 'cp'), 'tp'), parts along dimension 0
- v_cache: bfloat16 [2048, 8, 128], P(('dp', 'cp'), 'tp'), parts along dimension 0
- rope_table: float32 [8192, 64], P(('dp', 'cp')), parts along dimension 0
- norm_gain: bfloat16 [4096], replicated
- w_qkv: bfloat16 [4096, 14336], P(None, 'tp')
- b_qkv: bfloat16 [14336], P('tp')
- w_out: bfloat16 [12288, 4096], P('tp')
Outputs:
- output 1: bfloat16 [8192, 4096], P(('dp', 'cp')), parts along dimension 0
- output 2: bfloat16 [8192, 8, 128], P(('dp', 'cp'), 'tp'), parts along dimension 0
- output 3: bfloat16 [8192, 8, 128], P(('dp', 'cp'), 'tp'), parts along dimension 0
There are 2 independent parts. The reference program is written for one: setup_inputs(seed, part) draws one part's arguments, and reference() takes and returns one part's arrays. A program takes and returns all parts, laid end to end along the dimension named above; an argument that names none is the same for every part.
All inputs are finite; a program needn't handle non-finite values.
Results may differ from the reference program's by a relative error of at most 0.00443274.
Values are sent between devices in bfloat16 or wider.
A program may use at most 1 GiB of HBM per device.

```python
import math
import jax
import jax.numpy as jnp
from jax import lax

D = 4096
HEADS = 96
KV_HEADS = 8
HEAD = 128
NEW_TOKENS = 4096
PREFIX = 1024
EPS = 1.5625e-07
MASK_VALUE = -1e30
GROUP = HEADS // KV_HEADS
QKV_WIDTH = (HEADS + 2 * KV_HEADS) * HEAD
PAIR_COUNT = HEAD // 4
QUERY_BLOCK = math.gcd(NEW_TOKENS, 128)
KEY_BLOCK = math.gcd(PREFIX + NEW_TOKENS, 512)


def setup_inputs(seed: int = 0, part: int = 0) -> dict:
    part_keys = jax.random.split(jax.random.fold_in(jax.random.key(seed), part), 4)
    shared_keys = jax.random.split(jax.random.key(seed + 1), 4)
    x = jax.random.normal(part_keys[0], (NEW_TOKENS, D), jnp.float32)
    k_cache = 1.6 * jax.random.normal(part_keys[1], (PREFIX, KV_HEADS, HEAD), jnp.float32)
    v_cache = 1.6 * jax.random.normal(part_keys[2], (PREFIX, KV_HEADS, HEAD), jnp.float32)
    log_ratio = jax.random.uniform(part_keys[3], (), jnp.float32, math.log(100.0), math.log(10000.0))
    rope_base = 10000.0 * jnp.exp(log_ratio)
    inv_freq = rope_base ** (-jnp.arange(PAIR_COUNT, dtype=jnp.float32) / PAIR_COUNT)
    positions = (PREFIX + jnp.arange(NEW_TOKENS)).astype(jnp.float32)
    angles = positions[:, None] * inv_freq[None, :]
    rope_table = jnp.concatenate([jnp.cos(angles), jnp.sin(angles)], axis=1)
    norm_gain = 1.0 + 0.3 * jax.random.normal(shared_keys[0], (D,), jnp.float32)
    w_qkv = jax.random.normal(shared_keys[1], (D, QKV_WIDTH), jnp.float32) * (1.5 / math.sqrt(D))
    b_qkv = 0.5 * jax.random.normal(shared_keys[2], (QKV_WIDTH,), jnp.float32)
    w_out = jax.random.normal(shared_keys[3], (HEADS * HEAD, D), jnp.float32) / math.sqrt(HEADS * HEAD)
    return dict(x=x.astype(jnp.bfloat16), k_cache=k_cache.astype(jnp.bfloat16), v_cache=v_cache.astype(jnp.bfloat16), rope_table=rope_table.astype(jnp.float32), norm_gain=norm_gain.astype(jnp.bfloat16), w_qkv=w_qkv.astype(jnp.bfloat16), b_qkv=b_qkv.astype(jnp.bfloat16), w_out=w_out.astype(jnp.bfloat16))


def apply_rotary(vals, cos_t, sin_t):
    pair_count = cos_t.shape[-1]
    lead_shape = vals.shape[:-1]
    paired = vals[..., :2 * pair_count].reshape(lead_shape + (pair_count, 2))
    even_part = paired[..., 0]
    odd_part = paired[..., 1]
    turned = jnp.stack([even_part * cos_t - odd_part * sin_t, odd_part * cos_t + even_part * sin_t], axis=-1)
    return jnp.concatenate([turned.reshape(lead_shape + (2 * pair_count,)), vals[..., 2 * pair_count:]], axis=-1)


def reference(x, k_cache, v_cache, rope_table, norm_gain, w_qkv, b_qkv, w_out):
    x_f32 = x.astype(jnp.float32)
    inv_rms = lax.rsqrt(jnp.mean(x_f32 * x_f32, axis=-1, keepdims=True) + EPS)
    hidden = (x_f32 * inv_rms * norm_gain.astype(jnp.float32)).astype(jnp.bfloat16)
    qkv_all = jnp.dot(hidden, w_qkv, preferred_element_type=jnp.float32) + b_qkv.astype(jnp.float32)
    qkv_all = qkv_all.reshape(NEW_TOKENS, KV_HEADS, GROUP + 2, HEAD)
    cos_t = rope_table[:, :PAIR_COUNT]
    sin_t = rope_table[:, PAIR_COUNT:]
    queries = apply_rotary(qkv_all[:, :, :GROUP], cos_t[:, None, None], sin_t[:, None, None]).astype(jnp.bfloat16)
    new_k = apply_rotary(qkv_all[:, :, GROUP], cos_t[:, None], sin_t[:, None]).astype(jnp.bfloat16)
    new_v = qkv_all[:, :, GROUP + 1].astype(jnp.bfloat16)
    key_count = PREFIX + NEW_TOKENS
    key_blocks = key_count // KEY_BLOCK
    keys_all = jnp.concatenate([k_cache, new_k], axis=0).reshape(key_blocks, KEY_BLOCK, KV_HEADS, HEAD)
    vals_all = jnp.concatenate([v_cache, new_v], axis=0).reshape(key_blocks, KEY_BLOCK, KV_HEADS, HEAD)
    key_pos = jnp.arange(key_count).reshape(key_blocks, KEY_BLOCK)
    q_blocks = queries.reshape(NEW_TOKENS // QUERY_BLOCK, QUERY_BLOCK, KV_HEADS, GROUP, HEAD)
    q_pos = (PREFIX + jnp.arange(NEW_TOKENS)).reshape(NEW_TOKENS // QUERY_BLOCK, QUERY_BLOCK)
    scale = HEAD ** -0.5

    def query_block(block):
        q_vals, q_at = block
        q_f32 = q_vals.astype(jnp.float32)

        def key_step(carry, kv_block):
            run_max, run_sum, weighted = carry
            k_vals, v_vals, k_at = kv_block
            scores = jnp.einsum('qngd,knd->qngk', q_f32, k_vals.astype(jnp.float32)) * scale
            visible = (k_at[None, :] <= q_at[:, None])[:, None, None, :]
            scores = jnp.where(visible, scores, MASK_VALUE)
            new_max = jnp.maximum(run_max, scores.max(axis=-1))
            rescale = jnp.exp(run_max - new_max)
            probs = jnp.exp(scores - new_max[..., None])
            run_sum = run_sum * rescale + probs.sum(axis=-1)
            weighted = weighted * rescale[..., None] + jnp.einsum('qngk,knd->qngd', probs.astype(jnp.bfloat16).astype(jnp.float32), v_vals.astype(jnp.float32))
            return (new_max, run_sum, weighted), None

        start_carry = (jnp.full((QUERY_BLOCK, KV_HEADS, GROUP), MASK_VALUE, jnp.float32), jnp.zeros((QUERY_BLOCK, KV_HEADS, GROUP), jnp.float32), jnp.zeros((QUERY_BLOCK, KV_HEADS, GROUP, HEAD), jnp.float32))
        (run_max, run_sum, weighted), _ = lax.scan(key_step, start_carry, (keys_all, vals_all, key_pos))
        return weighted / run_sum[..., None]

    attn = lax.map(query_block, (q_blocks, q_pos))
    attn = attn.reshape(NEW_TOKENS, HEADS * HEAD).astype(jnp.bfloat16)
    y = (x_f32 + jnp.dot(attn, w_out, preferred_element_type=jnp.float32)).astype(jnp.bfloat16)
    return y, new_k, new_v
```

```python
import functools
import math

import jax
import jax.numpy as jnp
from jax import lax
from jax.experimental import pallas as pl
from jax.experimental.pallas import tpu as pltpu
from jax.sharding import PartitionSpec as P

EPS = 1.5625e-07
LOW = -1e30
HEAD = 128
QUAD = 4
MESH = pl.DeviceIdType.MESH


class Plan:
    def __init__(self, tok, dim, kv, group, cache, nm, kt):
        self.tok, self.dim, self.kv, self.group, self.cache = tok, dim, kv, group, cache
        self.nm = nm
        self.mr = tok // nm
        self.kt = kt
        self.nq = kv * group // QUAD
        self.qpg = group // QUAD
        self.n = QUAD * self.mr
        self.keys = tok * 5
        self.heads = kv * group
        self.wcols = QUAD * HEAD
        self.nt = dim // self.wcols
        self.cpm = 4
        self.cc = dim // self.cpm
        self.half = self.mr // 2
        self.wt = self.nq + self.nt
        self.slots = 3
        self.owns = 2
        self.s_own = self.nq
        self.s_near = self.s_own + 1
        self.s_far = self.s_near + self.nq
        self.s_fin = self.s_far + self.nq
        self.s_out = self.s_fin + 1
        self.nseg = self.s_out + self.nt
        self.sp = self.nseg // self.cpm
        self.ob = self.s_out + self.nt // self.cpm - 1
        self.od = 9
        self.ab = self.ob + 4 * self.od
        self.ad = 9
        self.chunks = self.nm * self.cpm
        self.total = self.nseg * (self.nm - 1) + self.ab + 2 * self.ad + self.sp * (self.cpm - 1) + 1


def kernel(p, x, kc, vc, rope_in, gain, bias, wqkv, wout, y, kn, vn,
           h, ka, vt, rope, q, o_t, o, s_a, s_b, p_s, mx_a, mx_b, m_s, l_s, own, land, yst, xb, w, vb,
           x_sem, w_sem, b_sem, out_sem, cs_send, cs_recv, kv_send, kv_recv,
           rs_send, rs_recv, ag_send, ag_recv, yl_sem):
    tp = lax.axis_index('tp')
    cp = lax.axis_index('cp')
    partner = cp + 1 - 2 * lax.rem(cp, 2)
    across = lax.rem(cp + 2, 4)
    scale = HEAD ** -0.5 * math.log2(math.e)
    new0 = p.tok * (1 + cp)
    rows4 = p.tok // 4

    def wq_col(j):
        return (j // p.qpg) * (p.group + 2) * HEAD + lax.rem(j, p.qpg) * p.wcols

    def w_copy(t, kind, slot):
        j = lax.rem(t, p.wt)
        if kind == 'q':
            col = pl.multiple_of(wq_col(j), HEAD)
            return pltpu.make_async_copy(wqkv.at[:, pl.ds(col, p.wcols)], w.at[slot], w_sem.at[slot])
        col = pl.multiple_of((j - p.nq) * p.wcols, HEAD)
        return pltpu.make_async_copy(wout.at[:, pl.ds(col, p.wcols)], w.at[slot, pl.ds(0, p.heads * HEAD)], w_sem.at[slot])

    def w_start(t):
        slot = lax.rem(t, p.slots)
        j = lax.rem(t, p.wt)

        @pl.when((t < p.nm * p.wt) & (j < p.nq))
        def _():
            w_copy(t, 'q', slot).start()

        @pl.when((t < p.nm * p.wt) & (j >= p.nq))
        def _():
            w_copy(t, 'o', slot).start()

    def x_copy(r):
        rows = pl.ds(r * rows4, rows4)
        return pltpu.make_async_copy(x.at[rows], h.at[rows], x_sem.at[r])

    kv_slot = p.slots - 1

    def wkv_copy(g):
        col = g * (p.group + 2) * HEAD + p.group * HEAD
        return pltpu.make_async_copy(wqkv.at[:, pl.ds(col, 2 * HEAD)], w.at[kv_slot, :, pl.ds(g * 2 * HEAD, 2 * HEAD)], b_sem.at[g])

    x_copy(0).start()
    for g in range(p.kv):
        wkv_copy(g).start()
    rope_copy = pltpu.make_async_copy(rope_in, rope, b_sem.at[2])
    rope_copy.start()
    kc_copy = pltpu.make_async_copy(kc, ka.at[:, pl.ds(cp * p.cache, p.cache)], b_sem.at[3])
    vc_copy = pltpu.make_async_copy(vc, vt.at[:, :, pl.ds(pl.multiple_of(cp * p.cache, p.cache), p.cache)], b_sem.at[4])
    kc_copy.start()
    vc_copy.start()
    for r in range(1, 4):
        x_copy(r).start()
    w_start(0)
    w_start(1)

    barrier = pltpu.get_barrier_semaphore()
    for k in range(1, 4):
        pl.semaphore_signal(barrier, inc=1, device_id={'tp': lax.rem(tp + k, 4)}, device_id_type=MESH)
        pl.semaphore_signal(barrier, inc=1, device_id={'cp': lax.rem(cp + k, 4)}, device_id_type=MESH)
    pl.semaphore_wait(barrier, 6)

    def cache_copies(owner, peer, k):
        at = pl.multiple_of(owner * p.cache, p.cache)
        ks = ka.at[:, pl.ds(at, p.cache)]
        vs = vt.at[:, :, pl.ds(at, p.cache)]
        return (pltpu.make_async_remote_copy(ks, ks, cs_send.at[k, 0], cs_recv.at[k, 0], device_id={'cp': peer}, device_id_type=MESH),
                pltpu.make_async_remote_copy(vs, vs, cs_send.at[k, 1], cs_recv.at[k, 1], device_id={'cp': peer}, device_id_type=MESH))

    def new_copies(at, size, peer, k):
        ks = ka.at[:, pl.ds(at, size)]
        vs = vt.at[:, :, pl.ds(at, size)]
        return (pltpu.make_async_remote_copy(ks, ks, kv_send.at[k, 0], kv_recv.at[k, 0], device_id={'cp': peer}, device_id_type=MESH),
                pltpu.make_async_remote_copy(vs, vs, kv_send.at[k, 1], kv_recv.at[k, 1], device_id={'cp': peer}, device_id_type=MESH))

    kc_copy.wait()
    vc_copy.wait()
    for peer, k in ((across, 1), (partner, 0)):
        for c in cache_copies(cp, peer, k):
            c.start()

    def send_new(r):
        at = pl.multiple_of(new0 + r * rows4, rows4)

        @pl.when(cp < 2)
        def _():
            for c in new_copies(at, rows4, across, 1):
                c.start()

        @pl.when(lax.rem(cp, 2) == 0)
        def _():
            for c in new_copies(at, rows4, partner, 0):
                c.start()

    lane = lax.broadcasted_iota(jnp.int32, (1, HEAD), 1)
    even = lax.rem(lane, 2) == 0
    turned = lane < 64

    def rotate(a, rows):
        c = rope[rows, 0:HEAD]
        s = rope[rows, HEAD:2 * HEAD]
        swap = jnp.where(even, pltpu.roll(a, HEAD - 1, 1), pltpu.roll(a, 1, 1))
        return jnp.where(turned, a * c + swap * s, a)

    rope_copy.wait()
    for g in range(p.kv):
        wkv_copy(g).wait()
    nsub = max(1, rows4 // 64)
    sub = rows4 // nsub

    def kv_step(r, _):
        x_copy(r).wait()

        @pl.when(r > 0)
        def _():
            send_new(r - 1)

        def norm(b, _):
            rows = pl.ds(pl.multiple_of(r * rows4 + b * sub, sub), sub)
            v = h[rows, :].astype(jnp.float32)
            inv = lax.rsqrt(jnp.mean(v * v, axis=1, keepdims=True) + EPS)
            h[rows, :] = (v * inv * gain[...]).astype(jnp.bfloat16)
            return 0

        lax.fori_loop(0, nsub, norm, 0)
        rows = pl.ds(pl.multiple_of(r * rows4, rows4), rows4)
        at = pl.multiple_of(new0 + r * rows4, rows4)
        a = jnp.dot(h[rows, :], w[kv_slot], preferred_element_type=jnp.float32)
        for g in range(p.kv):
            col = g * (p.group + 2) * HEAD + p.group * HEAD
            key = rotate(a[:, g * 2 * HEAD:g * 2 * HEAD + HEAD] + bias[0:1, col:col + HEAD], rows)
            val = a[:, g * 2 * HEAD + HEAD:(g + 1) * 2 * HEAD] + bias[0:1, col + HEAD:col + 2 * HEAD]
            ka[g, pl.ds(at, rows4), :] = key.astype(jnp.bfloat16)
            vb[g, rows, :] = val.astype(jnp.bfloat16)
            vt[g, :, pl.ds(at, rows4)] = val.T.astype(jnp.bfloat16)
        return 0

    lax.fori_loop(0, 4, kv_step, 0)
    send_new(3)
    w_start(2)

    def out_copies():
        res = []
        for g in range(p.kv):
            cols = pl.ds(g * HEAD, HEAD)
            res.append(pltpu.make_async_copy(ka.at[g, pl.ds(new0, p.tok)], kn.at[:, cols], out_sem.at[g]))
            res.append(pltpu.make_async_copy(vb.at[g], vn.at[:, cols], out_sem.at[p.kv + g]))
        return res

    for c in out_copies():
        c.start()

    def reset(i, _):
        m_s[i] = jnp.full((8, p.n), LOW, jnp.float32)
        l_s[i] = jnp.zeros((8, p.n), jnp.float32)
        o_t[i] = jnp.zeros((HEAD, p.n), jnp.float32)
        return 0

    lax.fori_loop(0, p.nq, reset, 0)

    sb = min(256, p.kt)
    ss = min(128, p.kt)
    pk = min(256, p.kt)

    def scores(hq, off, kk, s_ref, mx, bound):
        g = hq // p.qpg
        s = lax.dot_general(ka[g, pl.ds(pl.multiple_of(off + kk, sb), sb), :], q[hq], (((1,), (1,)), ((), ())),
                            preferred_element_type=jnp.float32)
        if bound is not None:
            row = lax.rem(lax.broadcasted_iota(jnp.int32, (sb, p.n), 1), p.mr)
            key = lax.broadcasted_iota(jnp.int32, (sb, p.n), 0)
            s = jnp.where(row - key >= kk - bound, s, LOW)
        s_ref[kk:kk + sb, :] = s
        top = jnp.max(s.reshape(sb // 8, 8, p.n), axis=0)
        return top if mx is None else jnp.maximum(mx, top)

    def all_scores(hq, off, s_ref, mx_ref, bound):
        mx = None
        for kk in range(0, p.kt, sb):
            mx = scores(hq, off, kk, s_ref, mx, bound)
        mx_ref[...] = mx

    def tile(hq, off, s_ref, mx_ref, hq_n, off_n, s_next, mx_next, bound_n):
        g = hq // p.qpg
        m_old = m_s[hq, 0:1, :]
        m_new = jnp.maximum(m_old, jnp.max(mx_ref[...], axis=0, keepdims=True))
        alpha = jnp.exp2((m_old - m_new) * scale)
        m_s[hq, 0:1, :] = m_new
        mc = m_new * scale
        mx = acc = out = None
        for kk in range(0, p.kt, pk):
            for k2 in range(kk, kk + pk, sb):
                mx = scores(hq_n, off_n, k2, s_next, mx, bound_n)
            for k2 in range(kk, kk + pk, ss):
                e = jnp.exp2(s_ref[k2:k2 + ss, :] * scale - mc)
                part = jnp.sum(e.reshape(ss // 8, 8, p.n), axis=0)
                acc = part if acc is None else acc + part
                p_s[k2:k2 + ss, :] = e.astype(jnp.bfloat16)
            d = jnp.dot(vt[g, :, pl.ds(pl.multiple_of(off + kk, pk), pk)], p_s[kk:kk + pk, :], preferred_element_type=jnp.float32)
            out = d if out is None else out + d
        mx_next[...] = mx
        l_s[hq] = l_s[hq] * alpha + acc
        o_t[hq] = o_t[hq] * alpha + out

    def own_segment(m):
        pairs = p.nq // 2
        tiles = (m * p.mr + p.mr + p.kt - 1) // p.kt
        last = tiles * pairs - 1

        def bound(j):
            return m * p.mr - j * p.kt

        all_scores(0, new0, s_a, mx_a, bound(0))

        def step(u, _):
            j = u // pairs
            hq = 2 * lax.rem(u, pairs)
            un = jnp.minimum(u + 1, last)
            jn = un // pairs
            hn = 2 * lax.rem(un, pairs)
            off = new0 + j * p.kt
            tile(hq, off, s_a, mx_a, hq + 1, off, s_b, mx_b, bound(j))
            tile(hq + 1, off, s_b, mx_b, hn, new0 + jn * p.kt, s_a, mx_a, bound(jn))
            return 0

        lax.fori_loop(0, tiles * pairs, step, 0)

    def block_segment(hq, count, offset):
        @pl.when(hq == 0)
        def _():
            all_scores(hq, offset(0), s_a, mx_a, None)

        def step(b, _):
            off = offset(b)
            more = b + 1 < count
            hn = jnp.where(more, hq, jnp.minimum(hq + 1, p.nq - 1))
            on = offset(jnp.where(more, b + 1, 0))
            tile(hq, off, s_a, mx_a, hq, off + p.kt, s_b, mx_b, None)
            tile(hq, off + p.kt, s_b, mx_b, hn, on, s_a, mx_a, None)
            return 0

        lax.fori_loop(0, count, step, 0)

    near = 1 + lax.rem(cp, 2)
    far = 2 * (cp // 2)

    role_a = 3 - tp
    role_b = tp

    def chain(d, i):
        m = i // p.cpm
        j = lax.rem(i, p.cpm)
        mine = own.at[lax.rem(m, p.owns), j, pl.ds(d * p.half, p.half)]
        rows = pl.ds(pl.multiple_of(m * p.mr + d * p.half, p.half), p.half)
        cols = pl.ds(pl.multiple_of(j * p.cc, p.cc), p.cc)
        return mine, land.at[d, i], y.at[rows, cols]

    def peers(d):
        return (jnp.maximum(tp - 1, 0), jnp.minimum(tp + 1, 3)) if d == 0 else (jnp.minimum(tp + 1, 3), jnp.maximum(tp - 1, 0))

    def rs_copy(d, i):
        mine, there, _ = chain(d, i)
        return pltpu.make_async_remote_copy(mine, there, rs_send.at[d, i], rs_recv.at[d, i], device_id={'tp': peers(d)[0]}, device_id_type=MESH)

    def ag_copy(d, i, src=None):
        out = chain(d, i)[2]
        return pltpu.make_async_remote_copy(out if src is None else src, out, ag_send.at[d, i], ag_recv.at[d, i],
                                            device_id={'tp': peers(d)[1]}, device_id_type=MESH)

    def yl_copy(d, i):
        k = lax.rem(i, p.cpm)
        return pltpu.make_async_copy(yst.at[d, k], chain(d, i)[2], yl_sem.at[d, k])

    def when_due(seg, first, act):
        t = jnp.maximum(seg - first, 0)
        m = t // p.nseg
        rest = lax.rem(t, p.nseg)

        @pl.when((seg >= first) & (m < p.nm) & (lax.rem(rest, p.sp) == 0) & (rest < p.sp * p.cpm))
        def _():
            act(m * p.cpm + rest // p.sp)

    def service(seg):
        for d, role in ((0, role_a), (1, role_b)):
            def sums(i, d=d, role=role):
                mine, arrived, _ = chain(d, i)

                @pl.when(role > 0)
                def _():
                    rs_copy(d, i).wait_recv()

                @pl.when((role > 0) & (role < 3))
                def _():
                    mine[...] = mine[...] + arrived[...]

                @pl.when(role < 3)
                def _():
                    rs_copy(d, i).start()

                @pl.when(role == 3)
                def _():
                    k = lax.rem(i, p.cpm)

                    @pl.when(i >= p.cpm)
                    def _():
                        yl_copy(d, i - p.cpm).wait()
                        ag_copy(d, i - p.cpm, yst.at[d, k]).wait_send()

                    yst[d, k] = (mine[...] + arrived[...]).astype(jnp.bfloat16)
                    yl_copy(d, i).start()
                    ag_copy(d, i, yst.at[d, k]).start()

            when_due(seg, p.ob + p.od * role, sums)

        for d, role in ((0, role_a), (1, role_b)):
            def rows(i, d=d, role=role):
                @pl.when(role < 3)
                def _():
                    ag_copy(d, i).wait_recv()

                @pl.when((role < 3) & (role > 0))
                def _():
                    ag_copy(d, i).start()

            when_due(seg, p.ab + p.ad * (2 - role), rows)

    row_id = lax.broadcasted_iota(jnp.int32, (p.mr, 1), 0)
    mine_a = jnp.where(tp == 0, 1, 0)
    mine_b = jnp.where(tp == 3, 1, 0)
    take_x = jnp.where(row_id < p.half, mine_a, mine_b).astype(jnp.float32)

    def xb_copy(m):
        return pltpu.make_async_copy(x.at[pl.ds(pl.multiple_of(m * p.mr, p.mr), p.mr)], xb, b_sem.at[5])

    def segment(seg, _):
        m = seg // p.nseg
        s = lax.rem(seg, p.nseg)
        busy = m < p.nm
        rows = pl.ds(pl.multiple_of(m * p.mr, p.mr), p.mr)

        @pl.when(busy & (s < p.nq))
        def _():
            t = m * p.wt + s
            slot = lax.rem(t, p.slots)

            @pl.when(s == 0)
            def _():
                xb_copy(m).start()

            w_copy(t, 'q', slot).wait()
            a = jnp.dot(h[rows, :], w[slot], preferred_element_type=jnp.float32)
            a = a + bias[0:1, pl.ds(pl.multiple_of(wq_col(s), HEAD), p.wcols)]
            for k in range(QUAD):
                q[s, k * p.mr:(k + 1) * p.mr, :] = rotate(a[:, k * HEAD:(k + 1) * HEAD], rows).astype(jnp.bfloat16)
            w_start(t + p.slots)

        @pl.when(busy & (s == p.s_own))
        def _():
            own_segment(m)

        @pl.when(seg == p.s_near)
        def _():
            for c in cache_copies(across, partner, 1):
                c.wait_recv()
            for c in cache_copies(across, partner, 2):
                c.start()
            for k in (0, 2):
                for c in cache_copies(cp, partner, k):
                    c.wait_recv()

            @pl.when(lax.rem(cp, 2) == 1)
            def _():
                for c in new_copies(pl.multiple_of(p.tok * cp, p.tok), p.tok, partner, 0):
                    c.wait_recv()

        @pl.when(busy & (s >= p.s_near) & (s < p.s_far))
        def _():
            block_segment(s - p.s_near, near, lambda b: b * p.tok * cp)

        @pl.when((seg == p.s_far) & (cp >= 2))
        def _():
            got = pl.multiple_of(p.tok * (cp - 1), p.tok)
            for c in new_copies(got, p.tok, partner, 1):
                c.wait_recv()
            for c in new_copies(got, p.tok, partner, 2):
                c.start()
            for c in new_copies(got, p.tok, partner, 2):
                c.wait_recv()

        @pl.when(busy & (s >= p.s_far) & (s < p.s_fin) & (far > 0))
        def _():
            block_segment(s - p.s_far, far, lambda b: (1 + b) * p.tok)

        @pl.when(busy & (s == p.s_fin))
        def _():
            def finish(i, _):
                inv = 1.0 / jnp.sum(l_s[i], axis=0, keepdims=True)
                v = o_t[i] * inv
                for k in range(QUAD):
                    o[:, pl.ds(pl.multiple_of((i * QUAD + k) * HEAD, HEAD), HEAD)] = v[:, k * p.mr:(k + 1) * p.mr].T.astype(jnp.bfloat16)
                return reset(i, 0)

            lax.fori_loop(0, p.nq, finish, 0)

        @pl.when(busy & (s >= p.s_out))
        def _():
            n = s - p.s_out
            t = m * p.wt + p.nq + n
            slot = lax.rem(t, p.slots)

            @pl.when(n == 0)
            def _():
                xb_copy(m).wait()

            @pl.when((n == 0) & (m >= p.owns))
            def _():
                for d, role in ((0, role_a), (1, role_b)):
                    @pl.when(role < 3)
                    def _():
                        for j in range(p.cpm):
                            rs_copy(d, (m - p.owns) * p.cpm + j).wait_send()

            w_copy(t, 'o', slot).wait()
            a = jnp.dot(o[...], w[slot, pl.ds(0, p.heads * HEAD), :], preferred_element_type=jnp.float32)
            a = a + xb[:, pl.ds(pl.multiple_of(n * p.wcols, HEAD), p.wcols)].astype(jnp.float32) * take_x
            per = p.nt // p.cpm
            own[lax.rem(m, p.owns), n // per, :, pl.ds(pl.multiple_of(lax.rem(n, per) * p.wcols, HEAD), p.wcols)] = a
            w_start(t + p.slots)

        service(seg)
        return 0

    lax.fori_loop(0, p.total, segment, 0)

    for d, role in ((0, role_a), (1, role_b)):
        @pl.when(role < 3)
        def _():
            def last_sums(i, _):
                rs_copy(d, i).wait_send()
                return 0
            lax.fori_loop((p.nm - p.owns) * p.cpm, p.chunks, last_sums, 0)

        @pl.when((role > 0) & (role < 3))
        def _():
            def last_rows(i, _):
                ag_copy(d, i).wait_send()
                return 0
            lax.fori_loop(0, p.chunks, last_rows, 0)

        @pl.when(role == 3)
        def _():
            for k in range(p.cpm):
                i = p.chunks - p.cpm + k
                yl_copy(d, i).wait()
                ag_copy(d, i, yst.at[d, k]).wait_send()

    for c in out_copies():
        c.wait()
    for k in (0, 1):
        for c in cache_copies(cp, partner, k):
            c.wait_send()
    for c in cache_copies(across, partner, 2):
        c.wait_send()

    @pl.when(cp < 2)
    def _():
        for c in new_copies(new0, p.tok, across, 1):
            c.wait_send()

    @pl.when(lax.rem(cp, 2) == 0)
    def _():
        for c in new_copies(new0, p.tok, partner, 0):
            c.wait_send()

    @pl.when(cp >= 2)
    def _():
        for c in new_copies(pl.multiple_of(p.tok * (cp - 1), p.tok), p.tok, partner, 2):
            c.wait_send()


def build(p):
    def local_step(x, k_cache, v_cache, rope_table, norm_gain, w_qkv, b_qkv, w_out):
        pairs = rope_table.shape[1] // 2
        cos = jnp.repeat(rope_table[:, :pairs], 2, axis=1)
        sin = jnp.repeat(rope_table[:, pairs:], 2, axis=1) * jnp.tile(jnp.array([-1.0, 1.0], jnp.float32), pairs)
        fill = jnp.zeros((p.tok, HEAD - 2 * pairs), jnp.float32)
        rope = jnp.concatenate([cos, fill, sin, fill], axis=1)
        anyspace = pl.BlockSpec(memory_space=pl.ANY)
        vmem = pl.BlockSpec(memory_space=pltpu.VMEM)
        bf, f32 = jnp.bfloat16, jnp.float32
        dma = pltpu.SemaphoreType.DMA
        kvw = p.kv * HEAD
        y, kn, vn = pl.pallas_call(
            functools.partial(kernel, p),
            name='block',
            out_shape=(jax.ShapeDtypeStruct((p.tok, p.dim), bf), jax.ShapeDtypeStruct((p.tok, kvw), bf), jax.ShapeDtypeStruct((p.tok, kvw), bf)),
            in_specs=[anyspace, anyspace, anyspace, anyspace, vmem, vmem, anyspace, anyspace],
            out_specs=(anyspace, anyspace, anyspace),
            scratch_shapes=[
                pltpu.VMEM((p.tok, p.dim), bf),
                pltpu.VMEM((p.kv, p.keys, HEAD), bf),
                pltpu.VMEM((p.kv, HEAD, p.keys), bf),
                pltpu.VMEM((p.tok, 2 * HEAD), f32),
                pltpu.VMEM((p.nq, p.n, HEAD), bf),
                pltpu.VMEM((p.nq, HEAD, p.n), f32),
                pltpu.VMEM((p.mr, p.heads * HEAD), bf),
                pltpu.VMEM((p.kt, p.n), f32),
                pltpu.VMEM((p.kt, p.n), f32),
                pltpu.VMEM((p.kt, p.n), bf),
                pltpu.VMEM((8, p.n), f32),
                pltpu.VMEM((8, p.n), f32),
                pltpu.VMEM((p.nq, 8, p.n), f32),
                pltpu.VMEM((p.nq, 8, p.n), f32),
                pltpu.VMEM((p.owns, p.cpm, p.mr, p.cc), f32),
                pltpu.VMEM((2, p.chunks, p.half, p.cc), f32),
                pltpu.VMEM((2, p.cpm, p.half, p.cc), bf),
                pltpu.VMEM((p.mr, p.dim), bf),
                pltpu.VMEM((p.slots, p.dim, p.wcols), bf),
                pltpu.VMEM((p.kv, p.tok, HEAD), bf),
                dma((4,)), dma((p.slots,)), dma((6,)), dma((2 * p.kv,)),
                dma((3, 2)), dma((3, 2)), dma((3, 2)), dma((3, 2)),
                dma((2, p.chunks)), dma((2, p.chunks)), dma((2, p.chunks)), dma((2, p.chunks)), dma((2, p.cpm)),
            ],
            compiler_params=pltpu.CompilerParams(collective_id=0, has_side_effects=True, vmem_limit_bytes=66_000_000),
        )(x, k_cache.transpose(1, 0, 2), v_cache.transpose(1, 2, 0), rope, norm_gain.astype(f32).reshape(1, p.dim),
          b_qkv.astype(f32).reshape(1, -1), w_qkv, w_out)
        shape = (p.tok, p.kv, HEAD)
        return y, kn.reshape(shape), vn.reshape(shape)

    return local_step


def solution(mesh):
    row_spec = P(('dp', 'cp'), None)
    cache_spec = P(('dp', 'cp'), 'tp', None)
    p = Plan(tok=1024, dim=4096, kv=2, group=12, cache=256, nm=8, kt=512)
    return jax.shard_map(build(p), mesh=mesh, in_specs=(row_spec, cache_spec, cache_spec, row_spec, P(None), P(None, 'tp'), P('tp'), P('tp', None)),
                         out_specs=(row_spec, cache_spec, cache_spec), check_vma=False)
```

```python
import functools
import math

import jax
import jax.numpy as jnp
from jax import lax
from jax.experimental import pallas as pl
from jax.experimental.pallas import tpu as pltpu
from jax.sharding import PartitionSpec as P

EPS = 1.5625e-07
LOW = -1e30
HEAD = 128
QUAD = 4
MESH = pl.DeviceIdType.MESH


class Plan:
    def __init__(self, tok, dim, kv, group, cache, nm, kt):
        self.tok, self.dim, self.kv, self.group, self.cache = tok, dim, kv, group, cache
        self.nm = nm
        self.mr = tok // nm
        self.np = nm // 2
        self.kt = kt
        self.nq = kv * group // QUAD
        self.qpg = group // QUAD
        self.hp = self.nq // 2
        self.n = QUAD * self.mr
        self.keys = tok * 5
        self.heads = kv * group
        self.wcols = QUAD * HEAD
        self.nt = dim // self.wcols
        self.cpm = 4
        self.per = self.nt // self.cpm
        self.cc = dim // self.cpm
        self.half = self.mr // 2
        self.owns = 2
        self.s_near = self.hp
        self.s_far = self.s_near + self.hp
        self.s_fin = self.s_far + self.hp
        self.s_out = self.s_fin + 1
        self.s_q = self.s_out + self.nt
        self.nseg = self.s_q + self.hp
        self.chunks = nm * self.cpm
        self.table([[self.s_out + self.per * (j + 1) - 1 + 3 * r for j in range(self.cpm)] for r in range(4)],
                   [[self.s_out + self.per * (j + 1) - 1 + 12 + 3 * r for j in range(self.cpm)] for r in range(3)])

    def table(self, sums, rows):
        self.sums, self.rows = sums, rows
        self.total = self.nseg * (self.nm - 1) + max(max(r) for r in sums + rows) + 1

def kernel(p, x, cache_in, rope_in, small, wqkv, wout, y, kn, vn, land,
           h, ka, vt, rope, q, o_t, o, s_a, s_b, p_s, mx_a, mx_b, m_s, l_s, own, stage, yst, xb, w, wo, vb,
           x_sem, w_sem, wo_sem, b_sem, out_sem, cs_send, cs_recv, kv_send, kv_recv,
           rs_send, rs_recv, st_sem, ag_send, ag_recv, yl_sem):
    tp = lax.axis_index('tp')
    cp = lax.axis_index('cp')
    partner = cp + 1 - 2 * lax.rem(cp, 2)
    across = lax.rem(cp + 2, 4)
    scale = HEAD ** -0.5 * math.log2(math.e)
    new0 = p.tok * (1 + cp)
    rows4 = p.tok // 4
    goff = (p.group + 2) * HEAD * p.kv

    def wq_col(j):
        return (j // p.qpg) * (p.group + 2) * HEAD + lax.rem(j, p.qpg) * p.wcols

    def wq_copy(t):
        slot = lax.rem(t, 2)
        col = pl.multiple_of(wq_col(lax.rem(t, p.nq)), HEAD)
        return pltpu.make_async_copy(wqkv.at[:, pl.ds(col, p.wcols)], w.at[slot], w_sem.at[slot])

    def wo_copy(n):
        return pltpu.make_async_copy(wout.at[:, pl.ds(pl.multiple_of(n * p.wcols, HEAD), p.wcols)], wo.at[n], wo_sem.at[n])

    def x_copy(r):
        rows = pl.ds(r * rows4, rows4)
        return pltpu.make_async_copy(x.at[rows], h.at[rows], x_sem.at[r])

    def wkv_copy(g):
        col = g * (p.group + 2) * HEAD + p.group * HEAD
        return pltpu.make_async_copy(wqkv.at[:, pl.ds(col, 2 * HEAD)], w.at[1, :, pl.ds(g * 2 * HEAD, 2 * HEAD)], b_sem.at[g])

    x_copy(0).start()
    for g in range(p.kv):
        wkv_copy(g).start()
    kc_copy = pltpu.make_async_copy(cache_in.at[0], ka.at[:, pl.ds(cp * p.cache, p.cache)], b_sem.at[3])
    vc_copy = pltpu.make_async_copy(cache_in.at[1], vb.at[:, pl.ds(0, p.cache)], b_sem.at[4])
    kc_copy.start()
    vc_copy.start()
    rope_copy = pltpu.make_async_copy(rope_in, rope, b_sem.at[2])
    rope_copy.start()
    for r in range(1, 4):
        x_copy(r).start()
    wq_copy(0).start()

    barrier = pltpu.get_barrier_semaphore()
    for k in range(1, 4):
        pl.semaphore_signal(barrier, inc=1, device_id={'tp': lax.rem(tp + k, 4)}, device_id_type=MESH)
        pl.semaphore_signal(barrier, inc=1, device_id={'cp': lax.rem(cp + k, 4)}, device_id_type=MESH)

    def cache_copies(owner, peer, k):
        at = pl.multiple_of(owner * p.cache, p.cache)
        ks = ka.at[:, pl.ds(at, p.cache)]
        vs = vt.at[:, :, pl.ds(at, p.cache)]
        return (pltpu.make_async_remote_copy(ks, ks, cs_send.at[k, 0], cs_recv.at[k, 0], device_id={'cp': peer}, device_id_type=MESH),
                pltpu.make_async_remote_copy(vs, vs, cs_send.at[k, 1], cs_recv.at[k, 1], device_id={'cp': peer}, device_id_type=MESH))

    def new_copies(at, size, peer, k):
        ks = ka.at[:, pl.ds(at, size)]
        vs = vt.at[:, :, pl.ds(at, size)]
        return (pltpu.make_async_remote_copy(ks, ks, kv_send.at[k, 0], kv_recv.at[k, 0], device_id={'cp': peer}, device_id_type=MESH),
                pltpu.make_async_remote_copy(vs, vs, kv_send.at[k, 1], kv_recv.at[k, 1], device_id={'cp': peer}, device_id_type=MESH))

    vc_copy.wait()
    for g in range(p.kv):
        vt[g, :, pl.ds(pl.multiple_of(cp * p.cache, p.cache), p.cache)] = vb[g, 0:p.cache, :].astype(jnp.float32).T.astype(jnp.bfloat16)
    kc_copy.wait()
    pl.semaphore_wait(barrier, 6)
    for peer, k in ((across, 1), (partner, 0)):
        for c in cache_copies(cp, peer, k):
            c.start()

    def send_new(r):
        at = pl.multiple_of(new0 + r * rows4, rows4)

        @pl.when(cp < 2)
        def _():
            for c in new_copies(at, rows4, across, 1):
                c.start()

        @pl.when(lax.rem(cp, 2) == 0)
        def _():
            for c in new_copies(at, rows4, partner, 0):
                c.start()

    lane = lax.broadcasted_iota(jnp.int32, (1, HEAD), 1)
    even = lax.rem(lane, 2) == 0
    turned = lane < 64

    def angles(rows, count):
        r = rope[rows, :]
        both = jnp.concatenate([r, r], axis=1)
        at = lax.broadcasted_iota(jnp.int32, (count, HEAD), 1)
        pair = lax.rem(at, 64) // 2
        c = jnp.take_along_axis(both, pair, axis=1)
        s = jnp.take_along_axis(both, pair + 32, axis=1)
        return c, jnp.where(even, -s, s)

    def rotate(a, c, s):
        swap = jnp.where(even, pltpu.roll(a, HEAD - 1, 1), pltpu.roll(a, 1, 1))
        return jnp.where(turned, a * c + swap * s, a)

    rope_copy.wait()
    for g in range(p.kv):
        wkv_copy(g).wait()
    nsub = max(1, rows4 // 64)
    sub = rows4 // nsub

    def kv_step(r, _):
        x_copy(r).wait()

        @pl.when(r > 0)
        def _():
            send_new(r - 1)

        def norm(b, _):
            rows = pl.ds(pl.multiple_of(r * rows4 + b * sub, sub), sub)
            v = h[rows, :].astype(jnp.float32)
            inv = lax.rsqrt(jnp.mean(v * v, axis=1, keepdims=True) + EPS)
            h[rows, :] = (v * inv * small[0:1, goff:goff + p.dim]).astype(jnp.bfloat16)
            return 0

        lax.fori_loop(0, nsub, norm, 0)
        rows = pl.ds(pl.multiple_of(r * rows4, rows4), rows4)
        at = pl.multiple_of(new0 + r * rows4, rows4)
        a = jnp.dot(h[rows, :], w[1], preferred_element_type=jnp.float32)
        c, s = angles(rows, rows4)
        for g in range(p.kv):
            col = g * (p.group + 2) * HEAD + p.group * HEAD
            key = rotate(a[:, g * 2 * HEAD:g * 2 * HEAD + HEAD] + small[0:1, col:col + HEAD], c, s)
            val = a[:, g * 2 * HEAD + HEAD:(g + 1) * 2 * HEAD] + small[0:1, col + HEAD:col + 2 * HEAD]
            ka[g, pl.ds(at, rows4), :] = key.astype(jnp.bfloat16)
            vb[g, rows, :] = val.astype(jnp.bfloat16)
            vt[g, :, pl.ds(at, rows4)] = val.T.astype(jnp.bfloat16)
        return 0

    lax.fori_loop(0, 4, kv_step, 0)
    send_new(3)
    wq_copy(1).start()

    def out_copies():
        res = []
        for g in range(p.kv):
            cols = pl.ds(g * HEAD, HEAD)
            res.append(pltpu.make_async_copy(ka.at[g, pl.ds(new0, p.tok)], kn.at[:, cols], out_sem.at[g]))
            res.append(pltpu.make_async_copy(vb.at[g], vn.at[:, cols], out_sem.at[p.kv + g]))
        return res

    for c in out_copies():
        c.start()

    def reset(i, _):
        m_s[i] = jnp.full((8, p.n), LOW, jnp.float32)
        l_s[i] = jnp.zeros((8, p.n), jnp.float32)
        o_t[i] = jnp.zeros((HEAD, p.n), jnp.float32)
        return 0

    lax.fori_loop(0, p.nq, reset, 0)

    def q_tile(t):
        pair = t // p.nq
        j = lax.rem(t, p.nq)
        rows = pl.ds(pl.multiple_of(pair * 2 * p.mr, 2 * p.mr), 2 * p.mr)
        wq_copy(t).wait()
        a = jnp.dot(h[rows, :], w[lax.rem(t, 2)], preferred_element_type=jnp.float32)
        a = a + small[0:1, pl.ds(pl.multiple_of(wq_col(j), HEAD), p.wcols)]
        c, s = angles(rows, 2 * p.mr)
        for k in range(QUAD):
            b = rotate(a[:, k * HEAD:(k + 1) * HEAD], c, s).astype(jnp.bfloat16)
            for u in range(2):
                q[2 * lax.rem(pair, 2) + u, j, k * p.mr:(k + 1) * p.mr, :] = b[u * p.mr:(u + 1) * p.mr, :]

        @pl.when(t + 2 < p.np * p.nq)
        def _():
            wq_copy(t + 2).start()

    sb = min(256, p.kt)
    ss = min(128, p.kt)
    pk = min(256, p.kt)

    def scores(qs, hq, off, kk, s_ref, mx, bound):
        g = hq // p.qpg
        s = lax.dot_general(ka[g, pl.ds(pl.multiple_of(off + kk, sb), sb), :], q[qs, hq], (((1,), (1,)), ((), ())),
                            preferred_element_type=jnp.float32) * scale
        if bound is not None:
            row = lax.rem(lax.broadcasted_iota(jnp.int32, (sb, p.n), 1), p.mr)
            key = lax.broadcasted_iota(jnp.int32, (sb, p.n), 0)
            s = jnp.where(row - key >= kk - bound, s, LOW)
        s_ref[kk:kk + sb, :] = s
        top = jnp.max(s.reshape(sb // 8, 8, p.n), axis=0)
        return top if mx is None else jnp.maximum(mx, top)

    def all_scores(qs, hq, off, s_ref, mx_ref, bound):
        mx = None
        for kk in range(0, p.kt, sb):
            mx = scores(qs, hq, off, kk, s_ref, mx, bound)
        mx_ref[...] = mx

    def tile(qs, hq, off, s_ref, mx_ref, hq_n, off_n, s_next, mx_next, bound_n):
        g = hq // p.qpg
        m_old = m_s[hq, 0:1, :]
        m_new = jnp.maximum(m_old, jnp.max(mx_ref[...], axis=0, keepdims=True))
        alpha = jnp.exp2(m_old - m_new)
        m_s[hq, 0:1, :] = m_new
        mx = acc = out = None
        for kk in range(0, p.kt, pk):
            for k2 in range(kk, kk + pk, sb):
                mx = scores(qs, hq_n, off_n, k2, s_next, mx, bound_n)
            for k2 in range(kk, kk + pk, ss):
                e = jnp.exp2(s_ref[k2:k2 + ss, :] - m_new)
                part = jnp.sum(e.reshape(ss // 8, 8, p.n), axis=0)
                acc = part if acc is None else acc + part
                p_s[k2:k2 + ss, :] = e.astype(jnp.bfloat16)
            d = jnp.dot(vt[g, :, pl.ds(pl.multiple_of(off + kk, pk), pk)], p_s[kk:kk + pk, :], preferred_element_type=jnp.float32)
            out = d if out is None else out + d
        mx_next[...] = mx
        l_s[hq] = l_s[hq] * alpha + acc
        o_t[hq] = o_t[hq] * alpha + out

    def own_segment(u, i):
        qs = lax.rem(u, 4)
        tiles = (u * p.mr + p.mr + p.kt - 1) // p.kt
        h0 = 2 * i

        def bound(j):
            return u * p.mr - j * p.kt

        @pl.when(i == 0)
        def _():
            all_scores(qs, 0, new0, s_a, mx_a, bound(0))

        def step(j, _):
            more = j + 1 < tiles
            hn = jnp.where(more, h0, jnp.minimum(h0 + 2, p.nq - 2))
            jn = jnp.where(more, j + 1, 0)
            off = new0 + j * p.kt
            tile(qs, h0, off, s_a, mx_a, h0 + 1, off, s_b, mx_b, bound(j))
            tile(qs, h0 + 1, off, s_b, mx_b, hn, new0 + jn * p.kt, s_a, mx_a, bound(jn))
            return 0

        lax.fori_loop(0, tiles, step, 0)

    def block_segment(u, i, count, offset):
        qs = lax.rem(u, 4)
        h0 = 2 * i

        @pl.when(i == 0)
        def _():
            all_scores(qs, 0, offset(0), s_a, mx_a, None)

        def step(b, _):
            off = offset(b)
            more = b + 1 < count
            hn = jnp.where(more, h0, jnp.minimum(h0 + 2, p.nq - 2))
            on = offset(jnp.where(more, b + 1, 0))
            tile(qs, h0, off, s_a, mx_a, h0, off + p.kt, s_b, mx_b, None)
            tile(qs, h0, off + p.kt, s_b, mx_b, h0 + 1, off, s_a, mx_a, None)
            tile(qs, h0 + 1, off, s_a, mx_a, h0 + 1, off + p.kt, s_b, mx_b, None)
            tile(qs, h0 + 1, off + p.kt, s_b, mx_b, hn, on, s_a, mx_a, None)
            return 0

        lax.fori_loop(0, count, step, 0)

    near = 1 + lax.rem(cp, 2)
    far = 2 * (cp // 2)

    role_a = 3 - tp
    role_b = tp

    def chain(d, i):
        m = i // p.cpm
        j = lax.rem(i, p.cpm)
        mine = own.at[lax.rem(m, p.owns), j, pl.ds(d * p.half, p.half)]
        rows = pl.ds(pl.multiple_of(m * p.mr + d * p.half, p.half), p.half)
        cols = pl.ds(pl.multiple_of(j * p.cc, p.cc), p.cc)
        return mine, land.at[d, i], y.at[rows, cols]

    def peers(d):
        return (jnp.maximum(tp - 1, 0), jnp.minimum(tp + 1, 3)) if d == 0 else (jnp.minimum(tp + 1, 3), jnp.maximum(tp - 1, 0))

    def rs_copy(d, i):
        mine, there, _ = chain(d, i)
        return pltpu.make_async_remote_copy(mine, there, rs_send.at[d, i], rs_recv.at[d, i], device_id={'tp': peers(d)[0]}, device_id_type=MESH)

    def st_copy(d, i):
        k = lax.rem(i, 2)
        return pltpu.make_async_copy(land.at[d, i], stage.at[d, k], st_sem.at[d, k])

    def ag_copy(d, i, src=None):
        out = chain(d, i)[2]
        return pltpu.make_async_remote_copy(out if src is None else src, out, ag_send.at[d, i], ag_recv.at[d, i],
                                            device_id={'tp': peers(d)[1]}, device_id_type=MESH)

    def yl_copy(d, i):
        k = lax.rem(i, p.cpm)
        return pltpu.make_async_copy(yst.at[d, k], chain(d, i)[2], yl_sem.at[d, k])

    def pick(role, table, j):
        v = table[0][j]
        for r in range(1, len(table)):
            v = jnp.where(role == r, table[r][j], v)
        return v

    def when_due(seg, role, table, ahead, act):
        hit = seg < 0
        i = 0
        for j in range(p.cpm):
            t = seg + ahead - pick(role, table, j)
            m = jnp.maximum(t, 0) // p.nseg
            due = (t >= 0) & (m < p.nm) & (lax.rem(jnp.maximum(t, 0), p.nseg) == 0)
            hit = hit | due
            i = i + jnp.where(due, m * p.cpm + j, 0)

        @pl.when(hit)
        def _():
            act(i)

    def service(seg):
        for d, role in ((0, role_a), (1, role_b)):
            def sums(i, d=d, role=role):
                mine = chain(d, i)[0]
                arrived = stage.at[d, lax.rem(i, 2)]

                @pl.when(role > 0)
                def _():
                    st_copy(d, i).wait()

                @pl.when((role > 0) & (role < 3))
                def _():
                    mine[...] = mine[...] + arrived[...]

                @pl.when(role < 3)
                def _():
                    rs_copy(d, i).start()

                @pl.when(role == 3)
                def _():
                    k = lax.rem(i, p.cpm)

                    @pl.when(i >= p.cpm)
                    def _():
                        yl_copy(d, i - p.cpm).wait()
                        ag_copy(d, i - p.cpm, yst.at[d, k]).wait_send()

                    yst[d, k] = (mine[...] + arrived[...]).astype(jnp.bfloat16)
                    yl_copy(d, i).start()
                    ag_copy(d, i, yst.at[d, k]).start()

            when_due(seg, role, p.sums, 0, sums)

        for d, role in ((0, role_a), (1, role_b)):
            def rows(i, d=d, role=role):
                @pl.when(role < 3)
                def _():
                    ag_copy(d, i).wait_recv()

                @pl.when((role < 3) & (role > 0))
                def _():
                    ag_copy(d, i).start()

            when_due(seg, 2 - role, p.rows, 0, rows)

        for d, role in ((0, role_a), (1, role_b)):
            def fetch(i, d=d, role=role):
                @pl.when(role > 0)
                def _():
                    rs_copy(d, i).wait_recv()
                    st_copy(d, i).start()

            when_due(seg, role, p.sums, 1, fetch)

    row_id = lax.broadcasted_iota(jnp.int32, (p.mr, 1), 0)
    mine_a = jnp.where(tp == 0, 1, 0)
    mine_b = jnp.where(tp == 3, 1, 0)
    take_x = jnp.where(row_id < p.half, mine_a, mine_b).astype(jnp.float32)

    def xb_copy(m):
        return pltpu.make_async_copy(x.at[pl.ds(pl.multiple_of(m * p.mr, p.mr), p.mr)], xb, b_sem.at[5])

    def first_q(t, _):
        q_tile(t)

        @pl.when(t == max(0, p.nq - 3))
        def _():
            for n in range(p.nt):
                wo_copy(n).start()

        return 0

    lax.fori_loop(0, p.nq, first_q, 0)

    def segment(seg, _):
        m = seg // p.nseg
        s = lax.rem(seg, p.nseg)
        busy = m < p.nm

        @pl.when(busy & (s < p.s_near))
        def _():
            @pl.when(s == 0)
            def _():
                xb_copy(m).start()

            own_segment(m, s)

        @pl.when(seg == p.s_near)
        def _():
            for c in cache_copies(across, partner, 1):
                c.wait_recv()
            for c in cache_copies(across, partner, 2):
                c.start()
            for k in (0, 2):
                for c in cache_copies(cp, partner, k):
                    c.wait_recv()

            @pl.when(lax.rem(cp, 2) == 1)
            def _():
                for c in new_copies(pl.multiple_of(p.tok * cp, p.tok), p.tok, partner, 0):
                    c.wait_recv()

        @pl.when(busy & (s >= p.s_near) & (s < p.s_far))
        def _():
            block_segment(m, s - p.s_near, near, lambda b: b * p.tok * cp)

        @pl.when((seg == p.s_far) & (cp >= 2))
        def _():
            got = pl.multiple_of(p.tok * (cp - 1), p.tok)
            for c in new_copies(got, p.tok, partner, 1):
                c.wait_recv()
            for c in new_copies(got, p.tok, partner, 2):
                c.start()
            for c in new_copies(got, p.tok, partner, 2):
                c.wait_recv()

        @pl.when(busy & (s >= p.s_far) & (s < p.s_fin) & (far > 0))
        def _():
            block_segment(m, s - p.s_far, far, lambda b: (1 + b) * p.tok)

        @pl.when(busy & (s == p.s_fin))
        def _():
            def finish(i, _):
                inv = 1.0 / jnp.sum(l_s[i], axis=0, keepdims=True)
                v = o_t[i] * inv
                for k in range(QUAD):
                    o[:, pl.ds(pl.multiple_of((i * QUAD + k) * HEAD, HEAD), HEAD)] = v[:, k * p.mr:(k + 1) * p.mr].T.astype(jnp.bfloat16)
                return reset(i, 0)

            lax.fori_loop(0, p.nq, finish, 0)

        @pl.when(busy & (s >= p.s_out) & (s < p.s_q))
        def _():
            n = s - p.s_out

            @pl.when(n == 0)
            def _():
                xb_copy(m).wait()

            @pl.when((n == 0) & (m >= p.owns))
            def _():
                for d, role in ((0, role_a), (1, role_b)):
                    @pl.when(role < 3)
                    def _():
                        for j in range(p.cpm):
                            rs_copy(d, (m - p.owns) * p.cpm + j).wait_send()

            @pl.when(m == 0)
            def _():
                wo_copy(n).wait()

            a = jnp.dot(o[...], wo[n], preferred_element_type=jnp.float32)
            a = a + xb[:, pl.ds(pl.multiple_of(n * p.wcols, HEAD), p.wcols)].astype(jnp.float32) * take_x
            own[lax.rem(m, p.owns), n // p.per, :, pl.ds(pl.multiple_of(lax.rem(n, p.per) * p.wcols, HEAD), p.wcols)] = a

        @pl.when((m // 2 + 1 < p.np) & (s >= p.s_q))
        def _():
            q_tile((m // 2 + 1) * p.nq + lax.rem(m, 2) * p.hp + s - p.s_q)

        service(seg)
        return 0

    lax.fori_loop(0, p.total, segment, 0)

    for d, role in ((0, role_a), (1, role_b)):
        @pl.when(role < 3)
        def _():
            def last_sums(i, _):
                rs_copy(d, i).wait_send()
                return 0
            lax.fori_loop((p.nm - p.owns) * p.cpm, p.chunks, last_sums, 0)

        @pl.when((role > 0) & (role < 3))
        def _():
            def last_rows(i, _):
                ag_copy(d, i).wait_send()
                return 0
            lax.fori_loop(0, p.chunks, last_rows, 0)

        @pl.when(role == 3)
        def _():
            for k in range(p.cpm):
                i = p.chunks - p.cpm + k
                yl_copy(d, i).wait()
                ag_copy(d, i, yst.at[d, k]).wait_send()

    for c in out_copies():
        c.wait()
    for k in (0, 1):
        for c in cache_copies(cp, partner, k):
            c.wait_send()
    for c in cache_copies(across, partner, 2):
        c.wait_send()

    @pl.when(cp < 2)
    def _():
        for c in new_copies(new0, p.tok, across, 1):
            c.wait_send()

    @pl.when(lax.rem(cp, 2) == 0)
    def _():
        for c in new_copies(new0, p.tok, partner, 0):
            c.wait_send()

    @pl.when(cp >= 2)
    def _():
        for c in new_copies(pl.multiple_of(p.tok * (cp - 1), p.tok), p.tok, partner, 2):
            c.wait_send()


def build(p):
    def local_step(x, k_cache, v_cache, rope_table, norm_gain, w_qkv, b_qkv, w_out):
        small = jnp.concatenate([b_qkv, norm_gain]).astype(jnp.float32).reshape(1, -1)
        cached = jnp.stack([k_cache, v_cache]).transpose(0, 2, 1, 3)
        anyspace = pl.BlockSpec(memory_space=pl.ANY)
        vmem = pl.BlockSpec(memory_space=pltpu.VMEM)
        bf, f32 = jnp.bfloat16, jnp.float32
        dma = pltpu.SemaphoreType.DMA
        kvw = p.kv * HEAD
        y, kn, vn, _ = pl.pallas_call(
            functools.partial(kernel, p),
            name='block',
            out_shape=(jax.ShapeDtypeStruct((p.tok, p.dim), bf), jax.ShapeDtypeStruct((p.tok, kvw), bf), jax.ShapeDtypeStruct((p.tok, kvw), bf),
                       jax.ShapeDtypeStruct((2, p.chunks, p.half, p.cc), f32)),
            in_specs=[anyspace, anyspace, anyspace, vmem, anyspace, anyspace],
            out_specs=(anyspace, anyspace, anyspace, anyspace),
            scratch_shapes=[
                pltpu.VMEM((p.tok, p.dim), bf),
                pltpu.VMEM((p.kv, p.keys, HEAD), bf),
                pltpu.VMEM((p.kv, HEAD, p.keys), bf),
                pltpu.VMEM((p.tok, 64), f32),
                pltpu.VMEM((4, p.nq, p.n, HEAD), bf),
                pltpu.VMEM((p.nq, HEAD, p.n), f32),
                pltpu.VMEM((p.mr, p.heads * HEAD), bf),
                pltpu.VMEM((p.kt, p.n), f32),
                pltpu.VMEM((p.kt, p.n), f32),
                pltpu.VMEM((p.kt, p.n), bf),
                pltpu.VMEM((8, p.n), f32),
                pltpu.VMEM((8, p.n), f32),
                pltpu.VMEM((p.nq, 8, p.n), f32),
                pltpu.VMEM((p.nq, 8, p.n), f32),
                pltpu.VMEM((p.owns, p.cpm, p.mr, p.cc), f32),
                pltpu.VMEM((2, 2, p.half, p.cc), f32),
                pltpu.VMEM((2, p.cpm, p.half, p.cc), bf),
                pltpu.VMEM((p.mr, p.dim), bf),
                pltpu.VMEM((2, p.dim, p.wcols), bf),
                pltpu.VMEM((p.nt, p.heads * HEAD, p.wcols), bf),
                pltpu.VMEM((p.kv, p.tok, HEAD), bf),
                dma((4,)), dma((2,)), dma((p.nt,)), dma((6,)), dma((2 * p.kv,)),
                dma((3, 2)), dma((3, 2)), dma((3, 2)), dma((3, 2)),
                dma((2, p.chunks)), dma((2, p.chunks)), dma((2, 2)), dma((2, p.chunks)), dma((2, p.chunks)), dma((2, p.cpm)),
            ],
            compiler_params=pltpu.CompilerParams(collective_id=0, has_side_effects=True, vmem_limit_bytes=67_000_000),
        )(x, cached, rope_table, small, w_qkv, w_out)
        shape = (p.tok, p.kv, HEAD)
        return y, kn.reshape(shape), vn.reshape(shape)

    return local_step


def solution(mesh):
    row_spec = P(('dp', 'cp'), None)
    cache_spec = P(('dp', 'cp'), 'tp', None)
    p = Plan(tok=1024, dim=4096, kv=2, group=12, cache=256, nm=8, kt=512)
    p.table([[11, 19, 22, 24], [21, 25, 28, 32], [26, 29, 37, 43], [37, 43, 45, 47]],
            [[45, 48, 53, 59], [48, 56, 65, 66], [64, 69, 71, 74]])
    return jax.shard_map(build(p), mesh=mesh, in_specs=(row_spec, cache_spec, cache_spec, row_spec, P(None), P(None, 'tp'), P('tp'), P('tp', None)),
                         out_specs=(row_spec, cache_spec, cache_spec), check_vma=False)
```

```python
import functools
import math

import jax
import jax.numpy as jnp
from jax import lax
from jax.experimental import pallas as pl
from jax.experimental.pallas import tpu as pltpu
from jax.sharding import PartitionSpec as P

EPS = 1.5625e-07
LOW = -1e30
HEAD = 128
QUAD = 4
MESH = pl.DeviceIdType.MESH


class Plan:
    def __init__(self, tok, dim, kv, group, cache, nm, kt):
        self.tok, self.dim, self.kv, self.group, self.cache = tok, dim, kv, group, cache
        self.nm = nm
        self.mr = tok // nm
        self.kt = kt
        self.heads = kv * group
        self.nd = self.heads // 2
        self.dpg = group // 2
        self.n = 2 * self.mr
        self.keys = tok * 5
        self.wcols = QUAD * HEAD
        self.nq = self.heads // QUAD
        self.qpg = group // QUAD
        self.hq = self.nq // 2
        self.nt = dim // self.wcols
        self.cpm = 4
        self.per = self.nt // self.cpm
        self.cc = dim // self.cpm
        self.half = self.mr // 2
        self.owns = 2
        self.look = 3
        self.wt = self.nq * (2 + nm // 2 - 1)
        self.s_blk = 2
        self.s_fin = self.s_blk + 4
        self.s_out = self.s_fin + 1
        self.s_q = self.s_out + self.nt
        self.nseg = self.s_q + self.hq
        self.chunks = nm * self.cpm
        self.table([[self.s_out + self.per * (j + 1) - 1 + 3 * r for j in range(self.cpm)] for r in range(4)],
                   [[self.s_out + self.per * (j + 1) - 1 + 12 + 3 * r for j in range(self.cpm)] for r in range(3)])

    def table(self, sums, rows):
        self.sums, self.rows = sums, rows
        self.total = self.nseg * (self.nm - 1) + max(max(r) for r in sums + rows) + 1

def kernel(p, x, cache_in, rope_in, small, wqkv, wout, y, kn, vn, land,
           h, ka, vt, rope, q, o_t, o, s_t, mx_t, m_s, l_s, own, stage, yst, xb, w, wo, vb,
           x_sem, w_sem, wo_sem, b_sem, out_sem, cs_send, cs_recv, kv_send, kv_recv,
           rs_send, rs_recv, st_sem, ag_send, ag_recv, yl_sem):
    tp = lax.axis_index('tp')
    cp = lax.axis_index('cp')
    partner = cp + 1 - 2 * lax.rem(cp, 2)
    across = lax.rem(cp + 2, 4)
    scale = HEAD ** -0.5 * math.log2(math.e)
    new0 = p.tok * (1 + cp)
    rows4 = p.tok // 4
    goff = (p.group + 2) * HEAD * p.kv

    def wq_col(j):
        return (j // p.qpg) * (p.group + 2) * HEAD + lax.rem(j, p.qpg) * p.wcols

    def wq_copy(t):
        slot = lax.rem(t, 2)
        col = pl.multiple_of(wq_col(lax.rem(t, p.nq)), HEAD)
        return pltpu.make_async_copy(wqkv.at[:, pl.ds(col, p.wcols)], w.at[slot], w_sem.at[slot])

    def wo_copy(n):
        return pltpu.make_async_copy(wout.at[:, pl.ds(pl.multiple_of(n * p.wcols, HEAD), p.wcols)], wo.at[n], wo_sem.at[n])

    def x_copy(r):
        rows = pl.ds(r * rows4, rows4)
        return pltpu.make_async_copy(x.at[rows], h.at[rows], x_sem.at[r])

    def wkv_copy(g):
        col = g * (p.group + 2) * HEAD + p.group * HEAD
        return pltpu.make_async_copy(wqkv.at[:, pl.ds(col, 2 * HEAD)], w.at[1, :, pl.ds(g * 2 * HEAD, 2 * HEAD)], b_sem.at[g])

    x_copy(0).start()
    for g in range(p.kv):
        wkv_copy(g).start()
    kc_copy = pltpu.make_async_copy(cache_in.at[0], ka.at[:, pl.ds(cp * p.cache, p.cache)], b_sem.at[3])
    vc_copy = pltpu.make_async_copy(cache_in.at[1], vb.at[:, pl.ds(0, p.cache)], b_sem.at[4])
    kc_copy.start()
    vc_copy.start()
    rope_copy = pltpu.make_async_copy(rope_in, rope, b_sem.at[2])
    rope_copy.start()

    barrier = pltpu.get_barrier_semaphore()
    for k in range(1, 4):
        pl.semaphore_signal(barrier, inc=1, device_id={'tp': lax.rem(tp + k, 4)}, device_id_type=MESH)
        pl.semaphore_signal(barrier, inc=1, device_id={'cp': lax.rem(cp + k, 4)}, device_id_type=MESH)

    def cache_copies(owner, peer, k):
        at = pl.multiple_of(owner * p.cache, p.cache)
        ks = ka.at[:, pl.ds(at, p.cache)]
        vs = vt.at[:, :, pl.ds(at, p.cache)]
        return (pltpu.make_async_remote_copy(ks, ks, cs_send.at[k, 0], cs_recv.at[k, 0], device_id={'cp': peer}, device_id_type=MESH),
                pltpu.make_async_remote_copy(vs, vs, cs_send.at[k, 1], cs_recv.at[k, 1], device_id={'cp': peer}, device_id_type=MESH))

    def new_copies(at, size, peer, k):
        ks = ka.at[:, pl.ds(at, size)]
        vs = vt.at[:, :, pl.ds(at, size)]
        return (pltpu.make_async_remote_copy(ks, ks, kv_send.at[k, 0], kv_recv.at[k, 0], device_id={'cp': peer}, device_id_type=MESH),
                pltpu.make_async_remote_copy(vs, vs, kv_send.at[k, 1], kv_recv.at[k, 1], device_id={'cp': peer}, device_id_type=MESH))

    vc_copy.wait()
    for g in range(p.kv):
        vt[g, :, pl.ds(pl.multiple_of(cp * p.cache, p.cache), p.cache)] = vb[g, 0:p.cache, :].astype(jnp.float32).T.astype(jnp.bfloat16)
    kc_copy.wait()
    pl.semaphore_wait(barrier, 6)
    for peer, k in ((across, 1), (partner, 0)):
        for c in cache_copies(cp, peer, k):
            c.start()

    def send_new(r):
        at = pl.multiple_of(new0 + r * rows4, rows4)

        @pl.when(cp < 2)
        def _():
            for c in new_copies(at, rows4, across, 1):
                c.start()

        @pl.when(lax.rem(cp, 2) == 0)
        def _():
            for c in new_copies(at, rows4, partner, 0):
                c.start()

    lane = lax.broadcasted_iota(jnp.int32, (1, HEAD), 1)
    even = lax.rem(lane, 2) == 0
    turned = lane < 64

    def angles(rows, count):
        r = rope[rows, :]
        both = jnp.concatenate([r, r], axis=1)
        at = lax.broadcasted_iota(jnp.int32, (count, HEAD), 1)
        pair = lax.rem(at, 64) // 2
        c = jnp.take_along_axis(both, pair, axis=1)
        s = jnp.take_along_axis(both, pair + 32, axis=1)
        return c, jnp.where(even, -s, s)

    def rotate(a, c, s):
        swap = jnp.where(even, pltpu.roll(a, HEAD - 1, 1), pltpu.roll(a, 1, 1))
        return jnp.where(turned, a * c + swap * s, a)

    rope_copy.wait()
    for g in range(p.kv):
        wkv_copy(g).wait()
    for r in range(1, 4):
        x_copy(r).start()
    wq_copy(0).start()
    nsub = max(1, rows4 // 128)
    sub = rows4 // nsub
    wide = 512

    def kv_step(r, _):
        x_copy(r).wait()

        @pl.when(r > 0)
        def _():
            send_new(r - 1)

        def norm(b, _):
            rows = pl.ds(pl.multiple_of(r * rows4 + b * sub, sub), sub)
            total = None
            for c in range(0, p.dim, wide):
                v = h[rows, c:c + wide].astype(jnp.float32)
                v = v * v
                for k in range(0, wide, HEAD):
                    total = v[:, k:k + HEAD] if total is None else total + v[:, k:k + HEAD]
            inv = lax.rsqrt(jnp.sum(total, axis=1, keepdims=True) * (1.0 / p.dim) + EPS)
            for c in range(0, p.dim, wide):
                v = h[rows, c:c + wide].astype(jnp.float32)
                h[rows, c:c + wide] = (v * inv * small[0:1, goff + c:goff + c + wide]).astype(jnp.bfloat16)
            return 0

        lax.fori_loop(0, nsub, norm, 0)
        rows = pl.ds(pl.multiple_of(r * rows4, rows4), rows4)
        at = pl.multiple_of(new0 + r * rows4, rows4)
        a = jnp.dot(h[rows, :], w[1], preferred_element_type=jnp.float32)
        c, s = angles(rows, rows4)
        for g in range(p.kv):
            col = g * (p.group + 2) * HEAD + p.group * HEAD
            key = rotate(a[:, g * 2 * HEAD:g * 2 * HEAD + HEAD] + small[0:1, col:col + HEAD], c, s)
            val = a[:, g * 2 * HEAD + HEAD:(g + 1) * 2 * HEAD] + small[0:1, col + HEAD:col + 2 * HEAD]
            ka[g, pl.ds(at, rows4), :] = key.astype(jnp.bfloat16)
            vb[g, rows, :] = val.astype(jnp.bfloat16)
            vt[g, :, pl.ds(at, rows4)] = val.T.astype(jnp.bfloat16)
        return 0

    lax.fori_loop(0, 4, kv_step, 0)
    send_new(3)
    wq_copy(1).start()

    def out_copies():
        res = []
        for g in range(p.kv):
            cols = pl.ds(g * HEAD, HEAD)
            res.append(pltpu.make_async_copy(ka.at[g, pl.ds(new0, p.tok)], kn.at[:, cols], out_sem.at[g]))
            res.append(pltpu.make_async_copy(vb.at[g], vn.at[:, cols], out_sem.at[p.kv + g]))
        return res

    for c in out_copies():
        c.start()

    def reset(i, _):
        m_s[i] = jnp.full((8, p.n), LOW, jnp.float32)
        l_s[i] = jnp.zeros((8, p.n), jnp.float32)
        o_t[i] = jnp.zeros((HEAD, p.n), jnp.float32)
        return 0

    lax.fori_loop(0, p.nd, reset, 0)

    def q_tile(t, first, count):
        j = lax.rem(t, p.nq)
        rows = pl.ds(pl.multiple_of(first * p.mr, p.mr), count * p.mr)
        wq_copy(t).wait()
        a = jnp.dot(h[rows, :], w[lax.rem(t, 2)], preferred_element_type=jnp.float32)
        a = a + small[0:1, pl.ds(pl.multiple_of(wq_col(j), HEAD), p.wcols)]
        c, s = angles(rows, count * p.mr)
        for k in range(QUAD):
            b = rotate(a[:, k * HEAD:(k + 1) * HEAD], c, s).astype(jnp.bfloat16)
            for u in range(count):
                q[lax.rem(first + u, 4), 2 * j + k // 2, (k % 2) * p.mr:(k % 2 + 1) * p.mr, :] = b[u * p.mr:(u + 1) * p.mr, :]

        @pl.when(t + 2 < p.wt)
        def _():
            wq_copy(t + 2).start()

    part_rows = min(256, p.kt)
    row_of = lax.rem(lax.broadcasted_iota(jnp.int32, (p.kt, p.n), 1), p.mr) - lax.broadcasted_iota(jnp.int32, (p.kt, p.n), 0)

    def scores(qs, pair, off, k, bound):
        g = pair // p.dpg
        s = lax.dot_general(ka[g, pl.ds(pl.multiple_of(off, p.kt), p.kt), :], q[qs, pair], (((1,), (1,)), ((), ())),
                            preferred_element_type=jnp.float32) * scale
        if bound is not None:
            s = jnp.where(row_of >= -bound, s, LOW)
        s_t[k] = s
        mx_t[k] = jnp.max(s.reshape(p.kt // 8, 8, p.n), axis=0)

    def weigh(pair, off, k):
        g = pair // p.dpg
        m_old = m_s[pair, 0:1, :]
        m_new = jnp.maximum(m_old, jnp.max(mx_t[k], axis=0, keepdims=True))
        alpha = jnp.exp2(m_old - m_new)
        m_s[pair, 0:1, :] = m_new
        acc = None
        es = []
        for r in range(0, p.kt, part_rows):
            e = jnp.exp2(s_t[k, r:r + part_rows, :] - m_new)
            part = jnp.sum(e.reshape(part_rows // 8, 8, p.n), axis=0)
            acc = part if acc is None else acc + part
            es.append(e.astype(jnp.bfloat16))
        d = jnp.dot(vt[g, :, pl.ds(pl.multiple_of(off, p.kt), p.kt)], jnp.concatenate(es, axis=0), preferred_element_type=jnp.float32)
        l_s[pair] = l_s[pair] * alpha + acc
        o_t[pair] = o_t[pair] * alpha + d

    anything = 1 << 20
    slots = p.look + 1

    def own_at(j):
        return new0 + j * p.kt

    def own_segment(u, j, tiles):
        qs = lax.rem(u, 4)
        bound = u * p.mr - j * p.kt
        more = j + 1 < tiles

        @pl.when(j == 0)
        def _():
            for i in range(p.look):
                scores(qs, i, new0, i, u * p.mr)

        for i in range(p.nd):
            n = i + p.look
            if n < p.nd:
                scores(qs, n, own_at(j), n % slots, bound)
            else:
                n -= p.nd
                scores(qs, jnp.where(more, n, n // 2), jnp.where(more, own_at(j + 1), (n % 2) * p.kt), (n + p.nd) % slots,
                       jnp.where(more, bound - p.kt, anything))
            weigh(i, own_at(j), i % slots)

    def block_at(b):
        return jnp.where(b == 0, 0, p.tok * (1 + jnp.where(lax.rem(cp, 2) == 1, cp - b, b - 1)))

    def block_segment(u, b, count):
        qs = lax.rem(u, 4)
        at = block_at(b)
        following = jnp.where((u > 0) & (b + 1 < count), block_at(b + 1), 0)

        @pl.when((u == 0) & (b > 0))
        def _():
            for i in range(p.look):
                scores(qs, i // 2, at + (i % 2) * p.kt, i, None)

        for i in range(2 * p.nd):
            n = i + p.look
            scores(qs, (n // 2) % p.nd, (at if n < 2 * p.nd else following) + (n % 2) * p.kt, n % slots, None)
            weigh(i // 2, at + (i % 2) * p.kt, i % slots)

    blocks = 1 + cp

    role_a = 3 - tp
    role_b = tp

    def chain(d, i):
        m = i // p.cpm
        j = lax.rem(i, p.cpm)
        mine = own.at[lax.rem(m, p.owns), j, pl.ds(d * p.half, p.half)]
        rows = pl.ds(pl.multiple_of(m * p.mr + d * p.half, p.half), p.half)
        cols = pl.ds(pl.multiple_of(j * p.cc, p.cc), p.cc)
        return mine, land.at[d, i], y.at[rows, cols]

    def peers(d):
        return (jnp.maximum(tp - 1, 0), jnp.minimum(tp + 1, 3)) if d == 0 else (jnp.minimum(tp + 1, 3), jnp.maximum(tp - 1, 0))

    def rs_copy(d, i):
        mine, there, _ = chain(d, i)
        return pltpu.make_async_remote_copy(mine, there, rs_send.at[d, i], rs_recv.at[d, i], device_id={'tp': peers(d)[0]}, device_id_type=MESH)

    def st_copy(d, i):
        k = lax.rem(i, 2)
        return pltpu.make_async_copy(land.at[d, i], stage.at[d, k], st_sem.at[d, k])

    def ag_copy(d, i, src=None):
        out = chain(d, i)[2]
        return pltpu.make_async_remote_copy(out if src is None else src, out, ag_send.at[d, i], ag_recv.at[d, i],
                                            device_id={'tp': peers(d)[1]}, device_id_type=MESH)

    def yl_copy(d, i):
        k = lax.rem(i, p.cpm)
        return pltpu.make_async_copy(yst.at[d, k], chain(d, i)[2], yl_sem.at[d, k])

    def pick(role, table, j):
        v = table[0][j]
        for r in range(1, len(table)):
            v = jnp.where(role == r, table[r][j], v)
        return v

    def when_due(seg, role, table, ahead, act):
        hit = seg < 0
        i = 0
        for j in range(p.cpm):
            t = seg + ahead - pick(role, table, j)
            m = jnp.maximum(t, 0) // p.nseg
            due = (t >= 0) & (m < p.nm) & (lax.rem(jnp.maximum(t, 0), p.nseg) == 0)
            hit = hit | due
            i = i + jnp.where(due, m * p.cpm + j, 0)

        @pl.when(hit)
        def _():
            act(i)

    def service(seg):
        for d, role in ((0, role_a), (1, role_b)):
            def sums(i, d=d, role=role):
                mine = chain(d, i)[0]
                arrived = stage.at[d, lax.rem(i, 2)]

                @pl.when(role > 0)
                def _():
                    st_copy(d, i).wait()

                @pl.when((role > 0) & (role < 3))
                def _():
                    mine[...] = mine[...] + arrived[...]

                @pl.when(role < 3)
                def _():
                    rs_copy(d, i).start()

                @pl.when(role == 3)
                def _():
                    k = lax.rem(i, p.cpm)

                    @pl.when(i >= p.cpm)
                    def _():
                        yl_copy(d, i - p.cpm).wait()
                        ag_copy(d, i - p.cpm, yst.at[d, k]).wait_send()

                    yst[d, k] = (mine[...] + arrived[...]).astype(jnp.bfloat16)
                    yl_copy(d, i).start()
                    ag_copy(d, i, yst.at[d, k]).start()

            when_due(seg, role, p.sums, 0, sums)

        for d, role in ((0, role_a), (1, role_b)):
            def rows(i, d=d, role=role):
                @pl.when(role < 3)
                def _():
                    ag_copy(d, i).wait_recv()

                @pl.when((role < 3) & (role > 0))
                def _():
                    ag_copy(d, i).start()

            when_due(seg, 2 - role, p.rows, 0, rows)

        for d, role in ((0, role_a), (1, role_b)):
            def fetch(i, d=d, role=role):
                @pl.when(role > 0)
                def _():
                    rs_copy(d, i).wait_recv()
                    st_copy(d, i).start()

            when_due(seg, role, p.sums, 1, fetch)

    take_a = jnp.where(tp == 0, 1, 0).astype(jnp.float32)
    take_b = jnp.where(tp == 3, 1, 0).astype(jnp.float32)
    x_half = jnp.where(tp == 3, p.half, 0)

    def xb_copy(m):
        return pltpu.make_async_copy(x.at[pl.ds(pl.multiple_of(m * p.mr + x_half, p.half), p.half)], xb, b_sem.at[5])

    def first_q(t, _):
        q_tile(t, 0, 1)

        @pl.when(t == max(0, p.nq - 3))
        def _():
            for n in range(p.nt):
                wo_copy(n).start()

        return 0

    lax.fori_loop(0, p.nq, first_q, 0)

    for c in cache_copies(across, partner, 1):
        c.wait_recv()
    for c in cache_copies(across, partner, 2):
        c.start()
    for k in (0, 2):
        for c in cache_copies(cp, partner, k):
            c.wait_recv()

    def segment(seg, _):
        m = seg // p.nseg
        s = lax.rem(seg, p.nseg)
        busy = m < p.nm
        tiles = (m * p.mr + p.mr + p.kt - 1) // p.kt

        @pl.when(busy & (s < tiles) & (s < p.s_blk))
        def _():
            @pl.when(s == 0)
            def _():
                xb_copy(m).start()

            own_segment(m, s, tiles)

        @pl.when((seg == p.s_blk + 1) & (lax.rem(cp, 2) == 1))
        def _():
            for c in new_copies(pl.multiple_of(p.tok * cp, p.tok), p.tok, partner, 0):
                c.wait_recv()

        @pl.when((cp >= 2) & (seg == p.s_blk + cp - 1))
        def _():
            direct = pl.multiple_of(p.tok * (cp - 1), p.tok)
            for c in new_copies(direct, p.tok, partner, 1):
                c.wait_recv()
            for c in new_copies(direct, p.tok, partner, 2):
                c.start()

        @pl.when((cp >= 2) & (seg == p.s_blk + cp))
        def _():
            for c in new_copies(pl.multiple_of(p.tok * (cp - 1), p.tok), p.tok, partner, 2):
                c.wait_recv()

        @pl.when(busy & (s >= p.s_blk) & (s < p.s_blk + blocks))
        def _():
            block_segment(m, s - p.s_blk, blocks)

        @pl.when(busy & (s == p.s_fin))
        def _():
            def finish(i, _):
                inv = 1.0 / jnp.sum(l_s[i], axis=0, keepdims=True)
                v = o_t[i] * inv
                for k in range(2):
                    o[:, pl.ds(pl.multiple_of((i * 2 + k) * HEAD, HEAD), HEAD)] = v[:, k * p.mr:(k + 1) * p.mr].T.astype(jnp.bfloat16)
                return reset(i, 0)

            lax.fori_loop(0, p.nd, finish, 0)

        @pl.when(busy & (s >= p.s_out) & (s < p.s_q))
        def _():
            n = s - p.s_out

            @pl.when(n == 0)
            def _():
                xb_copy(m).wait()

            @pl.when((n == 0) & (m >= p.owns))
            def _():
                for d, role in ((0, role_a), (1, role_b)):
                    @pl.when(role < 3)
                    def _():
                        for j in range(p.cpm):
                            rs_copy(d, (m - p.owns) * p.cpm + j).wait_send()

            @pl.when(m == 0)
            def _():
                wo_copy(n).wait()

            a = jnp.dot(o[...], wo[n], preferred_element_type=jnp.float32)
            r = xb[:, pl.ds(pl.multiple_of(n * p.wcols, HEAD), p.wcols)].astype(jnp.float32)
            cols = pl.ds(pl.multiple_of(lax.rem(n, p.per) * p.wcols, HEAD), p.wcols)
            own[lax.rem(m, p.owns), n // p.per, 0:p.half, cols] = a[0:p.half] + r * take_a
            own[lax.rem(m, p.owns), n // p.per, p.half:p.mr, cols] = a[p.half:p.mr] + r * take_b

        @pl.when((m == 0) & (s >= p.s_q))
        def _():
            for k in range(2):
                q_tile(p.nq + 2 * (s - p.s_q) + k, 1, 1)

        @pl.when((m == 1) & (s >= p.s_q))
        def _():
            for k in range(2):
                q_tile(2 * p.nq + 2 * (s - p.s_q) + k, 2, 2)

        @pl.when((m >= 2) & (m < p.nm - 2) & (s >= p.s_q))
        def _():
            q_tile(3 * p.nq + (m - 2) * p.hq + s - p.s_q, m - lax.rem(m, 2) + 2, 2)

        service(seg)
        return 0

    lax.fori_loop(0, p.total, segment, 0)

    for d, role in ((0, role_a), (1, role_b)):
        @pl.when(role < 3)
        def _():
            def last_sums(i, _):
                rs_copy(d, i).wait_send()
                return 0
            lax.fori_loop((p.nm - p.owns) * p.cpm, p.chunks, last_sums, 0)

        @pl.when((role > 0) & (role < 3))
        def _():
            def last_rows(i, _):
                ag_copy(d, i).wait_send()
                return 0
            lax.fori_loop(0, p.chunks, last_rows, 0)

        @pl.when(role == 3)
        def _():
            for k in range(p.cpm):
                i = p.chunks - p.cpm + k
                yl_copy(d, i).wait()
                ag_copy(d, i, yst.at[d, k]).wait_send()

    for c in out_copies():
        c.wait()
    for k in (0, 1):
        for c in cache_copies(cp, partner, k):
            c.wait_send()
    for c in cache_copies(across, partner, 2):
        c.wait_send()

    @pl.when(cp < 2)
    def _():
        for c in new_copies(new0, p.tok, across, 1):
            c.wait_send()

    @pl.when(lax.rem(cp, 2) == 0)
    def _():
        for c in new_copies(new0, p.tok, partner, 0):
            c.wait_send()

    @pl.when(cp >= 2)
    def _():
        for c in new_copies(pl.multiple_of(p.tok * (cp - 1), p.tok), p.tok, partner, 2):
            c.wait_send()


def build(p):
    def local_step(x, k_cache, v_cache, rope_table, norm_gain, w_qkv, b_qkv, w_out):
        small = jnp.concatenate([b_qkv, norm_gain]).astype(jnp.float32).reshape(1, -1)
        cached = jnp.stack([k_cache, v_cache]).transpose(0, 2, 1, 3)
        anyspace = pl.BlockSpec(memory_space=pl.ANY)
        vmem = pl.BlockSpec(memory_space=pltpu.VMEM)
        bf, f32 = jnp.bfloat16, jnp.float32
        dma = pltpu.SemaphoreType.DMA
        kvw = p.kv * HEAD
        y, kn, vn, _ = pl.pallas_call(
            functools.partial(kernel, p),
            name='block',
            out_shape=(jax.ShapeDtypeStruct((p.tok, p.dim), bf), jax.ShapeDtypeStruct((p.tok, kvw), bf), jax.ShapeDtypeStruct((p.tok, kvw), bf),
                       jax.ShapeDtypeStruct((2, p.chunks, p.half, p.cc), f32)),
            in_specs=[anyspace, anyspace, anyspace, vmem, anyspace, anyspace],
            out_specs=(anyspace, anyspace, anyspace, anyspace),
            scratch_shapes=[
                pltpu.VMEM((p.tok, p.dim), bf),
                pltpu.VMEM((p.kv, p.keys, HEAD), bf),
                pltpu.VMEM((p.kv, HEAD, p.keys), bf),
                pltpu.VMEM((p.tok, 64), f32),
                pltpu.VMEM((4, p.nd, p.n, HEAD), bf),
                pltpu.VMEM((p.nd, HEAD, p.n), f32),
                pltpu.VMEM((p.mr, p.heads * HEAD), bf),
                pltpu.VMEM((p.look + 1, p.kt, p.n), f32),
                pltpu.VMEM((p.look + 1, 8, p.n), f32),
                pltpu.VMEM((p.nd, 8, p.n), f32),
                pltpu.VMEM((p.nd, 8, p.n), f32),
                pltpu.VMEM((p.owns, p.cpm, p.mr, p.cc), f32),
                pltpu.VMEM((2, 2, p.half, p.cc), f32),
                pltpu.VMEM((2, p.cpm, p.half, p.cc), bf),
                pltpu.VMEM((p.half, p.dim), bf),
                pltpu.VMEM((2, p.dim, p.wcols), bf),
                pltpu.VMEM((p.nt, p.heads * HEAD, p.wcols), bf),
                pltpu.VMEM((p.kv, p.tok, HEAD), bf),
                dma((4,)), dma((2,)), dma((p.nt,)), dma((6,)), dma((2 * p.kv,)),
                dma((3, 2)), dma((3, 2)), dma((3, 2)), dma((3, 2)),
                dma((2, p.chunks)), dma((2, p.chunks)), dma((2, 2)), dma((2, p.chunks)), dma((2, p.chunks)), dma((2, p.cpm)),
            ],
            compiler_params=pltpu.CompilerParams(collective_id=0, has_side_effects=True, vmem_limit_bytes=67_000_000),
        )(x, cached, rope_table, small, w_qkv, w_out)
        shape = (p.tok, p.kv, HEAD)
        return y, kn.reshape(shape), vn.reshape(shape)

    return local_step


def solution(mesh):
    row_spec = P(('dp', 'cp'), None)
    cache_spec = P(('dp', 'cp'), 'tp', None)
    p = Plan(tok=1024, dim=4096, kv=2, group=12, cache=256, nm=8, kt=512)
    p.table([[8, 14, 16, 19], [15, 17, 20, 22], [19, 22, 27, 33], [31, 35, 38, 40]],
            [[36, 39, 41, 47], [39, 45, 51, 53], [54, 57, 59, 61]])
    return jax.shard_map(build(p), mesh=mesh, in_specs=(row_spec, cache_spec, cache_spec, row_spec, P(None), P(None, 'tp'), P('tp'), P('tp', None)),
                         out_specs=(row_spec, cache_spec, cache_spec), check_vma=False)
```

```python
import functools
import math

import jax
import jax.numpy as jnp
from jax import lax
from jax.experimental import pallas as pl
from jax.experimental.pallas import tpu as pltpu
from jax.sharding import PartitionSpec as P

EPS = 1.5625e-07
LOW = -1e30
HEAD = 128
QUAD = 4
MESH = pl.DeviceIdType.MESH


class Plan:
    def __init__(self, tok, dim, kv, group, cache, nm, kt):
        self.tok, self.dim, self.kv, self.group, self.cache = tok, dim, kv, group, cache
        self.nm = nm
        self.mr = tok // nm
        self.kt = kt
        self.heads = kv * group
        self.nd = self.heads // 2
        self.dpg = group // 2
        self.n = 2 * self.mr
        self.keys = tok * 5
        self.wcols = QUAD * HEAD
        self.nq = self.heads // QUAD
        self.qpg = group // QUAD
        self.hq = self.nq // 2
        self.nt = dim // self.wcols
        self.cpm = 4
        self.per = self.nt // self.cpm
        self.cc = dim // self.cpm
        self.half = self.mr // 2
        self.owns = 2
        self.fin = math.gcd(self.nd, 3)
        self.look = 3
        self.wt = self.nq * (nm // 2)
        self.s_blk = 2
        self.s_fin = self.s_blk + 4
        self.s_out = self.s_fin + 1
        self.s_q = self.s_out + self.nt
        self.nseg = self.s_q + self.hq
        self.chunks = nm * self.cpm
        self.table([[self.s_out + self.per * (j + 1) - 1 + 3 * r for j in range(self.cpm)] for r in range(4)],
                   [[self.s_out + self.per * (j + 1) - 1 + 12 + 3 * r for j in range(self.cpm)] for r in range(3)])

    def table(self, sums, rows):
        self.sums, self.rows = sums, rows
        self.total = self.nseg * (self.nm - 1) + max(max(r) for r in sums + rows) + 1

def kernel(p, x, k_in, v_in, rope_in, gain_in, bias_in, wqkv, wout, y, kn, vn, land,
           h, ka, vt, rope_t, rope, b1, g1, small, cached, q, o_t, o, s_t, mx_t, m_s, l_s, own, stage, yst, xb, w, wo, kv_out,
           x_sem, w_sem, wo_sem, b_sem, out_sem, cs_send, cs_recv, kv_send, kv_recv,
           rs_send, rs_recv, st_sem, ag_send, ag_recv, yl_sem):
    tp = lax.axis_index('tp')
    cp = lax.axis_index('cp')
    partner = cp + 1 - 2 * lax.rem(cp, 2)
    across = lax.rem(cp + 2, 4)
    scale = HEAD ** -0.5 * math.log2(math.e)
    new0 = p.tok * (1 + cp)
    rows4 = p.tok // 4
    goff = (p.group + 2) * HEAD * p.kv

    def wq_col(j):
        return (j // p.qpg) * (p.group + 2) * HEAD + lax.rem(j, p.qpg) * p.wcols

    def wq_copy(t):
        slot = lax.rem(t, 2)
        col = pl.multiple_of(wq_col(lax.rem(t, p.nq)), HEAD)
        return pltpu.make_async_copy(wqkv.at[:, pl.ds(col, p.wcols)], w.at[slot], w_sem.at[slot])

    def wo_copy(n):
        return pltpu.make_async_copy(wout.at[:, pl.ds(pl.multiple_of(n * p.wcols, HEAD), p.wcols)], wo.at[n], wo_sem.at[n])

    def x_copy(r):
        rows = pl.ds(r * rows4, rows4)
        return pltpu.make_async_copy(x.at[rows], h.at[rows], x_sem.at[r])

    def wkv_copy(g):
        col = g * (p.group + 2) * HEAD + p.group * HEAD
        return pltpu.make_async_copy(wqkv.at[:, pl.ds(col, 2 * HEAD)], w.at[1, :, pl.ds(g * 2 * HEAD, 2 * HEAD)], b_sem.at[g])

    x_copy(0).start()
    for g in range(p.kv):
        wkv_copy(g).start()
    little = [pltpu.make_async_copy(rope_in, rope_t, b_sem.at[2]), pltpu.make_async_copy(k_in, cached.at[0], b_sem.at[3]),
              pltpu.make_async_copy(v_in, cached.at[1], b_sem.at[4]), pltpu.make_async_copy(bias_in, b1, b_sem.at[6]),
              pltpu.make_async_copy(gain_in, g1, b_sem.at[7])]
    for c in little:
        c.start()

    barrier = pltpu.get_barrier_semaphore()
    for k in range(1, 4):
        pl.semaphore_signal(barrier, inc=1, device_id={'tp': lax.rem(tp + k, 4)}, device_id_type=MESH)
        pl.semaphore_signal(barrier, inc=1, device_id={'cp': lax.rem(cp + k, 4)}, device_id_type=MESH)

    def cache_copies(owner, peer, k):
        at = pl.multiple_of(owner * p.cache, p.cache)
        ks = ka.at[:, pl.ds(at, p.cache)]
        vs = vt.at[:, :, pl.ds(at, p.cache)]
        return (pltpu.make_async_remote_copy(ks, ks, cs_send.at[k, 0], cs_recv.at[k, 0], device_id={'cp': peer}, device_id_type=MESH),
                pltpu.make_async_remote_copy(vs, vs, cs_send.at[k, 1], cs_recv.at[k, 1], device_id={'cp': peer}, device_id_type=MESH))

    def new_copies(at, size, peer, k):
        ks = ka.at[:, pl.ds(at, size)]
        vs = vt.at[:, :, pl.ds(at, size)]
        return (pltpu.make_async_remote_copy(ks, ks, kv_send.at[k, 0], kv_recv.at[k, 0], device_id={'cp': peer}, device_id_type=MESH),
                pltpu.make_async_remote_copy(vs, vs, kv_send.at[k, 1], kv_recv.at[k, 1], device_id={'cp': peer}, device_id_type=MESH))

    for c in little:
        c.wait()
    here = pl.multiple_of(cp * p.cache, p.cache)
    for g in range(p.kv):
        ka[g, pl.ds(here, p.cache), :] = cached[0].astype(jnp.float32)[:, g, :].astype(jnp.bfloat16)
        vt[g, :, pl.ds(here, p.cache)] = cached[1].astype(jnp.float32)[:, g, :].T.astype(jnp.bfloat16)
    small[0:1, 0:goff] = b1[...].astype(jnp.float32).reshape(1, goff)
    small[0:1, goff:goff + p.dim] = g1[...].astype(jnp.float32).reshape(1, p.dim)
    rope[...] = rope_t[...].T
    pl.semaphore_wait(barrier, 6)
    for peer, k in ((across, 1), (partner, 0)):
        for c in cache_copies(cp, peer, k):
            c.start()

    def send_new(r):
        at = pl.multiple_of(new0 + r * rows4, rows4)

        @pl.when(cp < 2)
        def _():
            for c in new_copies(at, rows4, across, 1):
                c.start()

        @pl.when(lax.rem(cp, 2) == 0)
        def _():
            for c in new_copies(at, rows4, partner, 0):
                c.start()

    lane = lax.broadcasted_iota(jnp.int32, (1, HEAD), 1)
    even = lax.rem(lane, 2) == 0
    turned = lane < 64

    def angles(rows, count):
        r = rope[rows, :]
        both = jnp.concatenate([r, r], axis=1)
        at = lax.broadcasted_iota(jnp.int32, (count, HEAD), 1)
        pair = lax.rem(at, 64) // 2
        c = jnp.take_along_axis(both, pair, axis=1)
        s = jnp.take_along_axis(both, pair + 32, axis=1)
        return c, jnp.where(even, -s, s)

    def rotate(a, c, s):
        swap = jnp.where(even, pltpu.roll(a, HEAD - 1, 1), pltpu.roll(a, 1, 1))
        return jnp.where(turned, a * c + swap * s, a)

    for g in range(p.kv):
        wkv_copy(g).wait()
    for r in range(1, 4):
        x_copy(r).start()
    wq_copy(0).start()
    nsub = max(1, rows4 // 128)
    sub = rows4 // nsub
    wide = 512

    def norm(b):
        rows = pl.ds(pl.multiple_of(b * sub, sub), sub)
        total = None
        for c in range(0, p.dim, wide):
            v = h[rows, c:c + wide].astype(jnp.float32)
            v = v * v
            for k in range(0, wide, HEAD):
                total = v[:, k:k + HEAD] if total is None else total + v[:, k:k + HEAD]
        inv = lax.rsqrt(jnp.sum(total, axis=1, keepdims=True) * (1.0 / p.dim) + EPS)
        for c in range(0, p.dim, wide):
            v = h[rows, c:c + wide].astype(jnp.float32)
            h[rows, c:c + wide] = (v * inv * small[0:1, goff + c:goff + c + wide]).astype(jnp.bfloat16)

    def keys_values(r, ahead):
        rows = pl.ds(pl.multiple_of(r * rows4, rows4), rows4)
        at = pl.multiple_of(new0 + r * rows4, rows4)
        a = jnp.dot(h[rows, :], w[1], preferred_element_type=jnp.float32)
        if ahead:
            for b in range(nsub):
                norm((r + 1) * nsub + b)
        c, s = angles(rows, rows4)
        keys, vals = [], []
        for g in range(p.kv):
            col = g * (p.group + 2) * HEAD + p.group * HEAD
            keys.append(rotate(a[:, g * 2 * HEAD:g * 2 * HEAD + HEAD] + small[0:1, col:col + HEAD], c, s))
            vals.append(a[:, g * 2 * HEAD + HEAD:(g + 1) * 2 * HEAD] + small[0:1, col + HEAD:col + 2 * HEAD])
            ka[g, pl.ds(at, rows4), :] = keys[g].astype(jnp.bfloat16)
            vt[g, :, pl.ds(at, rows4)] = vals[g].T.astype(jnp.bfloat16)
        kv_out[0, rows] = jnp.swapaxes(jnp.stack(keys), 0, 1).astype(jnp.bfloat16)
        kv_out[1, rows] = jnp.swapaxes(jnp.stack(vals), 0, 1).astype(jnp.bfloat16)

    def kv_step(r, _):
        x_copy(r + 1).wait()

        @pl.when(r > 0)
        def _():
            send_new(r - 1)

        keys_values(r, True)
        return 0

    x_copy(0).wait()
    for b in range(nsub):
        norm(b)
    lax.fori_loop(0, 3, kv_step, 0)
    send_new(2)
    keys_values(3, False)
    wq_copy(1).start()
    send_new(3)

    def out_copies():
        return [pltpu.make_async_copy(kv_out.at[0], kn, out_sem.at[0]), pltpu.make_async_copy(kv_out.at[1], vn, out_sem.at[1])]

    for c in out_copies():
        c.start()

    def reset(i, _):
        m_s[i] = jnp.full((8, p.n), LOW, jnp.float32)
        l_s[i] = jnp.zeros((8, p.n), jnp.float32)
        o_t[i] = jnp.zeros((HEAD, p.n), jnp.float32)
        return 0

    lax.fori_loop(0, p.nd, reset, 0)

    def q_tile(t):
        j = lax.rem(t, p.nq)
        first = t // p.nq * 2
        count = 2
        rows = pl.ds(pl.multiple_of(first * p.mr, p.mr), count * p.mr)
        wq_copy(t).wait()
        a = jnp.dot(h[rows, :], w[lax.rem(t, 2)], preferred_element_type=jnp.float32)
        a = a + small[0:1, pl.ds(pl.multiple_of(wq_col(j), HEAD), p.wcols)]
        c, s = angles(rows, count * p.mr)
        for k in range(QUAD):
            b = rotate(a[:, k * HEAD:(k + 1) * HEAD], c, s).astype(jnp.bfloat16)
            for u in range(count):
                q[lax.rem(first + u, 4), 2 * j + k // 2, (k % 2) * p.mr:(k % 2 + 1) * p.mr, :] = b[u * p.mr:(u + 1) * p.mr, :]

        @pl.when(t + 2 < p.wt)
        def _():
            wq_copy(t + 2).start()

    part_rows = min(256, p.kt)
    row_of = lax.rem(lax.broadcasted_iota(jnp.int32, (p.kt, p.n), 1), p.mr) - lax.broadcasted_iota(jnp.int32, (p.kt, p.n), 0)

    def scores(qs, pair, off, k, bound):
        g = pair // p.dpg
        s = lax.dot_general(ka[g, pl.ds(pl.multiple_of(off, p.kt), p.kt), :], q[qs, pair], (((1,), (1,)), ((), ())),
                            preferred_element_type=jnp.float32) * scale
        if bound is not None:
            s = jnp.where(row_of >= -bound, s, LOW)
        s_t[k] = s
        mx_t[k] = jnp.max(s.reshape(p.kt // 8, 8, p.n), axis=0)

    def weigh(pair, off, k):
        g = pair // p.dpg
        m_old = m_s[pair, 0:1, :]
        m_new = jnp.maximum(m_old, jnp.max(mx_t[k], axis=0, keepdims=True))
        alpha = jnp.exp2(m_old - m_new)
        m_s[pair, 0:1, :] = m_new
        acc = None
        es = []
        for r in range(0, p.kt, part_rows):
            e = jnp.exp2(s_t[k, r:r + part_rows, :] - m_new)
            part = jnp.sum(e.reshape(part_rows // 8, 8, p.n), axis=0)
            acc = part if acc is None else acc + part
            es.append(e.astype(jnp.bfloat16))
        d = jnp.dot(vt[g, :, pl.ds(pl.multiple_of(off, p.kt), p.kt)], jnp.concatenate(es, axis=0), preferred_element_type=jnp.float32)
        l_s[pair] = l_s[pair] * alpha + acc
        o_t[pair] = o_t[pair] * alpha + d

    anything = 1 << 20
    slots = p.look + 1

    def own_at(j):
        return new0 + j * p.kt

    def own_segment(u, j, tiles):
        qs = lax.rem(u, 4)
        bound = u * p.mr - j * p.kt
        more = j + 1 < tiles

        @pl.when(j == 0)
        def _():
            for i in range(p.look):
                scores(qs, i, new0, i, u * p.mr)

        for i in range(p.nd):
            n = i + p.look
            if n < p.nd:
                scores(qs, n, own_at(j), n % slots, bound)
            else:
                n -= p.nd
                scores(qs, jnp.where(more, n, n // 2), jnp.where(more, own_at(j + 1), (n % 2) * p.kt), (n + p.nd) % slots,
                       jnp.where(more, bound - p.kt, anything))
            weigh(i, own_at(j), i % slots)

    def block_at(b):
        return jnp.where(b == 0, 0, p.tok * (1 + jnp.where(lax.rem(cp, 2) == 1, cp - b, b - 1)))

    def block_segment(u, b, count):
        qs = lax.rem(u, 4)
        at = block_at(b)
        following = jnp.where((u > 0) & (b + 1 < count), block_at(b + 1), 0)

        @pl.when((u == 0) & (b > 0))
        def _():
            for i in range(p.look):
                scores(qs, i // 2, at + (i % 2) * p.kt, i, None)

        for i in range(2 * p.nd):
            n = i + p.look
            scores(qs, (n // 2) % p.nd, (at if n < 2 * p.nd else following) + (n % 2) * p.kt, n % slots, None)
            weigh(i // 2, at + (i % 2) * p.kt, i % slots)

    blocks = 1 + cp

    role_a = 3 - tp
    role_b = tp

    def chain(d, i):
        m = i // p.cpm
        j = lax.rem(i, p.cpm)
        mine = own.at[lax.rem(m, p.owns), j, pl.ds(d * p.half, p.half)]
        rows = pl.ds(pl.multiple_of(m * p.mr + d * p.half, p.half), p.half)
        cols = pl.ds(pl.multiple_of(j * p.cc, p.cc), p.cc)
        return mine, land.at[d, i], y.at[rows, cols]

    def peers(d):
        return (jnp.maximum(tp - 1, 0), jnp.minimum(tp + 1, 3)) if d == 0 else (jnp.minimum(tp + 1, 3), jnp.maximum(tp - 1, 0))

    def rs_copy(d, i):
        mine, there, _ = chain(d, i)
        return pltpu.make_async_remote_copy(mine, there, rs_send.at[d, i], rs_recv.at[d, i], device_id={'tp': peers(d)[0]}, device_id_type=MESH)

    def st_copy(d, i):
        k = lax.rem(i, 2)
        return pltpu.make_async_copy(land.at[d, i], stage.at[d, k], st_sem.at[d, k])

    def ag_copy(d, i, src=None):
        out = chain(d, i)[2]
        return pltpu.make_async_remote_copy(out if src is None else src, out, ag_send.at[d, i], ag_recv.at[d, i],
                                            device_id={'tp': peers(d)[1]}, device_id_type=MESH)

    def yl_copy(d, i):
        k = lax.rem(i, p.cpm)
        return pltpu.make_async_copy(yst.at[d, k], chain(d, i)[2], yl_sem.at[d, k])

    def pick(role, table, j):
        v = table[0][j]
        for r in range(1, len(table)):
            v = jnp.where(role == r, table[r][j], v)
        return v

    def when_due(seg, role, table, ahead, act):
        hit = seg < 0
        i = 0
        for j in range(p.cpm):
            t = seg + ahead - pick(role, table, j)
            m = jnp.maximum(t, 0) // p.nseg
            due = (t >= 0) & (m < p.nm) & (lax.rem(jnp.maximum(t, 0), p.nseg) == 0)
            hit = hit | due
            i = i + jnp.where(due, m * p.cpm + j, 0)

        @pl.when(hit)
        def _():
            act(i)

    def service(seg):
        for d, role in ((0, role_a), (1, role_b)):
            def sums(i, d=d, role=role):
                mine = chain(d, i)[0]
                arrived = stage.at[d, lax.rem(i, 2)]

                @pl.when(role > 0)
                def _():
                    st_copy(d, i).wait()

                @pl.when((role > 0) & (role < 3))
                def _():
                    mine[...] = mine[...] + arrived[...]

                @pl.when(role < 3)
                def _():
                    rs_copy(d, i).start()

                @pl.when(role == 3)
                def _():
                    k = lax.rem(i, p.cpm)

                    @pl.when(i >= p.cpm)
                    def _():
                        yl_copy(d, i - p.cpm).wait()
                        ag_copy(d, i - p.cpm, yst.at[d, k]).wait_send()

                    yst[d, k] = (mine[...] + arrived[...]).astype(jnp.bfloat16)
                    yl_copy(d, i).start()
                    ag_copy(d, i, yst.at[d, k]).start()

            when_due(seg, role, p.sums, 0, sums)

        for d, role in ((0, role_a), (1, role_b)):
            def rows(i, d=d, role=role):
                @pl.when(role < 3)
                def _():
                    ag_copy(d, i).wait_recv()

                @pl.when((role < 3) & (role > 0))
                def _():
                    ag_copy(d, i).start()

            when_due(seg, 2 - role, p.rows, 0, rows)

        for d, role in ((0, role_a), (1, role_b)):
            def fetch(i, d=d, role=role):
                @pl.when(role > 0)
                def _():
                    rs_copy(d, i).wait_recv()
                    st_copy(d, i).start()

            when_due(seg, role, p.sums, 1, fetch)

    take_a = jnp.where(tp == 0, 1, 0).astype(jnp.float32)
    take_b = jnp.where(tp == 3, 1, 0).astype(jnp.float32)
    x_half = jnp.where(tp == 3, p.half, 0)

    def xb_copy(m):
        return pltpu.make_async_copy(x.at[pl.ds(pl.multiple_of(m * p.mr + x_half, p.half), p.half)], xb, b_sem.at[5])

    def first_q(t, _):
        q_tile(t)

        @pl.when(t == max(0, p.nq - 3))
        def _():
            for n in range(p.nt):
                wo_copy(n).start()

        return 0

    lax.fori_loop(0, p.nq, first_q, 0)

    for c in cache_copies(across, partner, 1):
        c.wait_recv()
    for c in cache_copies(across, partner, 2):
        c.start()
    for k in (0, 2):
        for c in cache_copies(cp, partner, k):
            c.wait_recv()

    def segment(seg, _):
        m = seg // p.nseg
        s = lax.rem(seg, p.nseg)
        busy = m < p.nm
        tiles = (m * p.mr + p.mr + p.kt - 1) // p.kt

        @pl.when(busy & (s < tiles) & (s < p.s_blk))
        def _():
            @pl.when(s == 0)
            def _():
                xb_copy(m).start()

            own_segment(m, s, tiles)

        @pl.when((seg == p.s_blk + 1) & (lax.rem(cp, 2) == 1))
        def _():
            for c in new_copies(pl.multiple_of(p.tok * cp, p.tok), p.tok, partner, 0):
                c.wait_recv()

        @pl.when((cp >= 2) & (seg == p.s_blk + cp - 1))
        def _():
            direct = pl.multiple_of(p.tok * (cp - 1), p.tok)
            for c in new_copies(direct, p.tok, partner, 1):
                c.wait_recv()
            for c in new_copies(direct, p.tok, partner, 2):
                c.start()

        @pl.when((cp >= 2) & (seg == p.s_blk + cp))
        def _():
            for c in new_copies(pl.multiple_of(p.tok * (cp - 1), p.tok), p.tok, partner, 2):
                c.wait_recv()

        @pl.when(busy & (s >= p.s_blk) & (s < p.s_blk + blocks))
        def _():
            block_segment(m, s - p.s_blk, blocks)

        @pl.when(busy & (s == p.s_fin))
        def _():
            def finish(i, _):
                for e in range(p.fin):
                    c = i * p.fin + e
                    v = o_t[c] * (1.0 / jnp.sum(l_s[c], axis=0, keepdims=True))
                    for k in range(2):
                        o[:, pl.ds(pl.multiple_of((c * 2 + k) * HEAD, HEAD), HEAD)] = v[:, k * p.mr:(k + 1) * p.mr].T.astype(jnp.bfloat16)
                    reset(c, 0)
                return 0

            lax.fori_loop(0, p.nd // p.fin, finish, 0)

        @pl.when(busy & (s >= p.s_out) & (s < p.s_q))
        def _():
            n = s - p.s_out

            @pl.when(n == 0)
            def _():
                xb_copy(m).wait()

            @pl.when((n == 0) & (m >= p.owns))
            def _():
                for d, role in ((0, role_a), (1, role_b)):
                    @pl.when(role < 3)
                    def _():
                        for j in range(p.cpm):
                            rs_copy(d, (m - p.owns) * p.cpm + j).wait_send()

            @pl.when(m == 0)
            def _():
                wo_copy(n).wait()

            a = jnp.dot(o[...], wo[n], preferred_element_type=jnp.float32)
            r = xb[:, pl.ds(pl.multiple_of(n * p.wcols, HEAD), p.wcols)].astype(jnp.float32)
            cols = pl.ds(pl.multiple_of(lax.rem(n, p.per) * p.wcols, HEAD), p.wcols)
            own[lax.rem(m, p.owns), n // p.per, 0:p.half, cols] = a[0:p.half] + r * take_a
            own[lax.rem(m, p.owns), n // p.per, p.half:p.mr, cols] = a[p.half:p.mr] + r * take_b

        @pl.when((m < p.nm - 2) & (s >= p.s_q))
        def _():
            q_tile((m // 2 + 1) * p.nq + lax.rem(m, 2) * p.hq + s - p.s_q)

        service(seg)
        return 0

    lax.fori_loop(0, p.total, segment, 0)

    for d, role in ((0, role_a), (1, role_b)):
        @pl.when(role < 3)
        def _():
            def last_sums(i, _):
                rs_copy(d, i).wait_send()
                return 0
            lax.fori_loop((p.nm - p.owns) * p.cpm, p.chunks, last_sums, 0)

        @pl.when((role > 0) & (role < 3))
        def _():
            def last_rows(i, _):
                ag_copy(d, i).wait_send()
                return 0
            lax.fori_loop(0, p.chunks, last_rows, 0)

        @pl.when(role == 3)
        def _():
            for k in range(p.cpm):
                i = p.chunks - p.cpm + k
                yl_copy(d, i).wait()
                ag_copy(d, i, yst.at[d, k]).wait_send()

    for c in out_copies():
        c.wait()
    for k in (0, 1):
        for c in cache_copies(cp, partner, k):
            c.wait_send()
    for c in cache_copies(across, partner, 2):
        c.wait_send()

    @pl.when(cp < 2)
    def _():
        for c in new_copies(new0, p.tok, across, 1):
            c.wait_send()

    @pl.when(lax.rem(cp, 2) == 0)
    def _():
        for c in new_copies(new0, p.tok, partner, 0):
            c.wait_send()

    @pl.when(cp >= 2)
    def _():
        for c in new_copies(pl.multiple_of(p.tok * (cp - 1), p.tok), p.tok, partner, 2):
            c.wait_send()


def build(p):
    def local_step(x, k_cache, v_cache, rope_table, norm_gain, w_qkv, b_qkv, w_out):
        anyspace = pl.BlockSpec(memory_space=pl.ANY)
        bf, f32 = jnp.bfloat16, jnp.float32
        dma = pltpu.SemaphoreType.DMA
        kv_shape = jax.ShapeDtypeStruct((p.tok, p.kv, HEAD), bf)
        y, k_new, v_new, _ = pl.pallas_call(
            functools.partial(kernel, p),
            name='block',
            out_shape=(jax.ShapeDtypeStruct((p.tok, p.dim), bf), kv_shape, kv_shape,
                       jax.ShapeDtypeStruct((2, p.chunks, p.half, p.cc), f32)),
            in_specs=[anyspace] * 8,
            out_specs=(anyspace, anyspace, anyspace, anyspace),
            scratch_shapes=[
                pltpu.VMEM((p.tok, p.dim), bf),
                pltpu.VMEM((p.kv, p.keys, HEAD), bf),
                pltpu.VMEM((p.kv, HEAD, p.keys), bf),
                pltpu.VMEM((64, p.tok), f32),
                pltpu.VMEM((p.tok, 64), f32),
                pltpu.VMEM(((p.group + 2) * p.kv * HEAD,), bf),
                pltpu.VMEM((p.dim,), bf),
                pltpu.VMEM((1, (p.group + 2) * p.kv * HEAD + p.dim), f32),
                pltpu.VMEM((2, p.cache, p.kv, HEAD), bf),
                pltpu.VMEM((4, p.nd, p.n, HEAD), bf),
                pltpu.VMEM((p.nd, HEAD, p.n), f32),
                pltpu.VMEM((p.mr, p.heads * HEAD), bf),
                pltpu.VMEM((p.look + 1, p.kt, p.n), f32),
                pltpu.VMEM((p.look + 1, 8, p.n), f32),
                pltpu.VMEM((p.nd, 8, p.n), f32),
                pltpu.VMEM((p.nd, 8, p.n), f32),
                pltpu.VMEM((p.owns, p.cpm, p.mr, p.cc), f32),
                pltpu.VMEM((2, 2, p.half, p.cc), f32),
                pltpu.VMEM((2, p.cpm, p.half, p.cc), bf),
                pltpu.VMEM((p.half, p.dim), bf),
                pltpu.VMEM((2, p.dim, p.wcols), bf),
                pltpu.VMEM((p.nt, p.heads * HEAD, p.wcols), bf),
                pltpu.VMEM((2, p.tok, p.kv, HEAD), bf),
                dma((4,)), dma((2,)), dma((p.nt,)), dma((8,)), dma((2,)),
                dma((3, 2)), dma((3, 2)), dma((3, 2)), dma((3, 2)),
                dma((2, p.chunks)), dma((2, p.chunks)), dma((2, 2)), dma((2, p.chunks)), dma((2, p.chunks)), dma((2, p.cpm)),
            ],
            compiler_params=pltpu.CompilerParams(collective_id=0, has_side_effects=True, vmem_limit_bytes=67_000_000),
        )(x, k_cache, v_cache, rope_table.T, norm_gain, b_qkv, w_qkv, w_out)
        return y, k_new, v_new

    return local_step


def solution(mesh):
    row_spec = P(('dp', 'cp'), None)
    cache_spec = P(('dp', 'cp'), 'tp', None)
    p = Plan(tok=1024, dim=4096, kv=2, group=12, cache=256, nm=8, kt=512)
    p.table([[8, 12, 16, 19], [16, 18, 21, 23], [20, 22, 26, 33], [32, 35, 38, 40]],
            [[35, 39, 42, 46], [38, 44, 52, 53], [54, 57, 58, 60]])
    return jax.shard_map(build(p), mesh=mesh, in_specs=(row_spec, cache_spec, cache_spec, row_spec, P(None), P(None, 'tp'), P('tp'), P('tp', None)),
                         out_specs=(row_spec, cache_spec, cache_spec), check_vma=False)
```

```python
import functools
import math

import jax
import jax.numpy as jnp
from jax import lax
from jax.experimental import pallas as pl
from jax.experimental.pallas import tpu as pltpu
from jax.sharding import PartitionSpec as P

EPS = 1.5625e-07
LOW = -1e30
HEAD = 128
QUAD = 4
MESH = pl.DeviceIdType.MESH


class Plan:
    def __init__(self, tok, dim, kv, group, cache, nm, kt):
        self.tok, self.dim, self.kv, self.group, self.cache = tok, dim, kv, group, cache
        self.nm = nm
        self.mr = tok // nm
        self.kt = kt
        self.heads = kv * group
        self.nd = self.heads // 2
        self.dpg = group // 2
        self.n = 2 * self.mr
        self.keys = tok * 5
        self.wcols = QUAD * HEAD
        self.nq = self.heads // QUAD
        self.qpg = group // QUAD
        self.hq = self.nq // 2
        self.nt = dim // self.wcols
        self.cpm = self.nt
        self.cc = self.wcols
        self.ring = self.cpm
        self.ys = 4
        self.half = self.mr // 2
        self.owns = 2
        self.fin = math.gcd(self.nd, 3)
        self.look = 3
        self.wt = self.nq * (nm // 2)
        self.s_blk = 2
        self.s_fin = self.s_blk + 4
        self.s_out = self.s_fin + 1
        self.s_q = self.s_out + self.nt
        self.nseg = self.s_q + self.hq
        self.chunks = nm * self.cpm
        self.table([[self.s_out + j + 2 * r for j in range(self.cpm)] for r in range(4)],
                   [[self.s_out + j + 8 + 2 * r for j in range(self.cpm)] for r in range(3)])

    def table(self, sums, rows):
        self.total = self.nseg * (self.nm - 1) + max(max(r) for r in sums + rows) + 1
        self.sums, self.rows = [self.words(r) for r in sums], [self.words(r) for r in rows]

    def words(self, due):
        res = [0] * (self.nseg // 5 + 1)
        for j, at in enumerate(due):
            rest = at % self.nseg
            assert res[rest // 5] >> 6 * (rest % 5) & 63 == 0
            res[rest // 5] += (1 + j + self.cpm * (at // self.nseg)) << 6 * (rest % 5)
        return res


def kernel(p, x, k_in, v_in, rope_in, gain_in, bias_in, wqkv, wout, y, kn, vn,
           h, ka, vt, rope_t, rope, b1, g1, small, cached, q, o_t, o, s_t, mx_t, m_s, l_s, own, land, yst, xb, w, wo, kv_out,
           x_sem, w_sem, wo_sem, b_sem, out_sem, cs_send, cs_recv, kv_send, kv_recv,
           rs_send, rs_recv, free_sem, ag_send, ag_recv, yl_sem):
    tp = lax.axis_index('tp')
    cp = lax.axis_index('cp')
    partner = cp + 1 - 2 * lax.rem(cp, 2)
    across = lax.rem(cp + 2, 4)
    scale = HEAD ** -0.5 * math.log2(math.e)
    new0 = p.tok * (1 + cp)
    rows4 = p.tok // 4
    goff = (p.group + 2) * HEAD * p.kv

    def wq_col(j):
        return (j // p.qpg) * (p.group + 2) * HEAD + lax.rem(j, p.qpg) * p.wcols

    def wq_copy(t):
        slot = lax.rem(t, 2)
        col = pl.multiple_of(wq_col(lax.rem(t, p.nq)), HEAD)
        return pltpu.make_async_copy(wqkv.at[:, pl.ds(col, p.wcols)], w.at[slot], w_sem.at[slot])

    def wo_copy(n):
        return pltpu.make_async_copy(wout.at[:, pl.ds(pl.multiple_of(n * p.wcols, HEAD), p.wcols)], wo.at[n], wo_sem.at[n])

    def x_copy(r):
        rows = pl.ds(r * rows4, rows4)
        return pltpu.make_async_copy(x.at[rows], h.at[rows], x_sem.at[r])

    def wkv_copy(g):
        col = g * (p.group + 2) * HEAD + p.group * HEAD
        return pltpu.make_async_copy(wqkv.at[:, pl.ds(col, 2 * HEAD)], w.at[1, :, pl.ds(g * 2 * HEAD, 2 * HEAD)], b_sem.at[g])

    x_copy(0).start()
    for g in range(p.kv):
        wkv_copy(g).start()
    little = [pltpu.make_async_copy(rope_in, rope_t, b_sem.at[2]), pltpu.make_async_copy(k_in, cached.at[0], b_sem.at[3]),
              pltpu.make_async_copy(v_in, cached.at[1], b_sem.at[4]), pltpu.make_async_copy(bias_in, b1, b_sem.at[6]),
              pltpu.make_async_copy(gain_in, g1, b_sem.at[7])]
    for c in little:
        c.start()

    barrier = pltpu.get_barrier_semaphore()
    for k in range(1, 4):
        pl.semaphore_signal(barrier, inc=1, device_id={'tp': lax.rem(tp + k, 4)}, device_id_type=MESH)
        pl.semaphore_signal(barrier, inc=1, device_id={'cp': lax.rem(cp + k, 4)}, device_id_type=MESH)

    def cache_copies(owner, peer, k):
        at = pl.multiple_of(owner * p.cache, p.cache)
        ks = ka.at[:, pl.ds(at, p.cache)]
        vs = vt.at[:, :, pl.ds(at, p.cache)]
        return (pltpu.make_async_remote_copy(ks, ks, cs_send.at[k, 0], cs_recv.at[k, 0], device_id={'cp': peer}, device_id_type=MESH),
                pltpu.make_async_remote_copy(vs, vs, cs_send.at[k, 1], cs_recv.at[k, 1], device_id={'cp': peer}, device_id_type=MESH))

    def new_copies(at, size, peer, k):
        ks = ka.at[:, pl.ds(at, size)]
        vs = vt.at[:, :, pl.ds(at, size)]
        return (pltpu.make_async_remote_copy(ks, ks, kv_send.at[k, 0], kv_recv.at[k, 0], device_id={'cp': peer}, device_id_type=MESH),
                pltpu.make_async_remote_copy(vs, vs, kv_send.at[k, 1], kv_recv.at[k, 1], device_id={'cp': peer}, device_id_type=MESH))

    for c in little:
        c.wait()
    here = pl.multiple_of(cp * p.cache, p.cache)
    for g in range(p.kv):
        ka[g, pl.ds(here, p.cache), :] = cached[0].astype(jnp.float32)[:, g, :].astype(jnp.bfloat16)
        vt[g, :, pl.ds(here, p.cache)] = cached[1].astype(jnp.float32)[:, g, :].T.astype(jnp.bfloat16)
    small[0:1, 0:goff] = b1[...].astype(jnp.float32).reshape(1, goff)
    small[0:1, goff:goff + p.dim] = g1[...].astype(jnp.float32).reshape(1, p.dim)
    rope[...] = rope_t[...].T
    pl.semaphore_wait(barrier, 6)
    for peer, k in ((across, 1), (partner, 0)):
        for c in cache_copies(cp, peer, k):
            c.start()

    def send_new(r):
        at = pl.multiple_of(new0 + r * rows4, rows4)

        @pl.when(cp < 2)
        def _():
            for c in new_copies(at, rows4, across, 1):
                c.start()

        @pl.when(lax.rem(cp, 2) == 0)
        def _():
            for c in new_copies(at, rows4, partner, 0):
                c.start()

    lane = lax.broadcasted_iota(jnp.int32, (1, HEAD), 1)
    even = lax.rem(lane, 2) == 0
    turned = lane < 64

    def angles(rows, count):
        r = rope[rows, :]
        both = jnp.concatenate([r, r], axis=1)
        at = lax.broadcasted_iota(jnp.int32, (count, HEAD), 1)
        pair = lax.rem(at, 64) // 2
        c = jnp.take_along_axis(both, pair, axis=1)
        s = jnp.take_along_axis(both, pair + 32, axis=1)
        return c, jnp.where(even, -s, s)

    def rotate(a, c, s):
        swap = jnp.where(even, pltpu.roll(a, HEAD - 1, 1), pltpu.roll(a, 1, 1))
        return jnp.where(turned, a * c + swap * s, a)

    for g in range(p.kv):
        wkv_copy(g).wait()
    for r in range(1, 4):
        x_copy(r).start()
    wq_copy(0).start()
    nsub = max(1, rows4 // 128)
    sub = rows4 // nsub
    wide = 512

    def norm(b):
        rows = pl.ds(pl.multiple_of(b * sub, sub), sub)
        total = None
        for c in range(0, p.dim, wide):
            v = h[rows, c:c + wide].astype(jnp.float32)
            v = v * v
            for k in range(0, wide, HEAD):
                total = v[:, k:k + HEAD] if total is None else total + v[:, k:k + HEAD]
        inv = lax.rsqrt(jnp.sum(total, axis=1, keepdims=True) * (1.0 / p.dim) + EPS)
        for c in range(0, p.dim, wide):
            v = h[rows, c:c + wide].astype(jnp.float32)
            h[rows, c:c + wide] = (v * inv * small[0:1, goff + c:goff + c + wide]).astype(jnp.bfloat16)

    def keys_values(r, ahead):
        rows = pl.ds(pl.multiple_of(r * rows4, rows4), rows4)
        at = pl.multiple_of(new0 + r * rows4, rows4)
        a = jnp.dot(h[rows, :], w[1], preferred_element_type=jnp.float32)
        if ahead:
            for b in range(nsub):
                norm((r + 1) * nsub + b)
        c, s = angles(rows, rows4)
        keys, vals = [], []
        for g in range(p.kv):
            col = g * (p.group + 2) * HEAD + p.group * HEAD
            keys.append(rotate(a[:, g * 2 * HEAD:g * 2 * HEAD + HEAD] + small[0:1, col:col + HEAD], c, s))
            vals.append(a[:, g * 2 * HEAD + HEAD:(g + 1) * 2 * HEAD] + small[0:1, col + HEAD:col + 2 * HEAD])
            ka[g, pl.ds(at, rows4), :] = keys[g].astype(jnp.bfloat16)
            vt[g, :, pl.ds(at, rows4)] = vals[g].T.astype(jnp.bfloat16)
        kv_out[0, rows] = jnp.swapaxes(jnp.stack(keys), 0, 1).astype(jnp.bfloat16)
        kv_out[1, rows] = jnp.swapaxes(jnp.stack(vals), 0, 1).astype(jnp.bfloat16)

    def kv_step(r, _):
        x_copy(r + 1).wait()

        @pl.when(r > 0)
        def _():
            send_new(r - 1)

        keys_values(r, True)
        return 0

    x_copy(0).wait()
    for b in range(nsub):
        norm(b)
    lax.fori_loop(0, 3, kv_step, 0)
    send_new(2)
    keys_values(3, False)
    wq_copy(1).start()
    send_new(3)

    def out_copies():
        return [pltpu.make_async_copy(kv_out.at[0], kn, out_sem.at[0]), pltpu.make_async_copy(kv_out.at[1], vn, out_sem.at[1])]

    for c in out_copies():
        c.start()

    def reset(i, _):
        m_s[i] = jnp.full((8, p.n), LOW, jnp.float32)
        l_s[i] = jnp.zeros((8, p.n), jnp.float32)
        o_t[i] = jnp.zeros((HEAD, p.n), jnp.float32)
        return 0

    lax.fori_loop(0, p.nd, reset, 0)

    def q_tile(t):
        j = lax.rem(t, p.nq)
        first = t // p.nq * 2
        count = 2
        rows = pl.ds(pl.multiple_of(first * p.mr, p.mr), count * p.mr)
        wq_copy(t).wait()
        a = jnp.dot(h[rows, :], w[lax.rem(t, 2)], preferred_element_type=jnp.float32)
        a = a + small[0:1, pl.ds(pl.multiple_of(wq_col(j), HEAD), p.wcols)]
        c, s = angles(rows, count * p.mr)
        for k in range(QUAD):
            b = rotate(a[:, k * HEAD:(k + 1) * HEAD], c, s).astype(jnp.bfloat16)
            for u in range(count):
                q[lax.rem(first + u, 4), 2 * j + k // 2, (k % 2) * p.mr:(k % 2 + 1) * p.mr, :] = b[u * p.mr:(u + 1) * p.mr, :]

        @pl.when(t + 2 < p.wt)
        def _():
            wq_copy(t + 2).start()

    part_rows = min(256, p.kt)
    row_of = lax.rem(lax.broadcasted_iota(jnp.int32, (p.kt, p.n), 1), p.mr) - lax.broadcasted_iota(jnp.int32, (p.kt, p.n), 0)

    def scores(qs, pair, off, k, bound):
        g = pair // p.dpg
        s = lax.dot_general(ka[g, pl.ds(pl.multiple_of(off, p.kt), p.kt), :], q[qs, pair], (((1,), (1,)), ((), ())),
                            preferred_element_type=jnp.float32) * scale
        if bound is not None:
            s = jnp.where(row_of >= -bound, s, LOW)
        s_t[k] = s
        mx_t[k] = jnp.max(s.reshape(p.kt // 8, 8, p.n), axis=0)

    def weigh(pair, off, k):
        g = pair // p.dpg
        m_old = m_s[pair, 0:1, :]
        m_new = jnp.maximum(m_old, jnp.max(mx_t[k], axis=0, keepdims=True))
        alpha = jnp.exp2(m_old - m_new)
        m_s[pair, 0:1, :] = m_new
        acc = None
        es = []
        for r in range(0, p.kt, part_rows):
            e = jnp.exp2(s_t[k, r:r + part_rows, :] - m_new)
            part = jnp.sum(e.reshape(part_rows // 8, 8, p.n), axis=0)
            acc = part if acc is None else acc + part
            es.append(e.astype(jnp.bfloat16))
        d = jnp.dot(vt[g, :, pl.ds(pl.multiple_of(off, p.kt), p.kt)], jnp.concatenate(es, axis=0), preferred_element_type=jnp.float32)
        l_s[pair] = l_s[pair] * alpha + acc
        o_t[pair] = o_t[pair] * alpha + d

    anything = 1 << 20
    slots = p.look + 1

    def own_at(j):
        return new0 + j * p.kt

    def own_segment(u, j, tiles):
        qs = lax.rem(u, 4)
        bound = u * p.mr - j * p.kt
        more = j + 1 < tiles

        @pl.when(j == 0)
        def _():
            for i in range(p.look):
                scores(qs, i, new0, i, u * p.mr)

        for i in range(p.nd):
            n = i + p.look
            if n < p.nd:
                scores(qs, n, own_at(j), n % slots, bound)
            else:
                n -= p.nd
                scores(qs, jnp.where(more, n, n // 2), jnp.where(more, own_at(j + 1), (n % 2) * p.kt), (n + p.nd) % slots,
                       jnp.where(more, bound - p.kt, anything))
            weigh(i, own_at(j), i % slots)

    def block_at(b):
        return jnp.where(b == 0, 0, p.tok * (1 + jnp.where(lax.rem(cp, 2) == 1, cp - b, b - 1)))

    def block_segment(u, b, count):
        qs = lax.rem(u, 4)
        at = block_at(b)
        following = jnp.where((u > 0) & (b + 1 < count), block_at(b + 1), 0)

        @pl.when((u == 0) & (b > 0))
        def _():
            for i in range(p.look):
                scores(qs, i // 2, at + (i % 2) * p.kt, i, None)

        for i in range(2 * p.nd):
            n = i + p.look
            scores(qs, (n // 2) % p.nd, (at if n < 2 * p.nd else following) + (n % 2) * p.kt, n % slots, None)
            weigh(i // 2, at + (i % 2) * p.kt, i % slots)

    blocks = 1 + cp

    role_a = 3 - tp
    role_b = tp

    def chain(d, i):
        m = i // p.cpm
        j = lax.rem(i, p.cpm)
        mine = own.at[lax.rem(m, p.owns), j, pl.ds(d * p.half, p.half)]
        rows = pl.ds(pl.multiple_of(m * p.mr + d * p.half, p.half), p.half)
        cols = pl.ds(pl.multiple_of(j * p.cc, p.cc), p.cc)
        return mine, land.at[d, lax.rem(i, p.ring)], y.at[rows, cols]

    def peers(d):
        return (jnp.maximum(tp - 1, 0), jnp.minimum(tp + 1, 3)) if d == 0 else (jnp.minimum(tp + 1, 3), jnp.maximum(tp - 1, 0))

    def rs_copy(d, i):
        mine, there, _ = chain(d, i)
        return pltpu.make_async_remote_copy(mine, there, rs_send.at[d, lax.rem(i, p.owns * p.cpm)], rs_recv.at[d, lax.rem(i, p.ring)],
                                            device_id={'tp': peers(d)[0]}, device_id_type=MESH)

    def ag_copy(d, i, src=None):
        out = chain(d, i)[2]
        return pltpu.make_async_remote_copy(out if src is None else src, out, ag_send.at[d, i], ag_recv.at[d, i],
                                            device_id={'tp': peers(d)[1]}, device_id_type=MESH)

    def yl_copy(d, i):
        k = lax.rem(i, p.ys)
        return pltpu.make_async_copy(yst.at[d, k], chain(d, i)[2], yl_sem.at[d, k])

    def pick(role, table):
        res = []
        for k in range(len(table[0])):
            v = table[0][k]
            for r in range(1, len(table)):
                v = jnp.where(role == r, table[r][k], v)
            res.append(v)
        return res

    due = [(d, role, pick(role, p.sums), pick(2 - role, p.rows)) for d, role in ((0, role_a), (1, role_b))]

    def when_due(seg, words, act):
        rest = lax.rem(seg, p.nseg)
        w = words[0]
        for k in range(1, len(words)):
            w = jnp.where(rest >= 5 * k, words[k], w)
        code = jnp.bitwise_and(jnp.right_shift(w, 6 * lax.rem(rest, 5)), 63) - 1
        m = seg // p.nseg - jnp.maximum(code, 0) // p.cpm

        @pl.when((code >= 0) & (m >= 0) & (m < p.nm))
        def _():
            act(m * p.cpm + lax.rem(code, p.cpm))

    def service(seg):
        for d, role, sum_words, _ in due:
            def sums(i, d=d, role=role):
                mine, arrived, _ = chain(d, i)

                @pl.when(role > 0)
                def _():
                    rs_copy(d, i).wait_recv()

                @pl.when((role > 0) & (role < 3))
                def _():
                    mine[...] = mine[...] + arrived[...]

                @pl.when((role < 3) & (i >= p.ring))
                def _():
                    pl.semaphore_wait(free_sem.at[d], 1)

                @pl.when(role < 3)
                def _():
                    rs_copy(d, i).start()

                @pl.when(role == 3)
                def _():
                    k = lax.rem(i, p.ys)

                    @pl.when(i >= p.ys)
                    def _():
                        yl_copy(d, i - p.ys).wait()
                        ag_copy(d, i - p.ys, yst.at[d, k]).wait_send()

                    yst[d, k] = (mine[...] + arrived[...]).astype(jnp.bfloat16)
                    yl_copy(d, i).start()
                    ag_copy(d, i, yst.at[d, k]).start()

                @pl.when((role > 0) & (i < p.chunks - p.ring))
                def _():
                    pl.semaphore_signal(free_sem.at[d], inc=1, device_id={'tp': peers(d)[1]}, device_id_type=MESH)

            when_due(seg, sum_words, sums)

        for d, role, _, row_words in due:
            def rows(i, d=d, role=role):
                @pl.when(role < 3)
                def _():
                    ag_copy(d, i).wait_recv()

                @pl.when((role < 3) & (role > 0))
                def _():
                    ag_copy(d, i).start()

            when_due(seg, row_words, rows)

    take_a = jnp.where(tp == 0, 1, 0).astype(jnp.float32)
    take_b = jnp.where(tp == 3, 1, 0).astype(jnp.float32)
    x_half = jnp.where(tp == 3, p.half, 0)

    def xb_copy(m):
        return pltpu.make_async_copy(x.at[pl.ds(pl.multiple_of(m * p.mr + x_half, p.half), p.half)], xb, b_sem.at[5])

    def first_q(t, _):
        q_tile(t)

        @pl.when(t == max(0, p.nq - 3))
        def _():
            for n in range(p.nt):
                wo_copy(n).start()

        return 0

    lax.fori_loop(0, p.nq, first_q, 0)

    for c in cache_copies(across, partner, 1):
        c.wait_recv()
    for c in cache_copies(across, partner, 2):
        c.start()
    for k in (0, 2):
        for c in cache_copies(cp, partner, k):
            c.wait_recv()

    def segment(seg, _):
        m = seg // p.nseg
        s = lax.rem(seg, p.nseg)
        busy = m < p.nm
        tiles = (m * p.mr + p.mr + p.kt - 1) // p.kt

        @pl.when(busy & (s < tiles) & (s < p.s_blk))
        def _():
            @pl.when(s == 0)
            def _():
                xb_copy(m).start()

            own_segment(m, s, tiles)

        @pl.when((seg == p.s_blk + 1) & (lax.rem(cp, 2) == 1))
        def _():
            for c in new_copies(pl.multiple_of(p.tok * cp, p.tok), p.tok, partner, 0):
                c.wait_recv()

        @pl.when((cp >= 2) & (seg == p.s_blk + cp - 1))
        def _():
            direct = pl.multiple_of(p.tok * (cp - 1), p.tok)
            for c in new_copies(direct, p.tok, partner, 1):
                c.wait_recv()
            for c in new_copies(direct, p.tok, partner, 2):
                c.start()

        @pl.when((cp >= 2) & (seg == p.s_blk + cp))
        def _():
            for c in new_copies(pl.multiple_of(p.tok * (cp - 1), p.tok), p.tok, partner, 2):
                c.wait_recv()

        @pl.when(busy & (s >= p.s_blk) & (s < p.s_blk + blocks))
        def _():
            block_segment(m, s - p.s_blk, blocks)

        @pl.when(busy & (s == p.s_fin))
        def _():
            def finish(i, _):
                for e in range(p.fin):
                    c = i * p.fin + e
                    v = o_t[c] * (1.0 / jnp.sum(l_s[c], axis=0, keepdims=True))
                    for k in range(2):
                        o[:, pl.ds(pl.multiple_of((c * 2 + k) * HEAD, HEAD), HEAD)] = v[:, k * p.mr:(k + 1) * p.mr].T.astype(jnp.bfloat16)
                    reset(c, 0)
                return 0

            lax.fori_loop(0, p.nd // p.fin, finish, 0)

        @pl.when(busy & (s >= p.s_out) & (s < p.s_q))
        def _():
            n = s - p.s_out

            @pl.when(n == 0)
            def _():
                xb_copy(m).wait()

            @pl.when((n == 0) & (m >= p.owns))
            def _():
                for d, role in ((0, role_a), (1, role_b)):
                    @pl.when(role < 3)
                    def _():
                        for j in range(p.cpm):
                            rs_copy(d, (m - p.owns) * p.cpm + j).wait_send()

            @pl.when(m == 0)
            def _():
                wo_copy(n).wait()

            a = jnp.dot(o[...], wo[n], preferred_element_type=jnp.float32)
            r = xb[:, pl.ds(pl.multiple_of(n * p.wcols, HEAD), p.wcols)].astype(jnp.float32)
            own[lax.rem(m, p.owns), n, 0:p.half, :] = a[0:p.half] + r * take_a
            own[lax.rem(m, p.owns), n, p.half:p.mr, :] = a[p.half:p.mr] + r * take_b

        @pl.when((m < p.nm - 2) & (s >= p.s_q))
        def _():
            q_tile((m // 2 + 1) * p.nq + lax.rem(m, 2) * p.hq + s - p.s_q)

        service(seg)
        return 0

    lax.fori_loop(0, p.total, segment, 0)

    for d, role in ((0, role_a), (1, role_b)):
        @pl.when(role < 3)
        def _():
            def last_sums(i, _):
                rs_copy(d, i).wait_send()
                return 0
            lax.fori_loop((p.nm - p.owns) * p.cpm, p.chunks, last_sums, 0)

        @pl.when((role > 0) & (role < 3))
        def _():
            def last_rows(i, _):
                ag_copy(d, i).wait_send()
                return 0
            lax.fori_loop(0, p.chunks, last_rows, 0)

        @pl.when(role == 3)
        def _():
            for k in range(p.ys):
                i = p.chunks - p.ys + k
                yl_copy(d, i).wait()
                ag_copy(d, i, yst.at[d, k]).wait_send()

    for c in out_copies():
        c.wait()
    for k in (0, 1):
        for c in cache_copies(cp, partner, k):
            c.wait_send()
    for c in cache_copies(across, partner, 2):
        c.wait_send()

    @pl.when(cp < 2)
    def _():
        for c in new_copies(new0, p.tok, across, 1):
            c.wait_send()

    @pl.when(lax.rem(cp, 2) == 0)
    def _():
        for c in new_copies(new0, p.tok, partner, 0):
            c.wait_send()

    @pl.when(cp >= 2)
    def _():
        for c in new_copies(pl.multiple_of(p.tok * (cp - 1), p.tok), p.tok, partner, 2):
            c.wait_send()


def build(p):
    def local_step(x, k_cache, v_cache, rope_table, norm_gain, w_qkv, b_qkv, w_out):
        anyspace = pl.BlockSpec(memory_space=pl.ANY)
        bf, f32 = jnp.bfloat16, jnp.float32
        dma = pltpu.SemaphoreType.DMA
        kv_shape = jax.ShapeDtypeStruct((p.tok, p.kv, HEAD), bf)
        y, k_new, v_new = pl.pallas_call(
            functools.partial(kernel, p),
            name='block',
            out_shape=(jax.ShapeDtypeStruct((p.tok, p.dim), bf), kv_shape, kv_shape),
            in_specs=[anyspace] * 8,
            out_specs=(anyspace, anyspace, anyspace),
            scratch_shapes=[
                pltpu.VMEM((p.tok, p.dim), bf),
                pltpu.VMEM((p.kv, p.keys, HEAD), bf),
                pltpu.VMEM((p.kv, HEAD, p.keys), bf),
                pltpu.VMEM((64, p.tok), f32),
                pltpu.VMEM((p.tok, 64), f32),
                pltpu.VMEM(((p.group + 2) * p.kv * HEAD,), bf),
                pltpu.VMEM((p.dim,), bf),
                pltpu.VMEM((1, (p.group + 2) * p.kv * HEAD + p.dim), f32),
                pltpu.VMEM((2, p.cache, p.kv, HEAD), bf),
                pltpu.VMEM((4, p.nd, p.n, HEAD), bf),
                pltpu.VMEM((p.nd, HEAD, p.n), f32),
                pltpu.VMEM((p.mr, p.heads * HEAD), bf),
                pltpu.VMEM((p.look + 1, p.kt, p.n), f32),
                pltpu.VMEM((p.look + 1, 8, p.n), f32),
                pltpu.VMEM((p.nd, 8, p.n), f32),
                pltpu.VMEM((p.nd, 8, p.n), f32),
                pltpu.VMEM((p.owns, p.cpm, p.mr, p.cc), f32),
                pltpu.VMEM((2, p.ring, p.half, p.cc), f32),
                pltpu.VMEM((2, p.ys, p.half, p.cc), bf),
                pltpu.VMEM((p.half, p.dim), bf),
                pltpu.VMEM((2, p.dim, p.wcols), bf),
                pltpu.VMEM((p.nt, p.heads * HEAD, p.wcols), bf),
                pltpu.VMEM((2, p.tok, p.kv, HEAD), bf),
                dma((4,)), dma((2,)), dma((p.nt,)), dma((8,)), dma((2,)),
                dma((3, 2)), dma((3, 2)), dma((3, 2)), dma((3, 2)),
                dma((2, p.owns * p.cpm)), dma((2, p.ring)), pltpu.SemaphoreType.REGULAR((2,)), dma((2, p.chunks)), dma((2, p.chunks)), dma((2, p.ys)),
            ],
            compiler_params=pltpu.CompilerParams(collective_id=0, has_side_effects=True, vmem_limit_bytes=67_000_000),
        )(x, k_cache, v_cache, rope_table.T, norm_gain, b_qkv, w_qkv, w_out)
        return y, k_new, v_new

    return local_step


def solution(mesh):
    row_spec = P(('dp', 'cp'), None)
    cache_spec = P(('dp', 'cp'), 'tp', None)
    p = Plan(tok=1024, dim=4096, kv=2, group=12, cache=256, nm=8, kt=512)
    p.table([[7, 10, 15, 16, 17, 19, 20, 21], [15, 17, 19, 20, 21, 22, 23, 28], [18, 20, 21, 22, 23, 27, 32, 33], [20, 22, 24, 29, 32, 34, 35, 37]],
            [[28, 32, 33, 36, 37, 38, 39, 40], [35, 36, 37, 38, 39, 40, 42, 46], [37, 38, 39, 40, 41, 47, 50, 52]])
    return jax.shard_map(build(p), mesh=mesh, in_specs=(row_spec, cache_spec, cache_spec, row_spec, P(None), P(None, 'tp'), P('tp'), P('tp', None)),
                         out_specs=(row_spec, cache_spec, cache_spec), check_vma=False)
```

```python
import functools
import math

import jax
import jax.numpy as jnp
from jax import lax
from jax.experimental import pallas as pl
from jax.experimental.pallas import tpu as pltpu
from jax.sharding import PartitionSpec as P

EPS = 1.5625e-07
LOW = -1e30
HEAD = 128
QUAD = 4
MESH = pl.DeviceIdType.MESH


class Plan:
    def __init__(self, tok, dim, kv, group, cache, nm, kt):
        self.tok, self.dim, self.kv, self.group, self.cache = tok, dim, kv, group, cache
        self.nm = nm
        self.mr = tok // nm
        self.kt = kt
        self.heads = kv * group
        self.nd = self.heads // 2
        self.dpg = group // 2
        self.n = 2 * self.mr
        self.keys = tok * 5
        self.wcols = QUAD * HEAD
        self.nq = self.heads // QUAD
        self.qpg = group // QUAD
        self.hq = self.nq // 2
        self.nt = dim // self.wcols
        self.cpm = self.nt
        self.cc = self.wcols
        self.ring = self.cpm
        self.ys = 4
        self.half = self.mr // 2
        self.owns = 2
        self.fin = math.gcd(self.nd, 3)
        self.look = 3
        self.wt = self.nq * (nm // 2)
        self.s_blk = 2
        self.s_fin = self.s_blk + 4
        self.s_out = self.s_fin + 1
        self.s_q = self.s_out + self.nt
        self.nseg = self.s_q + self.hq
        self.chunks = nm * self.cpm
        self.table([[self.s_out + j + 2 * r for j in range(self.cpm)] for r in range(4)],
                   [[self.s_out + j + 8 + 2 * r for j in range(self.cpm)] for r in range(3)])

    def table(self, sums, rows):
        self.total = self.nseg * (self.nm - 1) + max(max(r) for r in sums + rows) + 1
        self.sums, self.rows = [self.words(r) for r in sums], [self.words(r) for r in rows]

    def words(self, due):
        res = [0] * (self.nseg // 5 + 1)
        for j, at in enumerate(due):
            rest = at % self.nseg
            assert res[rest // 5] >> 6 * (rest % 5) & 63 == 0
            res[rest // 5] += (1 + j + self.cpm * (at // self.nseg)) << 6 * (rest % 5)
        return res


def kernel(p, x, k_in, v_in, rope_in, gain_in, bias_in, wqkv, wout, y, kn, vn,
           h, ka, vt, rope_t, rope, b1, g1, small, cached, q, o_t, o, s_t, mx_t, m_s, l_s, own, land, yst, xb, w, wo, kv_out,
           x_sem, w_sem, wo_sem, b_sem, out_sem, cs_send, cs_recv, kv_send, kv_recv,
           rs_send, rs_recv, free_sem, ag_send, ag_recv, yl_sem):
    tp = lax.axis_index('tp')
    cp = lax.axis_index('cp')
    partner = cp + 1 - 2 * lax.rem(cp, 2)
    across = lax.rem(cp + 2, 4)
    scale = HEAD ** -0.5 * math.log2(math.e)
    new0 = p.tok * (1 + cp)
    rows4 = p.tok // 4
    goff = (p.group + 2) * HEAD * p.kv

    def wq_col(j):
        return (j // p.qpg) * (p.group + 2) * HEAD + lax.rem(j, p.qpg) * p.wcols

    def wq_copy(t):
        slot = lax.rem(t, 2)
        col = pl.multiple_of(wq_col(lax.rem(t, p.nq)), HEAD)
        return pltpu.make_async_copy(wqkv.at[:, pl.ds(col, p.wcols)], w.at[slot], w_sem.at[slot])

    def wo_copy(n):
        return pltpu.make_async_copy(wout.at[:, pl.ds(pl.multiple_of(n * p.wcols, HEAD), p.wcols)], wo.at[n], wo_sem.at[n])

    def x_copy(r):
        rows = pl.ds(r * rows4, rows4)
        return pltpu.make_async_copy(x.at[rows], h.at[rows], x_sem.at[r])

    def wkv_copy(g):
        col = g * (p.group + 2) * HEAD + p.group * HEAD
        return pltpu.make_async_copy(wqkv.at[:, pl.ds(col, 2 * HEAD)], w.at[1, :, pl.ds(g * 2 * HEAD, 2 * HEAD)], b_sem.at[g])

    x_copy(0).start()
    for g in range(p.kv):
        wkv_copy(g).start()
    little = [pltpu.make_async_copy(rope_in, rope_t, b_sem.at[2]), pltpu.make_async_copy(k_in, cached.at[0], b_sem.at[3]),
              pltpu.make_async_copy(v_in, cached.at[1], b_sem.at[4]), pltpu.make_async_copy(bias_in, b1, b_sem.at[6]),
              pltpu.make_async_copy(gain_in, g1, b_sem.at[7])]
    for c in little:
        c.start()

    barrier = pltpu.get_barrier_semaphore()
    for k in range(1, 4):
        pl.semaphore_signal(barrier, inc=1, device_id={'tp': lax.rem(tp + k, 4)}, device_id_type=MESH)
        pl.semaphore_signal(barrier, inc=1, device_id={'cp': lax.rem(cp + k, 4)}, device_id_type=MESH)

    def cache_copies(owner, peer, k):
        at = pl.multiple_of(owner * p.cache, p.cache)
        ks = ka.at[:, pl.ds(at, p.cache)]
        vs = vt.at[:, :, pl.ds(at, p.cache)]
        return (pltpu.make_async_remote_copy(ks, ks, cs_send.at[k, 0], cs_recv.at[k, 0], device_id={'cp': peer}, device_id_type=MESH),
                pltpu.make_async_remote_copy(vs, vs, cs_send.at[k, 1], cs_recv.at[k, 1], device_id={'cp': peer}, device_id_type=MESH))

    def new_copies(at, size, peer, k):
        ks = ka.at[:, pl.ds(at, size)]
        vs = vt.at[:, :, pl.ds(at, size)]
        return (pltpu.make_async_remote_copy(ks, ks, kv_send.at[k, 0], kv_recv.at[k, 0], device_id={'cp': peer}, device_id_type=MESH),
                pltpu.make_async_remote_copy(vs, vs, kv_send.at[k, 1], kv_recv.at[k, 1], device_id={'cp': peer}, device_id_type=MESH))

    for c in little:
        c.wait()
    here = pl.multiple_of(cp * p.cache, p.cache)
    for g in range(p.kv):
        ka[g, pl.ds(here, p.cache), :] = cached[0].astype(jnp.float32)[:, g, :].astype(jnp.bfloat16)
        vt[g, :, pl.ds(here, p.cache)] = cached[1].astype(jnp.float32)[:, g, :].T.astype(jnp.bfloat16)
    small[0:1, 0:goff] = b1[...].astype(jnp.float32).reshape(1, goff)
    small[0:1, goff:goff + p.dim] = g1[...].astype(jnp.float32).reshape(1, p.dim)
    rope[...] = rope_t[...].T
    pl.semaphore_wait(barrier, 6)
    for peer, k in ((across, 1), (partner, 0)):
        for c in cache_copies(cp, peer, k):
            c.start()

    def send_new(r):
        at = pl.multiple_of(new0 + r * rows4, rows4)

        @pl.when(cp == 0)
        def _():
            for c in new_copies(at, rows4, across, 1):
                c.start()

        @pl.when(lax.rem(cp, 2) == 0)
        def _():
            for c in new_copies(at, rows4, partner, 0):
                c.start()

    lane = lax.broadcasted_iota(jnp.int32, (1, HEAD), 1)
    even = lax.rem(lane, 2) == 0
    turned = lane < 64

    def angles(rows, count):
        r = rope[rows, :]
        both = jnp.concatenate([r, r], axis=1)
        at = lax.broadcasted_iota(jnp.int32, (count, HEAD), 1)
        pair = lax.rem(at, 64) // 2
        c = jnp.take_along_axis(both, pair, axis=1)
        s = jnp.take_along_axis(both, pair + 32, axis=1)
        return c, jnp.where(even, -s, s)

    def rotate(a, c, s):
        swap = jnp.where(even, pltpu.roll(a, HEAD - 1, 1), pltpu.roll(a, 1, 1))
        return jnp.where(turned, a * c + swap * s, a)

    for g in range(p.kv):
        wkv_copy(g).wait()
    for r in range(1, 4):
        x_copy(r).start()
    wq_copy(0).start()
    nsub = max(8, rows4 // 32)
    sub = rows4 // nsub
    wide = 512

    def norm(b):
        rows = pl.ds(pl.multiple_of(b * sub, sub), sub)
        total = None
        for c in range(0, p.dim, wide):
            v = h[rows, c:c + wide].astype(jnp.float32)
            v = v * v
            for k in range(0, wide, HEAD):
                total = v[:, k:k + HEAD] if total is None else total + v[:, k:k + HEAD]
        inv = lax.rsqrt(jnp.sum(total, axis=1, keepdims=True) * (1.0 / p.dim) + EPS)
        for c in range(0, p.dim, wide):
            v = h[rows, c:c + wide].astype(jnp.float32)
            h[rows, c:c + wide] = (v * inv * small[0:1, goff + c:goff + c + wide]).astype(jnp.bfloat16)

    def keys_values(r, ahead):
        rows = pl.ds(pl.multiple_of(r * rows4, rows4), rows4)
        at = pl.multiple_of(new0 + r * rows4, rows4)
        a = None
        per = nsub // 8
        deep = p.dim // 8
        for e in range(8):
            part = jnp.dot(h[rows, e * deep:(e + 1) * deep], w[1, e * deep:(e + 1) * deep, :], preferred_element_type=jnp.float32)
            a = part if a is None else a + part
            if ahead:
                for b in range(per):
                    norm((r + 1) * nsub + e * per + b)
        c, s = angles(rows, rows4)
        keys, vals = [], []
        for g in range(p.kv):
            col = g * (p.group + 2) * HEAD + p.group * HEAD
            keys.append(rotate(a[:, g * 2 * HEAD:g * 2 * HEAD + HEAD] + small[0:1, col:col + HEAD], c, s))
            vals.append(a[:, g * 2 * HEAD + HEAD:(g + 1) * 2 * HEAD] + small[0:1, col + HEAD:col + 2 * HEAD])
            ka[g, pl.ds(at, rows4), :] = keys[g].astype(jnp.bfloat16)
            vt[g, :, pl.ds(at, rows4)] = vals[g].T.astype(jnp.bfloat16)
        kv_out[0, rows] = jnp.swapaxes(jnp.stack(keys), 0, 1).astype(jnp.bfloat16)
        kv_out[1, rows] = jnp.swapaxes(jnp.stack(vals), 0, 1).astype(jnp.bfloat16)

    def kv_step(r, _):
        x_copy(r + 1).wait()

        @pl.when(r > 0)
        def _():
            send_new(r - 1)

        keys_values(r, True)
        return 0

    x_copy(0).wait()
    for b in range(nsub):
        norm(b)
    lax.fori_loop(0, 3, kv_step, 0)
    send_new(2)
    keys_values(3, False)
    wq_copy(1).start()
    send_new(3)

    @pl.when(cp == 1)
    def _():
        for c in new_copies(new0, p.tok, across, 1):
            c.start()

    def out_copies():
        return [pltpu.make_async_copy(kv_out.at[0], kn, out_sem.at[0]), pltpu.make_async_copy(kv_out.at[1], vn, out_sem.at[1])]

    for c in out_copies():
        c.start()

    def reset(i, _):
        m_s[i] = jnp.full((8, p.n), LOW, jnp.float32)
        l_s[i] = jnp.zeros((8, p.n), jnp.float32)
        o_t[i] = jnp.zeros((HEAD, p.n), jnp.float32)
        return 0

    lax.fori_loop(0, p.nd, reset, 0)

    def q_tile(t):
        j = lax.rem(t, p.nq)
        first = t // p.nq * 2
        count = 2
        rows = pl.ds(pl.multiple_of(first * p.mr, p.mr), count * p.mr)
        wq_copy(t).wait()
        a = jnp.dot(h[rows, :], w[lax.rem(t, 2)], preferred_element_type=jnp.float32)
        a = a + small[0:1, pl.ds(pl.multiple_of(wq_col(j), HEAD), p.wcols)]
        c, s = angles(rows, count * p.mr)
        for k in range(QUAD):
            b = rotate(a[:, k * HEAD:(k + 1) * HEAD], c, s).astype(jnp.bfloat16)
            for u in range(count):
                q[lax.rem(first + u, 4), 2 * j + k // 2, (k % 2) * p.mr:(k % 2 + 1) * p.mr, :] = b[u * p.mr:(u + 1) * p.mr, :]

        @pl.when(t + 2 < p.wt)
        def _():
            wq_copy(t + 2).start()

    part_rows = min(256, p.kt)
    row_of = lax.rem(lax.broadcasted_iota(jnp.int32, (p.kt, p.n), 1), p.mr) - lax.broadcasted_iota(jnp.int32, (p.kt, p.n), 0)

    def scores(qs, pair, off, k, bound):
        g = pair // p.dpg
        s = lax.dot_general(ka[g, pl.ds(pl.multiple_of(off, p.kt), p.kt), :], q[qs, pair], (((1,), (1,)), ((), ())),
                            preferred_element_type=jnp.float32) * scale
        if bound is not None:
            s = jnp.where(row_of >= -bound, s, LOW)
        s_t[k] = s
        mx_t[k] = jnp.max(s.reshape(p.kt // 8, 8, p.n), axis=0)

    def weigh(pair, off, k):
        g = pair // p.dpg
        m_old = m_s[pair, 0:1, :]
        m_new = jnp.maximum(m_old, jnp.max(mx_t[k], axis=0, keepdims=True))
        alpha = jnp.exp2(m_old - m_new)
        m_s[pair, 0:1, :] = m_new
        acc = None
        es = []
        for r in range(0, p.kt, part_rows):
            e = jnp.exp2(s_t[k, r:r + part_rows, :] - m_new)
            part = jnp.sum(e.reshape(part_rows // 8, 8, p.n), axis=0)
            acc = part if acc is None else acc + part
            es.append(e.astype(jnp.bfloat16))
        d = jnp.dot(vt[g, :, pl.ds(pl.multiple_of(off, p.kt), p.kt)], jnp.concatenate(es, axis=0), preferred_element_type=jnp.float32)
        l_s[pair] = l_s[pair] * alpha + acc
        o_t[pair] = o_t[pair] * alpha + d

    anything = 1 << 20
    slots = p.look + 1

    def own_at(j):
        return new0 + j * p.kt

    def own_segment(u, j, tiles):
        qs = lax.rem(u, 4)
        bound = u * p.mr - j * p.kt
        more = j + 1 < tiles

        @pl.when(j == 0)
        def _():
            for i in range(p.look):
                scores(qs, i, new0, i, u * p.mr)

        for i in range(p.nd):
            n = i + p.look
            if n < p.nd:
                scores(qs, n, own_at(j), n % slots, bound)
            else:
                n -= p.nd
                scores(qs, jnp.where(more, n, n // 2), jnp.where(more, own_at(j + 1), (n % 2) * p.kt), (n + p.nd) % slots,
                       jnp.where(more, bound - p.kt, anything))
            weigh(i, own_at(j), i % slots)

    def block_at(b):
        return jnp.where(b == 0, 0, p.tok * (1 + jnp.where((cp == 3) & (b == 1), 2, jnp.where(cp == 3, b - 2, b - 1))))

    def block_segment(u, b, count):
        qs = lax.rem(u, 4)
        at = block_at(b)
        following = jnp.where((u > 0) & (b + 1 < count), block_at(b + 1), 0)

        @pl.when((u == 0) & (b > 0))
        def _():
            for i in range(p.look):
                scores(qs, i // 2, at + (i % 2) * p.kt, i, None)

        for i in range(2 * p.nd):
            n = i + p.look
            scores(qs, (n // 2) % p.nd, (at if n < 2 * p.nd else following) + (n % 2) * p.kt, n % slots, None)
            weigh(i // 2, at + (i % 2) * p.kt, i % slots)

    blocks = 1 + cp

    role_a = 3 - tp
    role_b = tp

    def chain(d, i):
        m = i // p.cpm
        j = lax.rem(i, p.cpm)
        mine = own.at[lax.rem(m, p.owns), j, pl.ds(d * p.half, p.half)]
        rows = pl.ds(pl.multiple_of(m * p.mr + d * p.half, p.half), p.half)
        cols = pl.ds(pl.multiple_of(j * p.cc, p.cc), p.cc)
        return mine, land.at[d, lax.rem(i, p.ring)], y.at[rows, cols]

    def peers(d):
        return (jnp.maximum(tp - 1, 0), jnp.minimum(tp + 1, 3)) if d == 0 else (jnp.minimum(tp + 1, 3), jnp.maximum(tp - 1, 0))

    def rs_copy(d, i):
        mine, there, _ = chain(d, i)
        return pltpu.make_async_remote_copy(mine, there, rs_send.at[d, lax.rem(i, p.owns * p.cpm)], rs_recv.at[d, lax.rem(i, p.ring)],
                                            device_id={'tp': peers(d)[0]}, device_id_type=MESH)

    def ag_copy(d, i, src=None):
        out = chain(d, i)[2]
        return pltpu.make_async_remote_copy(out if src is None else src, out, ag_send.at[d, i], ag_recv.at[d, i],
                                            device_id={'tp': peers(d)[1]}, device_id_type=MESH)

    def yl_copy(d, i):
        k = lax.rem(i, p.ys)
        return pltpu.make_async_copy(yst.at[d, k], chain(d, i)[2], yl_sem.at[d, k])

    def pick(role, table):
        res = []
        for k in range(len(table[0])):
            v = table[0][k]
            for r in range(1, len(table)):
                v = jnp.where(role == r, table[r][k], v)
            res.append(v)
        return res

    due = [(d, role, pick(role, p.sums), pick(2 - role, p.rows)) for d, role in ((0, role_a), (1, role_b))]

    def when_due(seg, words, act):
        rest = lax.rem(seg, p.nseg)
        w = words[0]
        for k in range(1, len(words)):
            w = jnp.where(rest >= 5 * k, words[k], w)
        code = jnp.bitwise_and(jnp.right_shift(w, 6 * lax.rem(rest, 5)), 63) - 1
        m = seg // p.nseg - jnp.maximum(code, 0) // p.cpm

        @pl.when((code >= 0) & (m >= 0) & (m < p.nm))
        def _():
            act(m * p.cpm + lax.rem(code, p.cpm))

    def service(seg):
        for d, role, sum_words, _ in due:
            def sums(i, d=d, role=role):
                mine, arrived, _ = chain(d, i)

                @pl.when(role > 0)
                def _():
                    rs_copy(d, i).wait_recv()

                @pl.when((role > 0) & (role < 3))
                def _():
                    mine[...] = mine[...] + arrived[...]

                @pl.when((role < 3) & (i >= p.ring))
                def _():
                    pl.semaphore_wait(free_sem.at[d], 1)

                @pl.when(role < 3)
                def _():
                    rs_copy(d, i).start()

                @pl.when(role == 3)
                def _():
                    k = lax.rem(i, p.ys)

                    @pl.when(i >= p.ys)
                    def _():
                        yl_copy(d, i - p.ys).wait()
                        ag_copy(d, i - p.ys, yst.at[d, k]).wait_send()

                    yst[d, k] = (mine[...] + arrived[...]).astype(jnp.bfloat16)
                    yl_copy(d, i).start()
                    ag_copy(d, i, yst.at[d, k]).start()

                @pl.when((role > 0) & (i < p.chunks - p.ring))
                def _():
                    pl.semaphore_signal(free_sem.at[d], inc=1, device_id={'tp': peers(d)[1]}, device_id_type=MESH)

            when_due(seg, sum_words, sums)

        for d, role, _, row_words in due:
            def rows(i, d=d, role=role):
                @pl.when(role < 3)
                def _():
                    ag_copy(d, i).wait_recv()

                @pl.when((role < 3) & (role > 0))
                def _():
                    ag_copy(d, i).start()

            when_due(seg, row_words, rows)

    take_a = jnp.where(tp == 0, 1, 0).astype(jnp.float32)
    take_b = jnp.where(tp == 3, 1, 0).astype(jnp.float32)
    x_half = jnp.where(tp == 3, p.half, 0)

    def xb_copy(m):
        return pltpu.make_async_copy(x.at[pl.ds(pl.multiple_of(m * p.mr + x_half, p.half), p.half)], xb, b_sem.at[5])

    def first_q(t, _):
        q_tile(t)

        @pl.when(t == max(0, p.nq - 3))
        def _():
            for n in range(p.nt):
                wo_copy(n).start()

        return 0

    lax.fori_loop(0, p.nq, first_q, 0)

    for c in cache_copies(across, partner, 1):
        c.wait_recv()
    for c in cache_copies(across, partner, 2):
        c.start()
    for k in (0, 2):
        for c in cache_copies(cp, partner, k):
            c.wait_recv()

    def segment(seg, _):
        m = seg // p.nseg
        s = lax.rem(seg, p.nseg)
        busy = m < p.nm
        tiles = (m * p.mr + p.mr + p.kt - 1) // p.kt

        @pl.when(busy & (s < tiles) & (s < p.s_blk))
        def _():
            @pl.when(s == 0)
            def _():
                xb_copy(m).start()

            own_segment(m, s, tiles)

        @pl.when((seg == p.s_blk + 1) & (lax.rem(cp, 2) == 1))
        def _():
            for c in new_copies(pl.multiple_of(p.tok * cp, p.tok), p.tok, partner, 0):
                c.wait_recv()

        direct = pl.multiple_of(p.tok * jnp.maximum(cp - 1, 0), p.tok)

        @pl.when((cp == 3) & (seg == p.s_blk + 2))
        def _():
            for c in new_copies(direct, p.tok, partner, 2):
                c.wait_recv()

        @pl.when((cp >= 2) & (seg == p.s_blk + cp - 1))
        def _():
            for c in new_copies(direct, p.tok, partner, 1):
                c.wait_recv()
            for c in new_copies(direct, p.tok, partner, 2):
                c.start()

        @pl.when((cp == 2) & (seg == p.s_blk + 2))
        def _():
            for c in new_copies(direct, p.tok, partner, 2):
                c.wait_recv()

        @pl.when(busy & (s >= p.s_blk) & (s < p.s_blk + blocks))
        def _():
            block_segment(m, s - p.s_blk, blocks)

        @pl.when(busy & (s == p.s_fin))
        def _():
            def finish(i, _):
                for e in range(p.fin):
                    c = i * p.fin + e
                    v = o_t[c] * (1.0 / jnp.sum(l_s[c], axis=0, keepdims=True))
                    for k in range(2):
                        o[:, pl.ds(pl.multiple_of((c * 2 + k) * HEAD, HEAD), HEAD)] = v[:, k * p.mr:(k + 1) * p.mr].T.astype(jnp.bfloat16)
                    reset(c, 0)
                return 0

            lax.fori_loop(0, p.nd // p.fin, finish, 0)

        @pl.when(busy & (s >= p.s_out) & (s < p.s_q))
        def _():
            n = s - p.s_out

            @pl.when(n == 0)
            def _():
                xb_copy(m).wait()

            @pl.when((n == 0) & (m >= p.owns))
            def _():
                for d, role in ((0, role_a), (1, role_b)):
                    @pl.when(role < 3)
                    def _():
                        for j in range(p.cpm):
                            rs_copy(d, (m - p.owns) * p.cpm + j).wait_send()

            @pl.when(m == 0)
            def _():
                wo_copy(n).wait()

            a = jnp.dot(o[...], wo[n], preferred_element_type=jnp.float32)
            r = xb[:, pl.ds(pl.multiple_of(n * p.wcols, HEAD), p.wcols)].astype(jnp.float32)
            own[lax.rem(m, p.owns), n, 0:p.half, :] = a[0:p.half] + r * take_a
            own[lax.rem(m, p.owns), n, p.half:p.mr, :] = a[p.half:p.mr] + r * take_b

        @pl.when((m < p.nm - 2) & (s >= p.s_q))
        def _():
            q_tile((m // 2 + 1) * p.nq + lax.rem(m, 2) * p.hq + s - p.s_q)

        service(seg)
        return 0

    lax.fori_loop(0, p.total, segment, 0)

    for d, role in ((0, role_a), (1, role_b)):
        @pl.when(role < 3)
        def _():
            def last_sums(i, _):
                rs_copy(d, i).wait_send()
                return 0
            lax.fori_loop((p.nm - p.owns) * p.cpm, p.chunks, last_sums, 0)

        @pl.when((role > 0) & (role < 3))
        def _():
            def last_rows(i, _):
                ag_copy(d, i).wait_send()
                return 0
            lax.fori_loop(0, p.chunks, last_rows, 0)

        @pl.when(role == 3)
        def _():
            for k in range(p.ys):
                i = p.chunks - p.ys + k
                yl_copy(d, i).wait()
                ag_copy(d, i, yst.at[d, k]).wait_send()

    for c in out_copies():
        c.wait()
    for k in (0, 1):
        for c in cache_copies(cp, partner, k):
            c.wait_send()
    for c in cache_copies(across, partner, 2):
        c.wait_send()

    @pl.when(cp < 2)
    def _():
        for c in new_copies(new0, p.tok, across, 1):
            c.wait_send()

    @pl.when(lax.rem(cp, 2) == 0)
    def _():
        for c in new_copies(new0, p.tok, partner, 0):
            c.wait_send()

    @pl.when(cp >= 2)
    def _():
        for c in new_copies(pl.multiple_of(p.tok * (cp - 1), p.tok), p.tok, partner, 2):
            c.wait_send()


def settle(pieces, *refs):
    n = len(pieces)
    src, dst, hold, sems = refs[:n], refs[n:2 * n], refs[2 * n:3 * n], refs[3 * n]
    into, out = [], []
    for a, count in enumerate(pieces):
        rows = src[a].shape[0] // count
        for k in range(count):
            at = pl.ds(k * rows, rows)
            i = len(into)
            into.append(pltpu.make_async_copy(src[a].at[at], hold[a].at[at], sems.at[0, i]))
            out.append(pltpu.make_async_copy(hold[a].at[at], dst[a].at[at], sems.at[1, i]))
    for c in into:
        c.start()
    for c, d in zip(into, out):
        c.wait()
        d.start()
    for d in out:
        d.wait()


def build(p):
    def local_step(x, k_cache, v_cache, rope_table, norm_gain, w_qkv, b_qkv, w_out):
        anyspace = pl.BlockSpec(memory_space=pl.ANY)
        bf, f32 = jnp.bfloat16, jnp.float32
        dma = pltpu.SemaphoreType.DMA
        kv_shape = jax.ShapeDtypeStruct((p.tok, p.kv, HEAD), bf)
        y, k_new, v_new = pl.pallas_call(
            functools.partial(kernel, p),
            name='block',
            out_shape=(jax.ShapeDtypeStruct((p.tok, p.dim), bf), kv_shape, kv_shape),
            in_specs=[anyspace] * 8,
            out_specs=(anyspace, anyspace, anyspace),
            scratch_shapes=[
                pltpu.VMEM((p.tok, p.dim), bf),
                pltpu.VMEM((p.kv, p.keys, HEAD), bf),
                pltpu.VMEM((p.kv, HEAD, p.keys), bf),
                pltpu.VMEM((64, p.tok), f32),
                pltpu.VMEM((p.tok, 64), f32),
                pltpu.VMEM(((p.group + 2) * p.kv * HEAD,), bf),
                pltpu.VMEM((p.dim,), bf),
                pltpu.VMEM((1, (p.group + 2) * p.kv * HEAD + p.dim), f32),
                pltpu.VMEM((2, p.cache, p.kv, HEAD), bf),
                pltpu.VMEM((4, p.nd, p.n, HEAD), bf),
                pltpu.VMEM((p.nd, HEAD, p.n), f32),
                pltpu.VMEM((p.mr, p.heads * HEAD), bf),
                pltpu.VMEM((p.look + 1, p.kt, p.n), f32),
                pltpu.VMEM((p.look + 1, 8, p.n), f32),
                pltpu.VMEM((p.nd, 8, p.n), f32),
                pltpu.VMEM((p.nd, 8, p.n), f32),
                pltpu.VMEM((p.owns, p.cpm, p.mr, p.cc), f32),
                pltpu.VMEM((2, p.ring, p.half, p.cc), f32),
                pltpu.VMEM((2, p.ys, p.half, p.cc), bf),
                pltpu.VMEM((p.half, p.dim), bf),
                pltpu.VMEM((2, p.dim, p.wcols), bf),
                pltpu.VMEM((p.nt, p.heads * HEAD, p.wcols), bf),
                pltpu.VMEM((2, p.tok, p.kv, HEAD), bf),
                dma((4,)), dma((2,)), dma((p.nt,)), dma((8,)), dma((2,)),
                dma((3, 2)), dma((3, 2)), dma((3, 2)), dma((3, 2)),
                dma((2, p.owns * p.cpm)), dma((2, p.ring)), pltpu.SemaphoreType.REGULAR((2,)), dma((2, p.chunks)), dma((2, p.chunks)), dma((2, p.ys)),
            ],
            compiler_params=pltpu.CompilerParams(collective_id=0, has_side_effects=True, vmem_limit_bytes=67_000_000),
        )(x, k_cache, v_cache, rope_table.T, norm_gain, b_qkv, w_qkv, w_out)
        res = (y, k_new, v_new)
        pieces = (16, 1, 1)
        return pl.pallas_call(
            functools.partial(settle, pieces),
            name='settle',
            out_shape=tuple(jax.ShapeDtypeStruct(r.shape, r.dtype) for r in res),
            in_specs=[anyspace] * 3,
            out_specs=(anyspace,) * 3,
            scratch_shapes=[pltpu.VMEM(r.shape, r.dtype) for r in res] + [dma((2, sum(pieces)))],
            compiler_params=pltpu.CompilerParams(vmem_limit_bytes=67_000_000),
        )(*res)

    return local_step


def solution(mesh):
    row_spec = P(('dp', 'cp'), None)
    cache_spec = P(('dp', 'cp'), 'tp', None)
    p = Plan(tok=1024, dim=4096, kv=2, group=12, cache=256, nm=8, kt=512)
    p.table([[7, 10, 15, 16, 17, 19, 20, 21], [15, 17, 19, 20, 21, 22, 23, 28], [18, 20, 21, 22, 23, 27, 32, 33], [20, 22, 24, 29, 32, 34, 35, 37]],
            [[28, 32, 33, 36, 37, 38, 39, 40], [35, 36, 37, 38, 39, 40, 42, 46], [37, 38, 39, 40, 41, 47, 50, 52]])
    return jax.shard_map(build(p), mesh=mesh, in_specs=(row_spec, cache_spec, cache_spec, row_spec, P(None), P(None, 'tp'), P('tp'), P('tp', None)),
                         out_specs=(row_spec, cache_spec, cache_spec), check_vma=False)
```

```python
import functools
import math

import jax
import jax.numpy as jnp
from jax import lax
from jax.experimental import pallas as pl
from jax.experimental.pallas import tpu as pltpu
from jax.sharding import PartitionSpec as P

EPS = 1.5625e-07
LOW = -1e30
HEAD = 128
QUAD = 4
MESH = pl.DeviceIdType.MESH


class Plan:
    def __init__(self, tok, dim, kv, group, cache, nm, kt):
        self.tok, self.dim, self.kv, self.group, self.cache = tok, dim, kv, group, cache
        self.nm = nm
        self.mr = tok // nm
        self.kt = kt
        self.heads = kv * group
        self.nd = self.heads // 2
        self.dpg = group // 2
        self.n = 2 * self.mr
        self.keys = tok * 5
        self.wcols = QUAD * HEAD
        self.nq = self.heads // QUAD
        self.qpg = group // QUAD
        self.hq = self.nq // 2
        self.nt = dim // self.wcols
        self.cpm = self.nt
        self.cc = self.wcols
        self.ring = self.cpm
        self.ys = 4
        self.half = self.mr // 2
        self.owns = 2
        self.fin = math.gcd(self.nd, 3)
        self.look = 3
        self.guest = (nm // 2 - 1) * self.cpm + self.cpm - 1
        self.wt = self.nq * (nm // 2)
        self.s_blk = 2
        self.s_fin = self.s_blk + 4
        self.s_out = self.s_fin + 1
        self.s_q = self.s_out + self.nt
        self.nseg = self.s_q + self.hq
        self.chunks = nm * self.cpm
        self.table([[self.s_out + j + 2 * r for j in range(self.cpm)] for r in range(4)],
                   [[self.s_out + j + 8 + 2 * r for j in range(self.cpm)] for r in range(3)])

    def table(self, sums, rows):
        self.total = self.nseg * (self.nm - 1) + max(max(r) for r in sums + rows) + 1
        self.sums, self.rows = [self.words(r) for r in sums], [self.words(r) for r in rows]
        first = self.guest // self.cpm * self.nseg + self.s_out + self.cpm - 1
        step = self.nseg // 3
        self.g_out = first
        self.g_sums = [first + self.nseg - step + step * r for r in range(4)]
        self.g_rows = [self.g_sums[3] + step * (r + 1) for r in range(3)]

    def words(self, due):
        res = [0] * (self.nseg // 5 + 1)
        for j, at in enumerate(due):
            rest = at % self.nseg
            assert res[rest // 5] >> 6 * (rest % 5) & 63 == 0
            res[rest // 5] += (1 + j + self.cpm * (at // self.nseg)) << 6 * (rest % 5)
        return res


def kernel(p, x, k_in, v_in, rope_in, gain_in, bias_in, wqkv, wout, y, kn, vn,
           h, ka, vt, rope_t, rope, b1, g1, small, q, o_t, o, s_t, mx_t, m_s, l_s, own, land, yst, g_in, g_land, g_y, xb, w, wo, kv_out,
           x_sem, w_sem, wo_sem, b_sem, out_sem, cs_send, cs_recv, kv_send, kv_recv,
           rs_send, rs_recv, free_sem, ag_send, ag_recv, yl_sem, g_send, g_recv):
    tp = lax.axis_index('tp')
    cp = lax.axis_index('cp')
    partner = cp + 1 - 2 * lax.rem(cp, 2)
    across = lax.rem(cp + 2, 4)
    scale = HEAD ** -0.5 * math.log2(math.e)
    new0 = p.tok * (1 + cp)
    rows4 = p.tok // 4
    goff = (p.group + 2) * HEAD * p.kv

    def wq_col(j):
        return (j // p.qpg) * (p.group + 2) * HEAD + lax.rem(j, p.qpg) * p.wcols

    def wq_copy(t):
        slot = lax.rem(t, 2)
        col = pl.multiple_of(wq_col(lax.rem(t, p.nq)), HEAD)
        return pltpu.make_async_copy(wqkv.at[:, pl.ds(col, p.wcols)], w.at[slot], w_sem.at[slot])

    def wo_copy(n):
        return pltpu.make_async_copy(wout.at[:, pl.ds(pl.multiple_of(n * p.wcols, HEAD), p.wcols)], wo.at[n], wo_sem.at[n])

    def x_copy(r):
        rows = pl.ds(r * rows4, rows4)
        return pltpu.make_async_copy(x.at[rows], h.at[rows], x_sem.at[r])

    def wkv_copy(g):
        col = g * (p.group + 2) * HEAD + p.group * HEAD
        return pltpu.make_async_copy(wqkv.at[:, pl.ds(col, 2 * HEAD)], w.at[1, :, pl.ds(g * 2 * HEAD, 2 * HEAD)], b_sem.at[g])

    x_copy(0).start()
    for g in range(p.kv):
        wkv_copy(g).start()
    little = [pltpu.make_async_copy(rope_in, rope_t, b_sem.at[2]), pltpu.make_async_copy(k_in, kv_out.at[0, pl.ds(0, p.cache)], b_sem.at[3]),
              pltpu.make_async_copy(v_in, kv_out.at[1, pl.ds(0, p.cache)], b_sem.at[4]), pltpu.make_async_copy(bias_in, b1, b_sem.at[6]),
              pltpu.make_async_copy(gain_in, g1, b_sem.at[7])]
    for c in little:
        c.start()

    barrier = pltpu.get_barrier_semaphore()
    for k in range(1, 4):
        pl.semaphore_signal(barrier, inc=1, device_id={'tp': lax.rem(tp + k, 4)}, device_id_type=MESH)
        pl.semaphore_signal(barrier, inc=1, device_id={'cp': lax.rem(cp + k, 4)}, device_id_type=MESH)

    def cache_copies(owner, peer, k):
        at = pl.multiple_of(owner * p.cache, p.cache)
        ks = ka.at[:, pl.ds(at, p.cache)]
        vs = vt.at[:, :, pl.ds(at, p.cache)]
        return (pltpu.make_async_remote_copy(ks, ks, cs_send.at[k, 0], cs_recv.at[k, 0], device_id={'cp': peer}, device_id_type=MESH),
                pltpu.make_async_remote_copy(vs, vs, cs_send.at[k, 1], cs_recv.at[k, 1], device_id={'cp': peer}, device_id_type=MESH))

    def new_copies(at, size, peer, k):
        ks = ka.at[:, pl.ds(at, size)]
        vs = vt.at[:, :, pl.ds(at, size)]
        return (pltpu.make_async_remote_copy(ks, ks, kv_send.at[k, 0], kv_recv.at[k, 0], device_id={'cp': peer}, device_id_type=MESH),
                pltpu.make_async_remote_copy(vs, vs, kv_send.at[k, 1], kv_recv.at[k, 1], device_id={'cp': peer}, device_id_type=MESH))

    little[1].wait()
    little[2].wait()
    here = pl.multiple_of(cp * p.cache, p.cache)
    for g in range(p.kv):
        ka[g, pl.ds(here, p.cache), :] = kv_out[0, 0:p.cache].astype(jnp.float32)[:, g, :].astype(jnp.bfloat16)
        vt[g, :, pl.ds(here, p.cache)] = kv_out[1, 0:p.cache].astype(jnp.float32)[:, g, :].T.astype(jnp.bfloat16)
    pl.semaphore_wait(barrier, 6)
    for peer, k in ((across, 1), (partner, 0)):
        for c in cache_copies(cp, peer, k):
            c.start()
    for c in (little[0], little[3], little[4]):
        c.wait()
    small[0:1, 0:goff] = b1[...].astype(jnp.float32).reshape(1, goff)
    small[0:1, goff:goff + p.dim] = g1[...].astype(jnp.float32).reshape(1, p.dim)
    rope[...] = rope_t[...].T

    def send_new(r):
        at = pl.multiple_of(new0 + r * rows4, rows4)

        @pl.when(cp == 0)
        def _():
            for c in new_copies(at, rows4, across, 1):
                c.start()

        @pl.when(lax.rem(cp, 2) == 0)
        def _():
            for c in new_copies(at, rows4, partner, 0):
                c.start()

    lane = lax.broadcasted_iota(jnp.int32, (1, HEAD), 1)
    even = lax.rem(lane, 2) == 0
    turned = lane < 64

    def angles(rows, count):
        r = rope[rows, :]
        both = jnp.concatenate([r, r], axis=1)
        at = lax.broadcasted_iota(jnp.int32, (count, HEAD), 1)
        pair = lax.rem(at, 64) // 2
        c = jnp.take_along_axis(both, pair, axis=1)
        s = jnp.take_along_axis(both, pair + 32, axis=1)
        return c, jnp.where(even, -s, s)

    def rotate(a, c, s):
        swap = jnp.where(even, pltpu.roll(a, HEAD - 1, 1), pltpu.roll(a, 1, 1))
        return jnp.where(turned, a * c + swap * s, a)

    for g in range(p.kv):
        wkv_copy(g).wait()
    for r in range(1, 4):
        x_copy(r).start()
    wq_copy(0).start()
    nsub = max(8, rows4 // 32)
    sub = rows4 // nsub
    wide = 512

    def norm(b):
        rows = pl.ds(pl.multiple_of(b * sub, sub), sub)
        total = None
        for c in range(0, p.dim, wide):
            v = h[rows, c:c + wide].astype(jnp.float32)
            v = v * v
            for k in range(0, wide, HEAD):
                total = v[:, k:k + HEAD] if total is None else total + v[:, k:k + HEAD]
        inv = lax.rsqrt(jnp.sum(total, axis=1, keepdims=True) * (1.0 / p.dim) + EPS)
        for c in range(0, p.dim, wide):
            v = h[rows, c:c + wide].astype(jnp.float32)
            h[rows, c:c + wide] = (v * inv * small[0:1, goff + c:goff + c + wide]).astype(jnp.bfloat16)

    def keys_values(r, ahead):
        rows = pl.ds(pl.multiple_of(r * rows4, rows4), rows4)
        at = pl.multiple_of(new0 + r * rows4, rows4)
        a = None
        per = nsub // 8
        deep = p.dim // 8
        for e in range(8):
            part = jnp.dot(h[rows, e * deep:(e + 1) * deep], w[1, e * deep:(e + 1) * deep, :], preferred_element_type=jnp.float32)
            a = part if a is None else a + part
            if ahead:
                for b in range(per):
                    norm((r + 1) * nsub + e * per + b)
        c, s = angles(rows, rows4)
        keys, vals = [], []
        for g in range(p.kv):
            col = g * (p.group + 2) * HEAD + p.group * HEAD
            keys.append(rotate(a[:, g * 2 * HEAD:g * 2 * HEAD + HEAD] + small[0:1, col:col + HEAD], c, s))
            vals.append(a[:, g * 2 * HEAD + HEAD:(g + 1) * 2 * HEAD] + small[0:1, col + HEAD:col + 2 * HEAD])
            ka[g, pl.ds(at, rows4), :] = keys[g].astype(jnp.bfloat16)
            vt[g, :, pl.ds(at, rows4)] = vals[g].T.astype(jnp.bfloat16)
        kv_out[0, rows] = jnp.swapaxes(jnp.stack(keys), 0, 1).astype(jnp.bfloat16)
        kv_out[1, rows] = jnp.swapaxes(jnp.stack(vals), 0, 1).astype(jnp.bfloat16)

    def kv_step(r, _):
        x_copy(r + 1).wait()

        @pl.when(r > 0)
        def _():
            send_new(r - 1)

        keys_values(r, True)
        return 0

    x_copy(0).wait()
    for b in range(nsub):
        norm(b)
    lax.fori_loop(0, 3, kv_step, 0)
    send_new(2)
    keys_values(3, False)
    wq_copy(1).start()
    send_new(3)

    @pl.when(cp == 1)
    def _():
        for c in new_copies(new0, p.tok, across, 1):
            c.start()

    def out_copies():
        return [pltpu.make_async_copy(kv_out.at[0], kn, out_sem.at[0]), pltpu.make_async_copy(kv_out.at[1], vn, out_sem.at[1])]

    for c in out_copies():
        c.start()

    def reset(i, _):
        m_s[i] = jnp.full((8, p.n), LOW, jnp.float32)
        l_s[i] = jnp.zeros((8, p.n), jnp.float32)
        o_t[i] = jnp.zeros((HEAD, p.n), jnp.float32)
        return 0

    lax.fori_loop(0, p.nd, reset, 0)

    def q_tile(t):
        j = lax.rem(t, p.nq)
        first = t // p.nq * 2
        count = 2
        rows = pl.ds(pl.multiple_of(first * p.mr, p.mr), count * p.mr)
        wq_copy(t).wait()
        a = jnp.dot(h[rows, :], w[lax.rem(t, 2)], preferred_element_type=jnp.float32)
        a = a + small[0:1, pl.ds(pl.multiple_of(wq_col(j), HEAD), p.wcols)]
        c, s = angles(rows, count * p.mr)
        for k in range(QUAD):
            b = rotate(a[:, k * HEAD:(k + 1) * HEAD], c, s).astype(jnp.bfloat16)
            for u in range(count):
                q[lax.rem(first + u, 4), 2 * j + k // 2, (k % 2) * p.mr:(k % 2 + 1) * p.mr, :] = b[u * p.mr:(u + 1) * p.mr, :]

        @pl.when(t + 2 < p.wt)
        def _():
            wq_copy(t + 2).start()

    part_rows = min(256, p.kt)
    row_of = lax.rem(lax.broadcasted_iota(jnp.int32, (p.kt, p.n), 1), p.mr) - lax.broadcasted_iota(jnp.int32, (p.kt, p.n), 0)

    def scores(qs, pair, off, k, bound):
        g = pair // p.dpg
        s = lax.dot_general(ka[g, pl.ds(pl.multiple_of(off, p.kt), p.kt), :], q[qs, pair], (((1,), (1,)), ((), ())),
                            preferred_element_type=jnp.float32) * scale
        if bound is not None:
            s = jnp.where(row_of >= -bound, s, LOW)
        s_t[k] = s
        mx_t[k] = jnp.max(s.reshape(p.kt // 8, 8, p.n), axis=0)

    def weigh(pair, off, k):
        g = pair // p.dpg
        m_old = m_s[pair, 0:1, :]
        m_new = jnp.maximum(m_old, jnp.max(mx_t[k], axis=0, keepdims=True))
        alpha = jnp.exp2(m_old - m_new)
        m_s[pair, 0:1, :] = m_new
        acc = None
        es = []
        for r in range(0, p.kt, part_rows):
            e = jnp.exp2(s_t[k, r:r + part_rows, :] - m_new)
            part = jnp.sum(e.reshape(part_rows // 8, 8, p.n), axis=0)
            acc = part if acc is None else acc + part
            es.append(e.astype(jnp.bfloat16))
        d = jnp.dot(vt[g, :, pl.ds(pl.multiple_of(off, p.kt), p.kt)], jnp.concatenate(es, axis=0), preferred_element_type=jnp.float32)
        l_s[pair] = l_s[pair] * alpha + acc
        o_t[pair] = o_t[pair] * alpha + d

    anything = 1 << 20
    slots = p.look + 1

    def own_at(j):
        return new0 + j * p.kt

    def own_segment(u, j, tiles):
        qs = lax.rem(u, 4)
        bound = u * p.mr - j * p.kt
        more = j + 1 < tiles

        @pl.when(j == 0)
        def _():
            for i in range(p.look):
                scores(qs, i, new0, i, u * p.mr)

        for i in range(p.nd):
            n = i + p.look
            if n < p.nd:
                scores(qs, n, own_at(j), n % slots, bound)
            else:
                n -= p.nd
                scores(qs, jnp.where(more, n, n // 2), jnp.where(more, own_at(j + 1), (n % 2) * p.kt), (n + p.nd) % slots,
                       jnp.where(more, bound - p.kt, anything))
            weigh(i, own_at(j), i % slots)

    def block_at(b):
        return jnp.where(b == 0, 0, p.tok * (1 + jnp.where((cp == 3) & (b == 1), 2, jnp.where(cp == 3, b - 2, b - 1))))

    def block_segment(u, b, count):
        qs = lax.rem(u, 4)
        at = block_at(b)
        following = jnp.where((u > 0) & (b + 1 < count), block_at(b + 1), 0)

        @pl.when((u == 0) & (b > 0))
        def _():
            for i in range(p.look):
                scores(qs, i // 2, at + (i % 2) * p.kt, i, None)

        for i in range(2 * p.nd):
            n = i + p.look
            scores(qs, (n // 2) % p.nd, (at if n < 2 * p.nd else following) + (n % 2) * p.kt, n % slots, None)
            weigh(i // 2, at + (i % 2) * p.kt, i % slots)

    blocks = 1 + cp

    role_a = 3 - tp
    role_b = tp

    def chain(d, i):
        m = i // p.cpm
        j = lax.rem(i, p.cpm)
        mine = own.at[lax.rem(m, p.owns), j, pl.ds(d * p.half, p.half)]
        rows = pl.ds(pl.multiple_of(m * p.mr + d * p.half, p.half), p.half)
        cols = pl.ds(pl.multiple_of(j * p.cc, p.cc), p.cc)
        return mine, land.at[d, lax.rem(i, p.ring)], y.at[rows, cols]

    def peers(d):
        return (jnp.maximum(tp - 1, 0), jnp.minimum(tp + 1, 3)) if d == 0 else (jnp.minimum(tp + 1, 3), jnp.maximum(tp - 1, 0))

    def rs_copy(d, i):
        mine, there, _ = chain(d, i)
        return pltpu.make_async_remote_copy(mine, there, rs_send.at[d, lax.rem(i, p.owns * p.cpm)], rs_recv.at[d, lax.rem(i, p.ring)],
                                            device_id={'tp': peers(d)[0]}, device_id_type=MESH)

    def ag_copy(d, i, src=None):
        out = chain(d, i)[2]
        return pltpu.make_async_remote_copy(out if src is None else src, out, ag_send.at[d, i], ag_recv.at[d, i],
                                            device_id={'tp': peers(d)[1]}, device_id_type=MESH)

    def yl_copy(d, i):
        k = lax.rem(i, p.ys)
        return pltpu.make_async_copy(yst.at[d, k], chain(d, i)[2], yl_sem.at[d, k])

    def guest_copy(src, dst, k, d, peer):
        return pltpu.make_async_remote_copy(src, dst, g_send.at[k, d], g_recv.at[k, d], device_id=peer, device_id_type=MESH)

    def guest_out(d):
        return guest_copy(chain(d, p.guest)[0], g_in.at[d], 0, d, {'cp': across})

    def guest_sum(d):
        return guest_copy(g_in.at[d], g_land.at[d], 1, d, {'tp': peers(d)[0]})

    def guest_row(d):
        return guest_copy(g_y.at[d], g_y.at[d], 2, d, {'tp': peers(d)[1]})

    def guest_home(d):
        return guest_copy(g_y.at[d], chain(d, p.guest)[2], 3, d, {'cp': across})

    def pick(role, table):
        res = []
        for k in range(len(table[0])):
            v = table[0][k]
            for r in range(1, len(table)):
                v = jnp.where(role == r, table[r][k], v)
            res.append(v)
        return res

    due = [(d, role, pick(role, p.sums), pick(2 - role, p.rows)) for d, role in ((0, role_a), (1, role_b))]

    def when_due(seg, words, act):
        rest = lax.rem(seg, p.nseg)
        w = words[0]
        for k in range(1, len(words)):
            w = jnp.where(rest >= 5 * k, words[k], w)
        code = jnp.bitwise_and(jnp.right_shift(w, 6 * lax.rem(rest, 5)), 63) - 1
        m = seg // p.nseg - jnp.maximum(code, 0) // p.cpm

        @pl.when((code >= 0) & (m >= 0) & (m < p.nm))
        def _():
            act(m * p.cpm + lax.rem(code, p.cpm))

    def service(seg):
        for d, role, sum_words, _ in due:
            def sums(i, d=d, role=role):
                mine, arrived, _ = chain(d, i)
                stays = (cp < 2) | (i != p.guest)

                @pl.when((role > 0) & stays)
                def _():
                    rs_copy(d, i).wait_recv()

                @pl.when((role > 0) & (role < 3) & stays)
                def _():
                    mine[...] = mine[...] + arrived[...]

                @pl.when((role < 3) & (i >= p.ring))
                def _():
                    pl.semaphore_wait(free_sem.at[d], 1)

                @pl.when((role < 3) & stays)
                def _():
                    rs_copy(d, i).start()

                k = lax.rem(i, p.ys)

                @pl.when((role == 3) & (i >= p.ys) & ((cp < 2) | (i - p.ys != p.guest)))
                def _():
                    yl_copy(d, i - p.ys).wait()
                    ag_copy(d, i - p.ys, yst.at[d, k]).wait_send()

                @pl.when((role == 3) & stays)
                def _():
                    yst[d, k] = (mine[...] + arrived[...]).astype(jnp.bfloat16)
                    yl_copy(d, i).start()
                    ag_copy(d, i, yst.at[d, k]).start()

                @pl.when((role > 0) & (i < p.chunks - p.ring))
                def _():
                    pl.semaphore_signal(free_sem.at[d], inc=1, device_id={'tp': peers(d)[1]}, device_id_type=MESH)

            when_due(seg, sum_words, sums)

        for d, role, _, row_words in due:
            def rows(i, d=d, role=role):
                stays = (cp < 2) | (i != p.guest)

                @pl.when((role < 3) & stays)
                def _():
                    ag_copy(d, i).wait_recv()

                @pl.when((role < 3) & (role > 0) & stays)
                def _():
                    ag_copy(d, i).start()

            when_due(seg, row_words, rows)

        @pl.when((cp >= 2) & (seg == p.g_out))
        def _():
            for d in range(2):
                guest_out(d).start()

        for d, role, _, _ in due:
            for r in range(4):
                @pl.when((cp < 2) & (role == r) & (seg == p.g_sums[r]))
                def _():
                    guest_out(d).wait_recv()
                    if r > 0:
                        guest_sum(d).wait_recv()
                    if r < 3:
                        if r > 0:
                            g_in[d] = g_in[d] + g_land[d]
                        guest_sum(d).start()
                    else:
                        g_y[d] = (g_in[d] + g_land[d]).astype(jnp.bfloat16)
                        guest_row(d).start()
                        guest_home(d).start()

            for r in range(3):
                @pl.when((cp < 2) & (role == 2 - r) & (seg == p.g_rows[r]))
                def _():
                    guest_row(d).wait_recv()
                    if r < 2:
                        guest_row(d).start()
                    guest_home(d).start()

    take_a = jnp.where(tp == 0, 1, 0).astype(jnp.float32)
    take_b = jnp.where(tp == 3, 1, 0).astype(jnp.float32)
    x_half = jnp.where(tp == 3, p.half, 0)

    def xb_copy(m):
        return pltpu.make_async_copy(x.at[pl.ds(pl.multiple_of(m * p.mr + x_half, p.half), p.half)], xb, b_sem.at[5])

    def first_q(t, _):
        q_tile(t)

        @pl.when(t == max(0, p.nq - 3))
        def _():
            for n in range(p.nt):
                wo_copy(n).start()

        return 0

    lax.fori_loop(0, p.nq, first_q, 0)

    for c in cache_copies(across, partner, 1):
        c.wait_recv()
    for c in cache_copies(across, partner, 2):
        c.start()
    for k in (0, 2):
        for c in cache_copies(cp, partner, k):
            c.wait_recv()

    def segment(seg, _):
        m = seg // p.nseg
        s = lax.rem(seg, p.nseg)
        busy = m < p.nm
        tiles = (m * p.mr + p.mr + p.kt - 1) // p.kt

        @pl.when(busy & (s < tiles) & (s < p.s_blk))
        def _():
            @pl.when(s == 0)
            def _():
                xb_copy(m).start()

            own_segment(m, s, tiles)

        @pl.when((seg == p.s_blk + 1) & (lax.rem(cp, 2) == 1))
        def _():
            for c in new_copies(pl.multiple_of(p.tok * cp, p.tok), p.tok, partner, 0):
                c.wait_recv()

        direct = pl.multiple_of(p.tok * jnp.maximum(cp - 1, 0), p.tok)

        @pl.when((cp == 3) & (seg == p.s_blk + 2))
        def _():
            for c in new_copies(direct, p.tok, partner, 2):
                c.wait_recv()

        @pl.when((cp >= 2) & (seg == p.s_blk + cp - 1))
        def _():
            for c in new_copies(direct, p.tok, partner, 1):
                c.wait_recv()
            for c in new_copies(direct, p.tok, partner, 2):
                c.start()

        @pl.when((cp == 2) & (seg == p.s_blk + 2))
        def _():
            for c in new_copies(direct, p.tok, partner, 2):
                c.wait_recv()

        @pl.when(busy & (s >= p.s_blk) & (s < p.s_blk + blocks))
        def _():
            block_segment(m, s - p.s_blk, blocks)

        @pl.when(busy & (s == p.s_fin))
        def _():
            def finish(i, _):
                for e in range(p.fin):
                    c = i * p.fin + e
                    v = o_t[c] * (1.0 / jnp.sum(l_s[c], axis=0, keepdims=True))
                    for k in range(2):
                        o[:, pl.ds(pl.multiple_of((c * 2 + k) * HEAD, HEAD), HEAD)] = v[:, k * p.mr:(k + 1) * p.mr].T.astype(jnp.bfloat16)
                    reset(c, 0)
                return 0

            lax.fori_loop(0, p.nd // p.fin, finish, 0)

        @pl.when(busy & (s >= p.s_out) & (s < p.s_q))
        def _():
            n = s - p.s_out

            @pl.when(n == 0)
            def _():
                xb_copy(m).wait()

            @pl.when((n == 0) & (m >= p.owns))
            def _():
                for d, role in ((0, role_a), (1, role_b)):
                    for j in range(p.cpm):
                        i = (m - p.owns) * p.cpm + j

                        @pl.when((role < 3) & ((cp < 2) | (i != p.guest)))
                        def _():
                            rs_copy(d, i).wait_send()

                        if j == p.guest % p.cpm:
                            @pl.when((cp >= 2) & (i == p.guest))
                            def _():
                                guest_out(d).wait_send()

            @pl.when(m == 0)
            def _():
                wo_copy(n).wait()

            a = jnp.dot(o[...], wo[n], preferred_element_type=jnp.float32)
            r = xb[:, pl.ds(pl.multiple_of(n * p.wcols, HEAD), p.wcols)].astype(jnp.float32)
            own[lax.rem(m, p.owns), n, 0:p.half, :] = a[0:p.half] + r * take_a
            own[lax.rem(m, p.owns), n, p.half:p.mr, :] = a[p.half:p.mr] + r * take_b

        @pl.when((m < p.nm - 2) & (s >= p.s_q))
        def _():
            q_tile((m // 2 + 1) * p.nq + lax.rem(m, 2) * p.hq + s - p.s_q)

        service(seg)
        return 0

    lax.fori_loop(0, p.total, segment, 0)

    for d, role in ((0, role_a), (1, role_b)):
        @pl.when(role < 3)
        def _():
            def last_sums(i, _):
                rs_copy(d, i).wait_send()
                return 0
            lax.fori_loop((p.nm - p.owns) * p.cpm, p.chunks, last_sums, 0)

        @pl.when((role > 0) & (role < 3))
        def _():
            def last_rows(i, _):
                @pl.when((cp < 2) | (i != p.guest))
                def _():
                    ag_copy(d, i).wait_send()
                return 0
            lax.fori_loop(0, p.chunks, last_rows, 0)

        @pl.when(role == 3)
        def _():
            for k in range(p.ys):
                i = p.chunks - p.ys + k
                yl_copy(d, i).wait()
                ag_copy(d, i, yst.at[d, k]).wait_send()

    for d, role in ((0, role_a), (1, role_b)):
        @pl.when(cp >= 2)
        def _():
            guest_home(d).wait_recv()

        @pl.when((cp < 2) & (role < 3))
        def _():
            guest_sum(d).wait_send()

        @pl.when((cp < 2) & (role > 0))
        def _():
            guest_row(d).wait_send()

        @pl.when(cp < 2)
        def _():
            guest_home(d).wait_send()

    for c in out_copies():
        c.wait()
    for k in (0, 1):
        for c in cache_copies(cp, partner, k):
            c.wait_send()
    for c in cache_copies(across, partner, 2):
        c.wait_send()

    @pl.when(cp < 2)
    def _():
        for c in new_copies(new0, p.tok, across, 1):
            c.wait_send()

    @pl.when(lax.rem(cp, 2) == 0)
    def _():
        for c in new_copies(new0, p.tok, partner, 0):
            c.wait_send()

    @pl.when(cp >= 2)
    def _():
        for c in new_copies(pl.multiple_of(p.tok * (cp - 1), p.tok), p.tok, partner, 2):
            c.wait_send()


def settle(pieces, *refs):
    n = len(pieces)
    src, dst, hold, sems = refs[:n], refs[n:2 * n], refs[2 * n:3 * n], refs[3 * n]
    into, out = [], []
    for a, count in enumerate(pieces):
        rows = src[a].shape[0] // count
        for k in range(count):
            at = pl.ds(k * rows, rows)
            i = len(into)
            into.append(pltpu.make_async_copy(src[a].at[at], hold[a].at[at], sems.at[0, i]))
            out.append(pltpu.make_async_copy(hold[a].at[at], dst[a].at[at], sems.at[1, i]))
    for c in into:
        c.start()
    for c, d in zip(into, out):
        c.wait()
        d.start()
    for d in out:
        d.wait()


def build(p):
    def local_step(x, k_cache, v_cache, rope_table, norm_gain, w_qkv, b_qkv, w_out):
        anyspace = pl.BlockSpec(memory_space=pl.ANY)
        bf, f32 = jnp.bfloat16, jnp.float32
        dma = pltpu.SemaphoreType.DMA
        kv_shape = jax.ShapeDtypeStruct((p.tok, p.kv, HEAD), bf)
        y, k_new, v_new = pl.pallas_call(
            functools.partial(kernel, p),
            name='block',
            out_shape=(jax.ShapeDtypeStruct((p.tok, p.dim), bf), kv_shape, kv_shape),
            in_specs=[anyspace] * 8,
            out_specs=(anyspace, anyspace, anyspace),
            scratch_shapes=[
                pltpu.VMEM((p.tok, p.dim), bf),
                pltpu.VMEM((p.kv, p.keys, HEAD), bf),
                pltpu.VMEM((p.kv, HEAD, p.keys), bf),
                pltpu.VMEM((64, p.tok), f32),
                pltpu.VMEM((p.tok, 64), f32),
                pltpu.VMEM(((p.group + 2) * p.kv * HEAD,), bf),
                pltpu.VMEM((p.dim,), bf),
                pltpu.VMEM((1, (p.group + 2) * p.kv * HEAD + p.dim), f32),
                pltpu.VMEM((4, p.nd, p.n, HEAD), bf),
                pltpu.VMEM((p.nd, HEAD, p.n), f32),
                pltpu.VMEM((p.mr, p.heads * HEAD), bf),
                pltpu.VMEM((p.look + 1, p.kt, p.n), f32),
                pltpu.VMEM((p.look + 1, 8, p.n), f32),
                pltpu.VMEM((p.nd, 8, p.n), f32),
                pltpu.VMEM((p.nd, 8, p.n), f32),
                pltpu.VMEM((p.owns, p.cpm, p.mr, p.cc), f32),
                pltpu.VMEM((2, p.ring, p.half, p.cc), f32),
                pltpu.VMEM((2, p.ys, p.half, p.cc), bf),
                pltpu.VMEM((2, p.half, p.cc), f32),
                pltpu.VMEM((2, p.half, p.cc), f32),
                pltpu.VMEM((2, p.half, p.cc), bf),
                pltpu.VMEM((p.half, p.dim), bf),
                pltpu.VMEM((2, p.dim, p.wcols), bf),
                pltpu.VMEM((p.nt, p.heads * HEAD, p.wcols), bf),
                pltpu.VMEM((2, p.tok, p.kv, HEAD), bf),
                dma((4,)), dma((2,)), dma((p.nt,)), dma((8,)), dma((2,)),
                dma((3, 2)), dma((3, 2)), dma((3, 2)), dma((3, 2)),
                dma((2, p.owns * p.cpm)), dma((2, p.ring)), pltpu.SemaphoreType.REGULAR((2,)), dma((2, p.chunks)), dma((2, p.chunks)), dma((2, p.ys)),
                dma((4, 2)), dma((4, 2)),
            ],
            compiler_params=pltpu.CompilerParams(collective_id=0, has_side_effects=True, vmem_limit_bytes=67_000_000),
        )(x, k_cache, v_cache, rope_table.T, norm_gain, b_qkv, w_qkv, w_out)
        res = (y, k_new, v_new)
        pieces = (16, 1, 1)
        return pl.pallas_call(
            functools.partial(settle, pieces),
            name='settle',
            out_shape=tuple(jax.ShapeDtypeStruct(r.shape, r.dtype) for r in res),
            in_specs=[anyspace] * 3,
            out_specs=(anyspace,) * 3,
            scratch_shapes=[pltpu.VMEM(r.shape, r.dtype) for r in res] + [dma((2, sum(pieces)))],
            compiler_params=pltpu.CompilerParams(vmem_limit_bytes=67_000_000),
        )(*res)

    return local_step


def solution(mesh):
    row_spec = P(('dp', 'cp'), None)
    cache_spec = P(('dp', 'cp'), 'tp', None)
    p = Plan(tok=1024, dim=4096, kv=2, group=12, cache=256, nm=8, kt=512)
    p.table([[7, 9, 14, 15, 17, 19, 20, 21], [14, 16, 18, 19, 20, 21, 22, 23], [17, 18, 20, 21, 22, 23, 25, 30], [20, 22, 23, 24, 27, 30, 34, 36]],
            [[22, 24, 25, 29, 34, 35, 37, 38], [30, 33, 34, 35, 37, 38, 39, 40], [37, 39, 40, 41, 42, 44, 48, 51]])
    return jax.shard_map(build(p), mesh=mesh, in_specs=(row_spec, cache_spec, cache_spec, row_spec, P(None), P(None, 'tp'), P('tp'), P('tp', None)),
                         out_specs=(row_spec, cache_spec, cache_spec), check_vma=False)
```

```python
import functools
import math

import jax
import jax.numpy as jnp
from jax import lax
from jax.experimental import pallas as pl
from jax.experimental.pallas import tpu as pltpu
from jax.sharding import PartitionSpec as P

EPS = 1.5625e-07
LOW = -1e30
HEAD = 128
QUAD = 4
MESH = pl.DeviceIdType.MESH


class Plan:
    def __init__(self, tok, dim, kv, group, cache, nm, kt):
        self.tok, self.dim, self.kv, self.group, self.cache = tok, dim, kv, group, cache
        self.nm = nm
        self.mr = tok // nm
        self.kt = kt
        self.heads = kv * group
        self.nd = self.heads // 2
        self.dpg = group // 2
        self.n = 2 * self.mr
        self.keys = tok * 5
        self.wcols = QUAD * HEAD
        self.nq = self.heads // QUAD
        self.qpg = group // QUAD
        self.hq = self.nq // 2
        self.nt = dim // self.wcols
        self.cpm = self.nt
        self.cc = self.wcols
        self.ring = self.cpm
        self.ys = 4
        self.half = self.mr // 2
        self.owns = 2
        self.fin = math.gcd(self.nd, 3)
        self.look = 3
        self.guest = (nm // 2 - 1) * self.cpm + self.cpm - 1
        self.wt = self.nq * (nm // 2)
        self.s_blk = 2
        self.s_fin = self.s_blk + 4
        self.s_out = self.s_fin + 1
        self.s_q = self.s_out + self.nt
        self.nseg = self.s_q + self.hq
        self.chunks = nm * self.cpm
        self.table([[self.s_out + j + 2 * r for j in range(self.cpm)] for r in range(4)],
                   [[self.s_out + j + 8 + 2 * r for j in range(self.cpm)] for r in range(3)])

    def table(self, sums, rows):
        self.total = self.nseg * (self.nm - 1) + max(max(r) for r in sums + rows) + 1
        self.sums, self.rows = [self.words(r) for r in sums], [self.words(r) for r in rows]
        first = self.guest // self.cpm * self.nseg + self.s_out + self.cpm - 1
        step = self.nseg // 3
        self.g_out = first
        self.g_sums = [first + self.nseg - step + step * r for r in range(4)]
        self.g_rows = [self.g_sums[3] + step * (r + 1) for r in range(3)]

    def words(self, due):
        res = [0] * (self.nseg // 5 + 1)
        for j, at in enumerate(due):
            rest = at % self.nseg
            assert res[rest // 5] >> 6 * (rest % 5) & 63 == 0
            res[rest // 5] += (1 + j + self.cpm * (at // self.nseg)) << 6 * (rest % 5)
        return res


def kernel(p, x, k_in, v_in, rope_in, gain_in, bias_in, wqkv, wout, y, kn, vn,
           h, ka, vt, rope_t, rope, b1, g1, small, q, o_t, o, s_t, mx_t, m_s, l_s, own, land, yst, g_in, g_land, g_y, xb, w, wo, kv_out,
           x_sem, w_sem, wo_sem, b_sem, out_sem, cs_send, cs_recv, kv_send, kv_recv,
           rs_send, rs_recv, free_sem, ag_send, ag_recv, yl_sem, g_send, g_recv):
    tp = lax.axis_index('tp')
    cp = lax.axis_index('cp')
    partner = cp + 1 - 2 * lax.rem(cp, 2)
    across = lax.rem(cp + 2, 4)
    scale = HEAD ** -0.5 * math.log2(math.e)
    new0 = p.tok * (1 + cp)
    rows4 = p.tok // 4
    goff = (p.group + 2) * HEAD * p.kv

    def wq_col(j):
        return (j // p.qpg) * (p.group + 2) * HEAD + lax.rem(j, p.qpg) * p.wcols

    def wq_copy(t):
        slot = lax.rem(t, 2)
        col = pl.multiple_of(wq_col(lax.rem(t, p.nq)), HEAD)
        return pltpu.make_async_copy(wqkv.at[:, pl.ds(col, p.wcols)], w.at[slot], w_sem.at[slot])

    def wo_copy(n):
        return pltpu.make_async_copy(wout.at[:, pl.ds(pl.multiple_of(n * p.wcols, HEAD), p.wcols)], wo.at[n], wo_sem.at[n])

    def x_copy(r):
        rows = pl.ds(r * rows4, rows4)
        return pltpu.make_async_copy(x.at[rows], h.at[rows], x_sem.at[r])

    def wkv_copy(g):
        col = g * (p.group + 2) * HEAD + p.group * HEAD
        return pltpu.make_async_copy(wqkv.at[:, pl.ds(col, 2 * HEAD)], w.at[1, :, pl.ds(g * 2 * HEAD, 2 * HEAD)], b_sem.at[g])

    x_copy(0).start()
    for g in range(p.kv):
        wkv_copy(g).start()
    little = [pltpu.make_async_copy(rope_in, rope_t, b_sem.at[2]), pltpu.make_async_copy(k_in, kv_out.at[0, pl.ds(0, p.cache)], b_sem.at[3]),
              pltpu.make_async_copy(v_in, kv_out.at[1, pl.ds(0, p.cache)], b_sem.at[4]), pltpu.make_async_copy(bias_in, b1, b_sem.at[6]),
              pltpu.make_async_copy(gain_in, g1, b_sem.at[7])]
    for c in little:
        c.start()

    barrier = pltpu.get_barrier_semaphore()
    for k in range(1, 4):
        pl.semaphore_signal(barrier, inc=1, device_id={'tp': lax.rem(tp + k, 4)}, device_id_type=MESH)
        pl.semaphore_signal(barrier, inc=1, device_id={'cp': lax.rem(cp + k, 4)}, device_id_type=MESH)

    def cache_copies(owner, peer, k):
        at = pl.multiple_of(owner * p.cache, p.cache)
        ks = ka.at[:, pl.ds(at, p.cache)]
        vs = vt.at[:, :, pl.ds(at, p.cache)]
        return (pltpu.make_async_remote_copy(ks, ks, cs_send.at[k, 0], cs_recv.at[k, 0], device_id={'cp': peer}, device_id_type=MESH),
                pltpu.make_async_remote_copy(vs, vs, cs_send.at[k, 1], cs_recv.at[k, 1], device_id={'cp': peer}, device_id_type=MESH))

    def new_copies(at, size, peer, k):
        ks = ka.at[:, pl.ds(at, size)]
        vs = vt.at[:, :, pl.ds(at, size)]
        return (pltpu.make_async_remote_copy(ks, ks, kv_send.at[k, 0], kv_recv.at[k, 0], device_id={'cp': peer}, device_id_type=MESH),
                pltpu.make_async_remote_copy(vs, vs, kv_send.at[k, 1], kv_recv.at[k, 1], device_id={'cp': peer}, device_id_type=MESH))

    little[1].wait()
    little[2].wait()
    here = pl.multiple_of(cp * p.cache, p.cache)
    for g in range(p.kv):
        ka[g, pl.ds(here, p.cache), :] = kv_out[0, 0:p.cache].astype(jnp.float32)[:, g, :].astype(jnp.bfloat16)
        vt[g, :, pl.ds(here, p.cache)] = kv_out[1, 0:p.cache].astype(jnp.float32)[:, g, :].T.astype(jnp.bfloat16)
    pl.semaphore_wait(barrier, 6)
    for peer, k in ((across, 1), (partner, 0)):
        for c in cache_copies(cp, peer, k):
            c.start()
    for c in (little[0], little[3], little[4]):
        c.wait()
    small[0:1, 0:goff] = b1[...].astype(jnp.float32).reshape(1, goff)
    small[0:1, goff:goff + p.dim] = g1[...].astype(jnp.float32).reshape(1, p.dim)
    rope[...] = rope_t[...].T

    def send_new(r):
        at = pl.multiple_of(new0 + r * rows4, rows4)

        @pl.when(cp == 0)
        def _():
            for c in new_copies(at, rows4, across, 1):
                c.start()

        @pl.when(lax.rem(cp, 2) == 0)
        def _():
            for c in new_copies(at, rows4, partner, 0):
                c.start()

    lane = lax.broadcasted_iota(jnp.int32, (1, HEAD), 1)
    even = lax.rem(lane, 2) == 0
    turned = lane < 64

    def angles(rows, count):
        r = rope[rows, :]
        both = jnp.concatenate([r, r], axis=1)
        at = lax.broadcasted_iota(jnp.int32, (count, HEAD), 1)
        pair = lax.rem(at, 64) // 2
        c = jnp.take_along_axis(both, pair, axis=1)
        s = jnp.take_along_axis(both, pair + 32, axis=1)
        return c, jnp.where(even, -s, s)

    def rotate(a, c, s):
        swap = jnp.where(even, pltpu.roll(a, HEAD - 1, 1), pltpu.roll(a, 1, 1))
        return jnp.where(turned, a * c + swap * s, a)

    for g in range(p.kv):
        wkv_copy(g).wait()
    for r in range(1, 4):
        x_copy(r).start()
    wq_copy(0).start()
    nsub = max(8, rows4 // 32)
    sub = rows4 // nsub
    wide = 512

    def norm(b):
        rows = pl.ds(pl.multiple_of(b * sub, sub), sub)
        total = None
        for c in range(0, p.dim, wide):
            v = h[rows, c:c + wide].astype(jnp.float32)
            v = v * v
            for k in range(0, wide, HEAD):
                total = v[:, k:k + HEAD] if total is None else total + v[:, k:k + HEAD]
        inv = lax.rsqrt(jnp.sum(total, axis=1, keepdims=True) * (1.0 / p.dim) + EPS)
        for c in range(0, p.dim, wide):
            v = h[rows, c:c + wide].astype(jnp.float32)
            h[rows, c:c + wide] = (v * inv * small[0:1, goff + c:goff + c + wide]).astype(jnp.bfloat16)

    def keys_values(r, ahead):
        rows = pl.ds(pl.multiple_of(r * rows4, rows4), rows4)
        at = pl.multiple_of(new0 + r * rows4, rows4)
        a = None
        per = nsub // 8
        deep = p.dim // 8
        for e in range(8):
            part = jnp.dot(h[rows, e * deep:(e + 1) * deep], w[1, e * deep:(e + 1) * deep, :], preferred_element_type=jnp.float32)
            a = part if a is None else a + part
            if ahead:
                for b in range(per):
                    norm((r + 1) * nsub + e * per + b)
        c, s = angles(rows, rows4)
        keys, vals = [], []
        for g in range(p.kv):
            col = g * (p.group + 2) * HEAD + p.group * HEAD
            keys.append(rotate(a[:, g * 2 * HEAD:g * 2 * HEAD + HEAD] + small[0:1, col:col + HEAD], c, s))
            vals.append(a[:, g * 2 * HEAD + HEAD:(g + 1) * 2 * HEAD] + small[0:1, col + HEAD:col + 2 * HEAD])
            ka[g, pl.ds(at, rows4), :] = keys[g].astype(jnp.bfloat16)
            vt[g, :, pl.ds(at, rows4)] = vals[g].T.astype(jnp.bfloat16)
        kv_out[0, rows] = jnp.swapaxes(jnp.stack(keys), 0, 1).astype(jnp.bfloat16)
        kv_out[1, rows] = jnp.swapaxes(jnp.stack(vals), 0, 1).astype(jnp.bfloat16)

    def kv_step(r, _):
        x_copy(r + 1).wait()

        @pl.when(r > 0)
        def _():
            send_new(r - 1)

        keys_values(r, True)
        return 0

    x_copy(0).wait()
    for b in range(nsub):
        norm(b)
    lax.fori_loop(0, 3, kv_step, 0)
    send_new(2)
    keys_values(3, False)
    wq_copy(1).start()
    send_new(3)

    @pl.when(cp == 1)
    def _():
        for c in new_copies(new0, p.tok, across, 1):
            c.start()

    def out_copies():
        return [pltpu.make_async_copy(kv_out.at[0], kn, out_sem.at[0]), pltpu.make_async_copy(kv_out.at[1], vn, out_sem.at[1])]

    for c in out_copies():
        c.start()

    def reset(i, _):
        m_s[i] = jnp.full((8, p.n), LOW, jnp.float32)
        l_s[i] = jnp.zeros((8, p.n), jnp.float32)
        o_t[i] = jnp.zeros((HEAD, p.n), jnp.float32)
        return 0

    lax.fori_loop(0, p.nd, reset, 0)

    def q_tile(t):
        j = lax.rem(t, p.nq)
        first = t // p.nq * 2
        count = 2
        rows = pl.ds(pl.multiple_of(first * p.mr, p.mr), count * p.mr)
        wq_copy(t).wait()
        a = jnp.dot(h[rows, :], w[lax.rem(t, 2)], preferred_element_type=jnp.float32)
        a = a + small[0:1, pl.ds(pl.multiple_of(wq_col(j), HEAD), p.wcols)]
        c, s = angles(rows, count * p.mr)
        for k in range(QUAD):
            b = rotate(a[:, k * HEAD:(k + 1) * HEAD], c, s).astype(jnp.bfloat16)
            for u in range(count):
                q[lax.rem(first + u, 4), 2 * j + k // 2, (k % 2) * p.mr:(k % 2 + 1) * p.mr, :] = b[u * p.mr:(u + 1) * p.mr, :]

        @pl.when(t + 2 < p.wt)
        def _():
            wq_copy(t + 2).start()

    part_rows = min(256, p.kt)
    row_of = lax.rem(lax.broadcasted_iota(jnp.int32, (p.kt, p.n), 1), p.mr) - lax.broadcasted_iota(jnp.int32, (p.kt, p.n), 0)

    def scores(qs, pair, off, k, bound):
        g = pair // p.dpg
        s = lax.dot_general(ka[g, pl.ds(pl.multiple_of(off, p.kt), p.kt), :], q[qs, pair], (((1,), (1,)), ((), ())),
                            preferred_element_type=jnp.float32) * scale
        if bound is not None:
            s = jnp.where(row_of >= -bound, s, LOW)
        s_t[k] = s
        mx_t[k] = jnp.max(s.reshape(p.kt // 8, 8, p.n), axis=0)

    def weigh(pair, off, k):
        g = pair // p.dpg
        m_old = m_s[pair, 0:1, :]
        m_new = jnp.maximum(m_old, jnp.max(mx_t[k], axis=0, keepdims=True))
        alpha = jnp.exp2(m_old - m_new)
        m_s[pair, 0:1, :] = m_new
        acc = None
        es = []
        for r in range(0, p.kt, part_rows):
            e = jnp.exp2(s_t[k, r:r + part_rows, :] - m_new)
            part = jnp.sum(e.reshape(part_rows // 8, 8, p.n), axis=0)
            acc = part if acc is None else acc + part
            es.append(e.astype(jnp.bfloat16))
        d = jnp.dot(vt[g, :, pl.ds(pl.multiple_of(off, p.kt), p.kt)], jnp.concatenate(es, axis=0), preferred_element_type=jnp.float32)
        l_s[pair] = l_s[pair] * alpha + acc
        o_t[pair] = o_t[pair] * alpha + d

    anything = 1 << 20
    slots = p.look + 1

    def own_at(j):
        return new0 + j * p.kt

    def own_segment(u, j, tiles):
        qs = lax.rem(u, 4)
        bound = u * p.mr - j * p.kt
        more = j + 1 < tiles

        @pl.when(j == 0)
        def _():
            for i in range(p.look):
                scores(qs, i, new0, i, u * p.mr)

        for i in range(p.nd):
            n = i + p.look
            if n < p.nd:
                scores(qs, n, own_at(j), n % slots, bound)
            else:
                n -= p.nd
                scores(qs, jnp.where(more, n, n // 2), jnp.where(more, own_at(j + 1), (n % 2) * p.kt), (n + p.nd) % slots,
                       jnp.where(more, bound - p.kt, anything))
            weigh(i, own_at(j), i % slots)

    def block_at(b):
        return jnp.where(b == 0, 0, p.tok * (1 + jnp.where((cp == 3) & (b == 1), 2, jnp.where(cp == 3, b - 2, b - 1))))

    def block_segment(u, b, count):
        qs = lax.rem(u, 4)
        at = block_at(b)
        following = jnp.where((u > 0) & (b + 1 < count), block_at(b + 1), 0)

        @pl.when((u == 0) & (b > 0))
        def _():
            for i in range(p.look):
                scores(qs, i // 2, at + (i % 2) * p.kt, i, None)

        for i in range(2 * p.nd):
            n = i + p.look
            scores(qs, (n // 2) % p.nd, (at if n < 2 * p.nd else following) + (n % 2) * p.kt, n % slots, None)
            weigh(i // 2, at + (i % 2) * p.kt, i % slots)

    blocks = 1 + cp

    role_a = 3 - tp
    role_b = tp

    def chain(d, i):
        m = i // p.cpm
        j = lax.rem(i, p.cpm)
        mine = own.at[lax.rem(m, p.owns), j, pl.ds(d * p.half, p.half)]
        rows = pl.ds(pl.multiple_of(m * p.mr + d * p.half, p.half), p.half)
        cols = pl.ds(pl.multiple_of(j * p.cc, p.cc), p.cc)
        return mine, land.at[d, lax.rem(i, p.ring)], y.at[rows, cols]

    def peers(d):
        return (jnp.maximum(tp - 1, 0), jnp.minimum(tp + 1, 3)) if d == 0 else (jnp.minimum(tp + 1, 3), jnp.maximum(tp - 1, 0))

    def rs_copy(d, i):
        mine, there, _ = chain(d, i)
        return pltpu.make_async_remote_copy(mine, there, rs_send.at[d, lax.rem(i, p.owns * p.cpm)], rs_recv.at[d, lax.rem(i, p.ring)],
                                            device_id={'tp': peers(d)[0]}, device_id_type=MESH)

    def ag_copy(d, i, src=None):
        out = chain(d, i)[2]
        return pltpu.make_async_remote_copy(out if src is None else src, out, ag_send.at[d, i], ag_recv.at[d, i],
                                            device_id={'tp': peers(d)[1]}, device_id_type=MESH)

    def yl_copy(d, i):
        k = lax.rem(i, p.ys)
        return pltpu.make_async_copy(yst.at[d, k], chain(d, i)[2], yl_sem.at[d, k])

    def guest_copy(src, dst, k, d, peer):
        return pltpu.make_async_remote_copy(src, dst, g_send.at[k, d], g_recv.at[k, d], device_id=peer, device_id_type=MESH)

    def guest_out(d):
        return guest_copy(chain(d, p.guest)[0], g_in.at[d], 0, d, {'cp': across})

    def guest_sum(d):
        return guest_copy(g_in.at[d], g_land.at[d], 1, d, {'tp': peers(d)[0]})

    def guest_row(d):
        return guest_copy(g_y.at[d], g_y.at[d], 2, d, {'tp': peers(d)[1]})

    def guest_home(d):
        return guest_copy(g_y.at[d], chain(d, p.guest)[2], 3, d, {'cp': across})

    def pick(role, table):
        res = []
        for k in range(len(table[0])):
            v = table[0][k]
            for r in range(1, len(table)):
                v = jnp.where(role == r, table[r][k], v)
            res.append(v)
        return res

    due = [(d, role, pick(role, p.sums), pick(2 - role, p.rows)) for d, role in ((0, role_a), (1, role_b))]

    def when_due(seg, words, act):
        rest = lax.rem(seg, p.nseg)
        w = words[0]
        for k in range(1, len(words)):
            w = jnp.where(rest >= 5 * k, words[k], w)
        code = jnp.bitwise_and(jnp.right_shift(w, 6 * lax.rem(rest, 5)), 63) - 1
        m = seg // p.nseg - jnp.maximum(code, 0) // p.cpm

        @pl.when((code >= 0) & (m >= 0) & (m < p.nm))
        def _():
            act(m * p.cpm + lax.rem(code, p.cpm))

    def service(seg):
        for d, role, sum_words, _ in due:
            def sums(i, d=d, role=role):
                mine, arrived, _ = chain(d, i)
                stays = (cp < 2) | (i != p.guest)

                @pl.when((role > 0) & stays)
                def _():
                    rs_copy(d, i).wait_recv()

                @pl.when((role > 0) & (role < 3) & stays)
                def _():
                    mine[...] = mine[...] + arrived[...]

                @pl.when((role < 3) & (i >= p.ring))
                def _():
                    pl.semaphore_wait(free_sem.at[d], 1)

                @pl.when((role < 3) & stays)
                def _():
                    rs_copy(d, i).start()

                k = lax.rem(i, p.ys)

                @pl.when((role == 3) & (i >= p.ys) & ((cp < 2) | (i - p.ys != p.guest)))
                def _():
                    yl_copy(d, i - p.ys).wait()
                    ag_copy(d, i - p.ys, yst.at[d, k]).wait_send()

                @pl.when((role == 3) & stays)
                def _():
                    yst[d, k] = (mine[...] + arrived[...]).astype(jnp.bfloat16)
                    yl_copy(d, i).start()
                    ag_copy(d, i, yst.at[d, k]).start()

                @pl.when((role > 0) & (i < p.chunks - p.ring))
                def _():
                    pl.semaphore_signal(free_sem.at[d], inc=1, device_id={'tp': peers(d)[1]}, device_id_type=MESH)

            when_due(seg, sum_words, sums)

        for d, role, _, row_words in due:
            def rows(i, d=d, role=role):
                stays = (cp < 2) | (i != p.guest)

                @pl.when((role < 3) & stays)
                def _():
                    ag_copy(d, i).wait_recv()

                @pl.when((role < 3) & (role > 0) & stays)
                def _():
                    ag_copy(d, i).start()

            when_due(seg, row_words, rows)

        @pl.when((cp >= 2) & (seg == p.g_out))
        def _():
            for d in range(2):
                guest_out(d).start()

        for d, role, _, _ in due:
            for r in range(4):
                @pl.when((cp < 2) & (role == r) & (seg == p.g_sums[r]))
                def _():
                    guest_out(d).wait_recv()
                    if r > 0:
                        guest_sum(d).wait_recv()
                    if r < 3:
                        if r > 0:
                            g_in[d] = g_in[d] + g_land[d]
                        guest_sum(d).start()
                    else:
                        g_y[d] = (g_in[d] + g_land[d]).astype(jnp.bfloat16)
                        guest_row(d).start()
                        guest_home(d).start()

            for r in range(3):
                @pl.when((cp < 2) & (role == 2 - r) & (seg == p.g_rows[r]))
                def _():
                    guest_row(d).wait_recv()
                    if r < 2:
                        guest_row(d).start()
                    guest_home(d).start()

    take_a = jnp.where(tp == 0, 1, 0).astype(jnp.float32)
    take_b = jnp.where(tp == 3, 1, 0).astype(jnp.float32)
    x_half = jnp.where(tp == 3, p.half, 0)

    def xb_copy(m):
        return pltpu.make_async_copy(x.at[pl.ds(pl.multiple_of(m * p.mr + x_half, p.half), p.half)], xb, b_sem.at[5])

    def first_q(t, _):
        q_tile(t)

        @pl.when(t == max(0, p.nq - 3))
        def _():
            for n in range(p.nt):
                wo_copy(n).start()

        return 0

    lax.fori_loop(0, p.nq, first_q, 0)

    for c in cache_copies(across, partner, 1):
        c.wait_recv()
    for c in cache_copies(across, partner, 2):
        c.start()
    for k in (0, 2):
        for c in cache_copies(cp, partner, k):
            c.wait_recv()

    def segment(seg, _):
        m = seg // p.nseg
        s = lax.rem(seg, p.nseg)
        busy = m < p.nm
        tiles = (m * p.mr + p.mr + p.kt - 1) // p.kt

        @pl.when(busy & (s < tiles) & (s < p.s_blk))
        def _():
            @pl.when(s == 0)
            def _():
                xb_copy(m).start()

            own_segment(m, s, tiles)

        @pl.when((seg == p.s_blk + 1) & (lax.rem(cp, 2) == 1))
        def _():
            for c in new_copies(pl.multiple_of(p.tok * cp, p.tok), p.tok, partner, 0):
                c.wait_recv()

        direct = pl.multiple_of(p.tok * jnp.maximum(cp - 1, 0), p.tok)

        @pl.when((cp == 3) & (seg == p.s_blk + 2))
        def _():
            for c in new_copies(direct, p.tok, partner, 2):
                c.wait_recv()

        @pl.when((cp >= 2) & (seg == p.s_blk + cp - 1))
        def _():
            for c in new_copies(direct, p.tok, partner, 1):
                c.wait_recv()
            for c in new_copies(direct, p.tok, partner, 2):
                c.start()

        @pl.when((cp == 2) & (seg == p.s_blk + 2))
        def _():
            for c in new_copies(direct, p.tok, partner, 2):
                c.wait_recv()

        @pl.when(busy & (s >= p.s_blk) & (s < p.s_blk + blocks))
        def _():
            block_segment(m, s - p.s_blk, blocks)

        @pl.when(busy & (s == p.s_fin))
        def _():
            def finish(i, _):
                for e in range(p.fin):
                    c = i * p.fin + e
                    v = o_t[c] * (1.0 / jnp.sum(l_s[c], axis=0, keepdims=True))
                    for k in range(2):
                        o[:, pl.ds(pl.multiple_of((c * 2 + k) * HEAD, HEAD), HEAD)] = v[:, k * p.mr:(k + 1) * p.mr].T.astype(jnp.bfloat16)
                    reset(c, 0)
                return 0

            lax.fori_loop(0, p.nd // p.fin, finish, 0)

        @pl.when(busy & (s >= p.s_out) & (s < p.s_q))
        def _():
            n = s - p.s_out

            @pl.when(n == 0)
            def _():
                xb_copy(m).wait()

            @pl.when((n == 0) & (m >= p.owns))
            def _():
                for d, role in ((0, role_a), (1, role_b)):
                    for j in range(p.cpm):
                        i = (m - p.owns) * p.cpm + j

                        @pl.when((role < 3) & ((cp < 2) | (i != p.guest)))
                        def _():
                            rs_copy(d, i).wait_send()

                        if j == p.guest % p.cpm:
                            @pl.when((cp >= 2) & (i == p.guest))
                            def _():
                                guest_out(d).wait_send()

            @pl.when(m == 0)
            def _():
                wo_copy(n).wait()

            a = jnp.dot(o[...], wo[n], preferred_element_type=jnp.float32)
            r = xb[:, pl.ds(pl.multiple_of(n * p.wcols, HEAD), p.wcols)].astype(jnp.float32)
            own[lax.rem(m, p.owns), n, 0:p.half, :] = a[0:p.half] + r * take_a
            own[lax.rem(m, p.owns), n, p.half:p.mr, :] = a[p.half:p.mr] + r * take_b

        @pl.when((m < p.nm - 2) & (s >= p.s_q))
        def _():
            q_tile((m // 2 + 1) * p.nq + lax.rem(m, 2) * p.hq + s - p.s_q)

        service(seg)
        return 0

    lax.fori_loop(0, p.total, segment, 0)

    for d, role in ((0, role_a), (1, role_b)):
        @pl.when(role < 3)
        def _():
            def last_sums(i, _):
                rs_copy(d, i).wait_send()
                return 0
            lax.fori_loop((p.nm - p.owns) * p.cpm, p.chunks, last_sums, 0)

        @pl.when((role > 0) & (role < 3))
        def _():
            def last_rows(i, _):
                @pl.when((cp < 2) | (i != p.guest))
                def _():
                    ag_copy(d, i).wait_send()
                return 0
            lax.fori_loop(0, p.chunks, last_rows, 0)

        @pl.when(role == 3)
        def _():
            for k in range(p.ys):
                i = p.chunks - p.ys + k
                yl_copy(d, i).wait()
                ag_copy(d, i, yst.at[d, k]).wait_send()

    for d, role in ((0, role_a), (1, role_b)):
        @pl.when(cp >= 2)
        def _():
            guest_home(d).wait_recv()

        @pl.when((cp < 2) & (role < 3))
        def _():
            guest_sum(d).wait_send()

        @pl.when((cp < 2) & (role > 0))
        def _():
            guest_row(d).wait_send()

        @pl.when(cp < 2)
        def _():
            guest_home(d).wait_send()

    for c in out_copies():
        c.wait()
    for k in (0, 1):
        for c in cache_copies(cp, partner, k):
            c.wait_send()
    for c in cache_copies(across, partner, 2):
        c.wait_send()

    @pl.when(cp < 2)
    def _():
        for c in new_copies(new0, p.tok, across, 1):
            c.wait_send()

    @pl.when(lax.rem(cp, 2) == 0)
    def _():
        for c in new_copies(new0, p.tok, partner, 0):
            c.wait_send()

    @pl.when(cp >= 2)
    def _():
        for c in new_copies(pl.multiple_of(p.tok * (cp - 1), p.tok), p.tok, partner, 2):
            c.wait_send()


def settle(pieces, *refs):
    n = len(pieces)
    src, dst, hold, sems = refs[:n], refs[n:2 * n], refs[2 * n:3 * n], refs[3 * n]
    into, out = [], []
    for a, count in enumerate(pieces):
        rows = src[a].shape[0] // count
        for k in range(count):
            at = pl.ds(k * rows, rows)
            i = len(into)
            into.append(pltpu.make_async_copy(src[a].at[at], hold[a].at[at], sems.at[0, i]))
            out.append(pltpu.make_async_copy(hold[a].at[at], dst[a].at[at], sems.at[1, i]))
    for c in into:
        c.start()
    for c, d in zip(into, out):
        c.wait()
        d.start()
    for d in out:
        d.wait()


def build(p):
    def local_step(x, k_cache, v_cache, rope_table, norm_gain, w_qkv, b_qkv, w_out):
        anyspace = pl.BlockSpec(memory_space=pl.ANY)
        bf, f32 = jnp.bfloat16, jnp.float32
        dma = pltpu.SemaphoreType.DMA
        kv_shape = jax.ShapeDtypeStruct((p.tok, p.kv, HEAD), bf)
        y, k_new, v_new = pl.pallas_call(
            functools.partial(kernel, p),
            name='block',
            out_shape=(jax.ShapeDtypeStruct((p.tok, p.dim), bf), kv_shape, kv_shape),
            in_specs=[anyspace] * 8,
            out_specs=(anyspace, anyspace, anyspace),
            scratch_shapes=[
                pltpu.VMEM((p.tok, p.dim), bf),
                pltpu.VMEM((p.kv, p.keys, HEAD), bf),
                pltpu.VMEM((p.kv, HEAD, p.keys), bf),
                pltpu.VMEM((64, p.tok), f32),
                pltpu.VMEM((p.tok, 64), f32),
                pltpu.VMEM(((p.group + 2) * p.kv * HEAD,), bf),
                pltpu.VMEM((p.dim,), bf),
                pltpu.VMEM((1, (p.group + 2) * p.kv * HEAD + p.dim), f32),
                pltpu.VMEM((4, p.nd, p.n, HEAD), bf),
                pltpu.VMEM((p.nd, HEAD, p.n), f32),
                pltpu.VMEM((p.mr, p.heads * HEAD), bf),
                pltpu.VMEM((p.look + 1, p.kt, p.n), f32),
                pltpu.VMEM((p.look + 1, 8, p.n), f32),
                pltpu.VMEM((p.nd, 8, p.n), f32),
                pltpu.VMEM((p.nd, 8, p.n), f32),
                pltpu.VMEM((p.owns, p.cpm, p.mr, p.cc), f32),
                pltpu.VMEM((2, p.ring, p.half, p.cc), f32),
                pltpu.VMEM((2, p.ys, p.half, p.cc), bf),
                pltpu.VMEM((2, p.half, p.cc), f32),
                pltpu.VMEM((2, p.half, p.cc), f32),
                pltpu.VMEM((2, p.half, p.cc), bf),
                pltpu.VMEM((p.half, p.dim), bf),
                pltpu.VMEM((2, p.dim, p.wcols), bf),
                pltpu.VMEM((p.nt, p.heads * HEAD, p.wcols), bf),
                pltpu.VMEM((2, p.tok, p.kv, HEAD), bf),
                dma((4,)), dma((2,)), dma((p.nt,)), dma((8,)), dma((2,)),
                dma((3, 2)), dma((3, 2)), dma((3, 2)), dma((3, 2)),
                dma((2, p.owns * p.cpm)), dma((2, p.ring)), pltpu.SemaphoreType.REGULAR((2,)), dma((2, p.chunks)), dma((2, p.chunks)), dma((2, p.ys)),
                dma((4, 2)), dma((4, 2)),
            ],
            compiler_params=pltpu.CompilerParams(collective_id=0, has_side_effects=True, vmem_limit_bytes=67_000_000),
        )(x, k_cache, v_cache, rope_table.T, norm_gain, b_qkv, w_qkv, w_out)
        res = (y, k_new, v_new)
        pieces = (16, 1, 1)
        return pl.pallas_call(
            functools.partial(settle, pieces),
            name='settle',
            out_shape=tuple(jax.ShapeDtypeStruct(r.shape, r.dtype) for r in res),
            in_specs=[anyspace] * 3,
            out_specs=(anyspace,) * 3,
            scratch_shapes=[pltpu.VMEM(r.shape, r.dtype) for r in res] + [dma((2, sum(pieces)))],
            compiler_params=pltpu.CompilerParams(vmem_limit_bytes=67_000_000),
        )(*res)

    return local_step


def solution(mesh):
    row_spec = P(('dp', 'cp'), None)
    cache_spec = P(('dp', 'cp'), 'tp', None)
    p = Plan(tok=1024, dim=4096, kv=2, group=12, cache=256, nm=8, kt=512)
    p.table([[7, 10, 15, 16, 17, 19, 20, 21], [15, 17, 19, 20, 21, 22, 23, 28], [18, 20, 21, 22, 23, 27, 32, 33], [20, 22, 24, 29, 32, 34, 35, 37]],
            [[28, 32, 33, 36, 37, 38, 39, 40], [35, 36, 37, 38, 39, 40, 42, 46], [37, 38, 39, 40, 41, 47, 50, 52]])
    return jax.shard_map(build(p), mesh=mesh, in_specs=(row_spec, cache_spec, cache_spec, row_spec, P(None), P(None, 'tp'), P('tp'), P('tp', None)),
                         out_specs=(row_spec, cache_spec, cache_spec), check_vma=False)
```
